256 devices in a mesh: seq: 32 (over y, x, core), tp: 8 (over z).
Axes of the slice: x: 4, y: 4, z: 8, core: 2. Of those that a mesh axis runs over, the one named last changes fastest.
Arguments:
- hidden_in: bfloat16 [2, 16384, 2560], P(None, 'seq'), may hold values from -6 to 6
- gate_proj: bfloat16 [2560, 5120], P(None, 'tp'), may hold values from -0.125 to 0.125
- value_proj: bfloat16 [2560, 5120], P(None, 'tp'), may hold values from -0.125 to 0.125
- bc_proj: bfloat16 [2560, 256], P(None, 'tp'), may hold values from -0.125 to 0.125
- step_proj: bfloat16 [2560, 80], P(None, 'tp'), may hold values from -0.125 to 0.125
- value_conv: float32 [4, 5120], P(None, 'tp'), may hold values from -3 to 3
- bc_conv: float32 [4, 256], replicated, may hold values from -3 to 3
- step_bias: float32 [80], P('tp'), may hold values from -1.5 to 0
- log_rate: float32 [80], P('tp'), as said below
- norm_gain: float32 [5120], P('tp'), may hold values from 0.25 to 1.75
Outputs:
- mixer_out: bfloat16 [2, 16384, 5120], P(None, 'seq', 'tp')
The draws below stay inside these ranges and needn't reach their ends.
Inputs may be any that keep to these rules, and one draw needn't show every extreme that they name: log_rate lies between -1.5 - ln(16384) and 1.0 - ln(16384).
All inputs are finite; a program needn't handle non-finite values.
Results may differ from the reference program's by a relative error of at most 0.0095.
Values may be sent and summed in bfloat16 or wider, within the bound.
A program may use at most 128 MiB of HBM per device.

```python
import math
import jax
import jax.numpy as jnp
from jax import lax

D = 2560
DI = 5120
HEADS = 80
HEAD_DIM = 64
STATE = 128
CONV = 4
BATCH = 2
BLOCK = 64
SEQ_LEN = 16384


def draw_log_rate(key, part):
    shift = math.log(SEQ_LEN)
    return jax.random.uniform(key, (HEADS,), jnp.float32, -1.5 - shift, 1.0 - shift)


def level_of(own_key, dims, cuts, smallest, top_value):
    def one(axis_at, blocks):
        draws = jax.random.uniform(jax.random.fold_in(jax.random.fold_in(own_key, 6), axis_at), (blocks,), jnp.float32, smallest / len(cuts), top_value / len(cuts))
        return jnp.repeat(jnp.exp(draws), dims[axis_at] // blocks).reshape((-1,) + (1,) * (len(dims) - axis_at - 1))

    level = one(*cuts[0])
    for cut in cuts[1:]:
        level = level * one(*cut)
    return level


def noise(rng, extent, deviation, reach, shards=(), kind=jnp.bfloat16):
    entries = deviation * jax.random.normal(rng, extent, jnp.float32)
    if shards:
        entries = entries * level_of(rng, extent, shards, -0.22, 0.18)
    return jnp.clip(entries, -reach, reach).astype(kind)


def setup_inputs(seed: int = 0) -> dict:
    streams_of = jax.random.split(jax.random.key(seed), 11)
    hidden_in = noise(streams_of[0], (BATCH, SEQ_LEN, D), 1.0, 6.0, ((1, 32),))
    gate_proj = noise(streams_of[1], (D, DI), D ** -0.5, 0.125, ((1, 8),))
    value_proj = noise(streams_of[2], (D, DI), D ** -0.5, 0.125, ((1, 8),))
    bc_proj = noise(streams_of[3], (D, 2 * STATE), D ** -0.5, 0.125, ((1, 8),))
    step_proj = noise(streams_of[4], (D, HEADS), D ** -0.5, 0.125, ((1, 8),))
    value_conv = noise(streams_of[5], (CONV, DI), CONV ** -0.5, 3.0, ((1, 8),), jnp.float32)
    bc_conv = noise(streams_of[6], (CONV, 2 * STATE), CONV ** -0.5, 3.0, (), jnp.float32)
    step_bias = jnp.clip(-1.5 + 1.5 * jax.random.uniform(streams_of[7], (HEADS,), jnp.float32) ** level_of(streams_of[7], (HEADS,), ((0, 8),), -0.2, 0.2), -1.5, 0.0)
    log_rate = draw_log_rate(jax.random.fold_in(streams_of[10], 71), 0)
    norm_gain = jnp.clip(1.0 + 0.15 * jax.random.normal(streams_of[9], (DI,), jnp.float32), 0.25, 1.75)
    return {"hidden_in": hidden_in, "gate_proj": gate_proj, "value_proj": value_proj, "bc_proj": bc_proj, "step_proj": step_proj, "value_conv": value_conv, "bc_conv": bc_conv, "step_bias": step_bias, "log_rate": log_rate, "norm_gain": norm_gain}


epsilon = 1e-05

def conv_silu(padded, kernel, length):
    running = jnp.zeros((padded.shape[0], length, padded.shape[2]), jnp.float32)
    for tap_index in range(kernel.shape[0]):
        running = running + kernel[tap_index] * padded[:, tap_index:tap_index + length, :]
    return jax.nn.silu(running)

def block_step(carried, inputs):
    values, log_decay, step_sizes, b_rows, c_rows = inputs
    length = log_decay.shape[1]
    cumulative = jnp.cumsum(log_decay, axis=1)
    log_gap = cumulative[:, :, None, :] - cumulative[:, None, :, :]
    causal = jnp.arange(length)[:, None] >= jnp.arange(length)[None, :]
    weights_in = jnp.exp(jnp.where(causal[None, :, :, None], log_gap, -jnp.inf))
    scores = jnp.einsum('bin,bjn->bij', c_rows, b_rows, precision=lax.Precision.HIGHEST)
    mixing = scores[:, :, :, None] * weights_in * step_sizes[:, None, :, :]
    within = jnp.einsum('bijh,bjhp->bihp', mixing, values, precision=lax.Precision.HIGHEST)
    earlier = jnp.einsum('bin,bhpn->bihp', c_rows, carried, precision=lax.Precision.HIGHEST)
    earlier = earlier * jnp.exp(cumulative)[..., None]
    remain = jnp.exp(cumulative[:, -1:, :] - cumulative) * step_sizes
    added_state = jnp.einsum('bjh,bjhp,bjn->bhpn', remain, values, b_rows, precision=lax.Precision.HIGHEST)
    updated = jnp.exp(cumulative[:, -1, :])[:, :, None, None] * carried + added_state
    return (updated, within + earlier)

def to_blocks(series, batch_size, blocks):
    return jnp.moveaxis(series.reshape((batch_size, blocks, BLOCK) + series.shape[2:]), 1, 0)

def reference(hidden_in, gate_proj, value_proj, bc_proj, step_proj, value_conv, bc_conv, step_bias, log_rate, norm_gain):
    flat_rows = hidden_in.reshape(-1, D)
    gate_pre = jnp.dot(flat_rows, gate_proj, preferred_element_type=jnp.float32).astype(jnp.bfloat16)
    value_pre = jnp.dot(flat_rows, value_proj, preferred_element_type=jnp.float32).astype(jnp.bfloat16)
    bc_pre = jnp.dot(flat_rows, bc_proj, preferred_element_type=jnp.float32).astype(jnp.bfloat16)
    step_pre = jnp.dot(flat_rows, step_proj, preferred_element_type=jnp.float32)
    value_pad = jnp.pad(value_pre.reshape(BATCH, SEQ_LEN, DI).astype(jnp.float32), ((0, 0), (CONV - 1, 0), (0, 0)))
    bc_pad = jnp.pad(bc_pre.reshape(BATCH, SEQ_LEN, 2 * STATE).astype(jnp.float32), ((0, 0), (CONV - 1, 0), (0, 0)))
    values = conv_silu(value_pad, value_conv, SEQ_LEN).reshape(BATCH, SEQ_LEN, HEADS, HEAD_DIM)
    bc_rows = conv_silu(bc_pad, bc_conv, SEQ_LEN)
    b_rows = bc_rows[..., :STATE]
    c_rows = bc_rows[..., STATE:]
    step_sizes = jax.nn.softplus(step_pre.reshape(BATCH, SEQ_LEN, HEADS) + step_bias)
    log_decay = -step_sizes * jnp.exp(log_rate)
    blocks = SEQ_LEN // BLOCK
    initial = jnp.zeros((BATCH, HEADS, HEAD_DIM, STATE), jnp.float32)
    final_state, outputs = lax.scan(block_step, initial, (to_blocks(values, BATCH, blocks), to_blocks(log_decay, BATCH, blocks), to_blocks(step_sizes, BATCH, blocks), to_blocks(b_rows, BATCH, blocks), to_blocks(c_rows, BATCH, blocks)))
    mixed_out = jnp.moveaxis(outputs, 0, 1).reshape(BATCH, SEQ_LEN, DI)
    gated_out = mixed_out * jax.nn.silu(gate_pre.reshape(BATCH, SEQ_LEN, DI).astype(jnp.float32))
    scale_sq = lax.optimization_barrier(jnp.sum(gated_out * gated_out, axis=-1, keepdims=True)) / DI
    return (gated_out * lax.rsqrt(scale_sq + epsilon) * norm_gain).astype(jnp.bfloat16)
```

```python
import jax
import jax.numpy as jnp
from jax import lax
from jax.experimental import pallas as pl
from jax.experimental.pallas import tpu as pltpu
from jax.sharding import PartitionSpec as P

MESH = pl.DeviceIdType.MESH
F32, BF16 = jnp.float32, jnp.bfloat16

NS, NZ = 32, 8
D, DI = 2560, 5120
CI = 640
LEN = 512
Q = 128
NB = LEN // Q
PAD = 16
HL = 32
HEADS = 10
EPS = 1e-05


def dot(a, b):
    return jnp.dot(a, b, preferred_element_type=F32)


def silu(x):
    half = 0.5 * x
    return half + half * jnp.tanh(half)


def split(x):
    high = x.astype(BF16)
    low = (x - high.astype(F32)).astype(BF16)
    return jnp.concatenate([high, low], axis=1)


def kernel(
    hid, gw, vw, bw, sw, vconv, bconv, sbias, lrate, gain, out,
    hx, w, bwv, swv, cv, bcv, sb, lr, gn, prm, tap, ee, bs, vp, bct, cmat, bmat,
    av, ev, fg, g, rx, dsum, dall, dxl, dx, vv, sbl, st, p1, po, pin, ssm, ssa, osc,
    ld, lo, hs, hr, bsend, brecv, bhs, bhr, dsend, drecv, s1, r1, s2, r2, zs, zr,
):
    me, z = lax.axis_index("seq"), lax.axis_index("tp")
    core, chip = lax.rem(me, 2), lax.div(me, 2)

    def remote(src, dst, ss, rs, seq=None, tp=None):
        where = {"seq": me if seq is None else seq, "tp": z if tp is None else tp}
        return pltpu.make_async_remote_copy(
            src_ref=src, dst_ref=dst, send_sem=ss, recv_sem=rs, device_id=where, device_id_type=MESH
        )

    small = [
        pltpu.make_async_copy(src, dst, ld.at[9 + n])
        for n, (src, dst) in enumerate(
            [(vconv, cv), (bconv, bcv), (sbias, sb), (lrate, lr), (gain, gn)]
        )
    ]
    load_b = pltpu.make_async_copy(bw, bwv, ld.at[0])
    load_s = pltpu.make_async_copy(sw, swv, ld.at[1])
    load_v0 = pltpu.make_async_copy(vw.at[:, 0:128], w.at[:, 128:256], ld.at[2])
    load_v1 = pltpu.make_async_copy(vw.at[:, 128:CI], w.at[:, 256:768], ld.at[7])
    load_g = pltpu.make_async_copy(gw, w.at[:, 768:1408], ld.at[8])

    def load_h(i):
        s, h = i // 2, i % 2
        return pltpu.make_async_copy(
            hid.at[s, pl.ds(256 * h, 256)], hx.at[s, pl.ds(PAD + 256 * h, 256)], ld.at[3 + i]
        )

    for copy in small:
        copy.start()
    load_b.start()
    load_s.start()
    load_v0.start()
    for i in range(4):
        load_h(i).start()
    load_g.start()
    load_v1.start()

    barrier = pltpu.get_barrier_semaphore()

    def greet_seq(r, _):
        pl.semaphore_signal(
            barrier, inc=1, device_id={"seq": lax.rem(me + r, NS), "tp": z}, device_id_type=MESH
        )
        return 0

    def greet_tp(r, _):
        pl.semaphore_signal(
            barrier, inc=1, device_id={"seq": me, "tp": lax.rem(z + r, NZ)}, device_id_type=MESH
        )
        return 0

    lax.fori_loop(1, NS, greet_seq, 0)
    lax.fori_loop(1, NZ, greet_tp, 0)

    row = lax.broadcasted_iota(jnp.int32, (256, CI), 0)
    col = lax.broadcasted_iota(jnp.int32, (256, CI), 1)
    ee[...] = jnp.where((row & 127) == HL + (col >> 6), 1.0, 0.0).astype(BF16)
    tri_at = lax.broadcasted_iota(jnp.int32, (Q, Q), 0) >= lax.broadcasted_iota(
        jnp.int32, (Q, Q), 1
    )
    tri = jnp.where(tri_at, 1.0, 0.0).astype(BF16)
    prm[...] = jnp.zeros((8, 128), F32)
    dsum[...] = jnp.zeros((8, 128), F32)
    w[:, 0:128] = jnp.zeros((D, 128), BF16)
    for s in range(2):
        hx[s, 0:8, :] = jnp.zeros((8, D), BF16)

    @pl.when(me == 0)
    def _():
        for s in range(2):
            hx[s, 8:16, :] = jnp.zeros((8, D), BF16)

    for copy in small:
        copy.wait()
    prm[0:1, HL : HL + HEADS] = sb[...]
    prm[1:2, HL : HL + HEADS] = lr[...]
    for k in range(4):
        for h in range(2):
            taps = bcv[k : k + 1, 128 * h : 128 * h + 128]
            tap[2 * k + h] = jnp.broadcast_to(taps, (128, 128)).T
    load_b.wait()
    w[:, 0:HL] = bwv[...]
    load_s.wait()
    w[:, HL : HL + HEADS] = swv[...]
    load_v0.wait()

    def first(i, _):
        s, h = lax.div(i, 2), lax.rem(i, 2)
        at = pl.multiple_of(256 * h, 256)
        pltpu.make_async_copy(
            hid.at[s, pl.ds(at, 256)], hx.at[s, pl.ds(PAD + at, 256)], ld.at[3 + i]
        ).wait()
        got = dot(hx[s, pl.ds(PAD + at, 256), :], w[:, 0:256])
        bs[s, pl.ds(at, 256), :] = got[:, 0:128]
        vp[s, pl.ds(PAD + at, 256), 0:128] = got[:, 128:256]
        return 0

    lax.fori_loop(0, 4, first, 0)

    def turn(s, _):
        for b in range(NB):
            got = bs[s, Q * b : Q * b + Q, :].T
            bct[s, z, :, 128 + Q * b : 128 + Q * b + Q] = got[0:32, :].astype(BF16)
        return 0

    lax.fori_loop(0, 2, turn, 0)

    pl.semaphore_wait(barrier, NS - 1 + NZ - 1)

    def bulk(s, owner, peer):
        part = bct.at[s, owner, :, 128:640]
        return remote(part, part, bsend.at[s, peer], brecv.at[s, owner], tp=peer)

    def send_bulk(n, _):
        s, r = lax.div(n, NZ - 1), 1 + lax.rem(n, NZ - 1)
        bulk(s, z, lax.rem(z + r, NZ)).start()
        return 0

    lax.fori_loop(0, 2 * (NZ - 1), send_bulk, 0)

    def halo():
        return remote(hx.at[:, 520:528], hx.at[:, 8:16], hs, hr, seq=lax.rem(me + 1, NS))

    @pl.when(me < NS - 1)
    def _():
        halo().start()

    lane = lax.broadcasted_iota(jnp.int32, (Q, 128), 1)
    is_head = (lane >= HL) & (lane < HL + HEADS)
    rate = jnp.exp(prm[1:2, :])

    def steps(s, _):
        so_far = jnp.zeros((1, 128), F32)
        halves, ahead = [], []
        for b in range(NB):
            x = bs[s, Q * b : Q * b + Q, :] + prm[0:1, :]
            size = jnp.maximum(x, 0.0) + jnp.log1p(jnp.exp(-jnp.abs(x)))
            size = jnp.where(is_head, size, 0.0)
            sums = dot(tri, split(-size * rate))
            cum = sums[:, 0:128] + sums[:, 128:256]
            total = cum[Q - 1 : Q, :]
            mid = 0.5 * total
            av[s, Q * b : Q * b + Q, :] = dot(split(size * jnp.exp(mid - cum)), ee[...])
            ev[s, Q * b : Q * b + Q, :] = dot(split(jnp.exp(cum - mid)), ee[...])
            halves.append(jnp.exp(mid))
            ahead.append(jnp.exp(so_far + mid))
            so_far = so_far + total
        rows = jnp.concatenate(halves + ahead + [jnp.zeros((8, 128), F32)], axis=0)
        rx[s] = dot(split(rows), ee[...])[0:8, :]
        dsum[pl.ds(s, 1), :] = so_far
        return 0

    lax.fori_loop(0, 2, steps, 0)

    def decay(owner, peer):
        src = dsum if owner is None else dall.at[owner]
        slot = me if owner is None else owner
        return remote(src, dall.at[slot], dsend.at[peer], drecv.at[slot], seq=peer)

    def send_decay(r, _):
        decay(None, lax.rem(me + r, NS)).start()
        return 0

    lax.fori_loop(1, NS, send_decay, 0)
    dall[me] = dsum[...]

    load_g.wait()

    def gate(s, _):
        for at, wide in ((0, 256), (256, 256), (512, 128)):
            got = dot(hx[s, PAD : PAD + LEN, :], w[:, 768 + at : 768 + at + wide])
            fg[s, :, at : at + wide] = silu(got) * ev[s, :, at : at + wide]
        return 0

    lax.fori_loop(0, 2, gate, 0)

    @pl.when(me > 0)
    def _():
        halo().wait_recv()

    both = jnp.concatenate([hx[0, 8:16, :], hx[1, 8:16, :]], axis=0)
    got = dot(both, w[:, 0:256])
    for s in range(2):
        rows = got[8 * s : 8 * s + 8, :]
        vp[s, 8:16, 0:128] = rows[:, 128:256]
        tail = jnp.concatenate([jnp.zeros((120, 128), F32), rows[:, 0:128]], axis=0).T
        bct[s, z, :, 0:128] = tail[0:32, :].astype(BF16)

    def bc_halo(owner, peer):
        part = bct.at[:, owner, :, 0:128]
        return remote(part, part, bhs.at[peer], bhr.at[owner], tp=peer)

    def send_bc_halo(r, _):
        bc_halo(z, lax.rem(z + r, NZ)).start()
        return 0

    lax.fori_loop(1, NZ, send_bc_halo, 0)

    load_v1.wait()

    def value(s, _):
        for at in (0, 256):
            vp[s, :, 128 + at : 384 + at] = dot(hx[s], w[:, 256 + at : 512 + at])
        for b in range(NB):
            for c in range(5):
                lanes = slice(128 * c, 128 * c + 128)
                rows = vp[s, 8 + Q * b : 8 + Q * b + Q + 8, lanes]
                mixed = cv[0:1, lanes] * rows[5 : 5 + Q]
                for k in range(1, 4):
                    mixed = mixed + cv[k : k + 1, lanes] * rows[5 + k : 5 + k + Q]
                here = (s, slice(Q * b, Q * b + Q), lanes)
                vv[here] = (silu(mixed) * av[here]).astype(BF16)
        return 0

    lax.fori_loop(0, 2, value, 0)

    def wait_bc_halo(r, _):
        peer = lax.rem(z + r, NZ)
        bc_halo(peer, peer).wait_recv()
        return 0

    lax.fori_loop(1, NZ, wait_bc_halo, 0)

    def first_hop(source, k, s):
        owner = 2 * k + s
        return remote(st.at[s, k], p1.at[source], s1.at[owner], r1.at[source], seq=owner)

    def states(s, _):
        def wait_bulk(r, _):
            peer = lax.rem(z + r, NZ)
            bulk(s, peer, peer).wait_recv()
            return 0

        lax.fori_loop(1, NZ, wait_bulk, 0)
        for h in range(2):
            x = bct[s, 4 * h : 4 * h + 4].astype(F32).reshape(128, 640)
            turned = [pltpu.roll(x, 3 - k, 1) for k in range(3)] + [x]
            for b in range(NB):
                lanes = slice(128 + Q * b, 256 + Q * b)
                mixed = tap[h] * turned[0][:, lanes]
                for k in range(1, 4):
                    mixed = mixed + tap[2 * k + h] * turned[k][:, lanes]
                mixed = silu(mixed)
                if h == 0:
                    bmat[s, :, Q * b : Q * b + Q] = mixed.astype(BF16)
                else:
                    cmat[s, Q * b : Q * b + Q, :] = mixed.T.astype(BF16)
        state = None
        for b in range(NB):
            half = rx[s, b : b + 1, :]
            added = dot(bmat[s, :, Q * b : Q * b + Q], vv[s, Q * b : Q * b + Q, :]) * half
            if state is None:
                sbl[s, b] = jnp.zeros((128, CI), BF16)
                state = added
            else:
                lifted = state * half
                sbl[s, b] = lifted.astype(BF16)
                state = lifted * half + added
        for k in range(16):
            st[s, k] = state[8 * k : 8 * k + 8, :].astype(BF16)

        def send(r, _):
            k = lax.rem(chip + r, 16)

            @pl.when(2 * k + s != me)
            def _():
                first_hop(me, k, s).start()

            return 0

        lax.fori_loop(0, 16, send, 0)
        return 0

    lax.fori_loop(0, 2, states, 0)
    p1[me] = st[core, chip]

    def within(s, _):
        for b in range(NB):
            rows = slice(Q * b, Q * b + Q)
            c_rows = cmat[s, rows, :]
            scores = dot(c_rows, bmat[s, :, rows])
            scores = jnp.where(tri_at, scores, 0.0).astype(BF16)
            left = jnp.concatenate([scores, c_rows], axis=1)
            right = jnp.concatenate([vv[s, rows, :], sbl[s, b]], axis=0)
            g[s, rows, :] = dot(left, right)
        return 0

    lax.fori_loop(0, 2, within, 0)

    def wait_decay(r, _):
        source = lax.rem(me + r, NS)
        decay(source, source).wait_recv()
        return 0

    lax.fori_loop(1, NS, wait_decay, 0)

    def pick(j, _):
        dxl[pl.ds(j, 1), :] = dall[j, pl.ds(core, 1), :]
        return 0

    lax.fori_loop(0, NS, pick, 0)
    dx[...] = dot(split(jnp.exp(dxl[...])), ee[...])

    def wait_first(r, _):
        source = lax.rem(me + r, NS)
        first_hop(source, chip, core).wait_recv()
        return 0

    lax.fori_loop(1, NS, wait_first, 0)

    def scan(j, so_far):
        po[j] = so_far.astype(BF16)
        return so_far * dx[pl.ds(j, 1), :] + p1[j].astype(F32)

    lax.fori_loop(0, NS, scan, jnp.zeros((8, CI), F32))

    def second_hop(target, source):
        slot = pin.at[lax.rem(source, 2), lax.div(source, 2)]
        return remote(po.at[target], slot, s2.at[target], r2.at[source], seq=target)

    def send_second(r, _):
        second_hop(lax.rem(me + r, NS), me).start()
        return 0

    lax.fori_loop(1, NS, send_second, 0)
    pin[core, chip] = po[me]

    ones = jnp.ones((16, CI), BF16)
    at_row = lax.broadcasted_iota(jnp.int32, (8, 128), 0)

    def finish(s, squares):
        def wait_second(k, _):
            source = 2 * k + s

            @pl.when(source != me)
            def _():
                second_hop(source, source).wait_recv()

            return 0

        lax.fori_loop(0, 16, wait_second, 0)
        arrived = pin[s].astype(F32).reshape(128, CI)
        for b in range(NB):
            rows = slice(Q * b, Q * b + Q)
            scaled = (arrived * rx[s, 4 + b : 5 + b, :]).astype(BF16)
            gated = fg[s, rows, :] * (g[s, rows, :] + dot(cmat[s, rows, :], scaled))
            g[s, rows, :] = gated
            sq = (gated * gated).astype(BF16)
            summed = lax.dot_general(
                ones, sq, (((1,), (1,)), ((), ())), preferred_element_type=F32
            )[0:8, :]
            squares = jnp.where(at_row == 4 * s + b, summed, squares)
        return squares

    ssm[...] = lax.fori_loop(0, 2, finish, jnp.zeros((8, 128), F32))

    def total_sq(owner, peer):
        return remote(ssm, ssa.at[owner], zs.at[peer], zr.at[owner], tp=peer)

    def send_sq(r, _):
        total_sq(z, lax.rem(z + r, NZ)).start()
        return 0

    lax.fori_loop(1, NZ, send_sq, 0)
    ssa[z] = ssm[...]

    def wait_sq(r, _):
        peer = lax.rem(z + r, NZ)
        total_sq(peer, peer).wait_recv()
        return 0

    lax.fori_loop(1, NZ, wait_sq, 0)
    scale = lax.rsqrt(jnp.sum(ssa[...], axis=0) * (1.0 / DI) + EPS)
    for s in range(2):
        for b in range(NB):
            rows = slice(Q * b, Q * b + Q)
            by_token = jnp.broadcast_to(scale[4 * s + b : 4 * s + b + 1, :], (128, 128)).T
            for c in range(5):
                lanes = slice(128 * c, 128 * c + 128)
                osc[s, rows, lanes] = (g[s, rows, lanes] * by_token * gn[:, lanes]).astype(BF16)
        pltpu.make_async_copy(osc.at[s], out.at[s], lo.at[s]).start()

    def sent_tp(r, _):
        peer = lax.rem(z + r, NZ)
        bulk(0, z, peer).wait_send()
        bulk(1, z, peer).wait_send()
        bc_halo(z, peer).wait_send()
        total_sq(z, peer).wait_send()
        return 0

    lax.fori_loop(1, NZ, sent_tp, 0)

    def sent_seq(r, _):
        peer = lax.rem(me + r, NS)
        decay(None, peer).wait_send()
        first_hop(me, lax.div(peer, 2), lax.rem(peer, 2)).wait_send()
        second_hop(peer, me).wait_send()
        return 0

    lax.fori_loop(1, NS, sent_seq, 0)

    @pl.when(me < NS - 1)
    def _():
        halo().wait_send()

    for s in range(2):
        pltpu.make_async_copy(osc.at[s], out.at[s], lo.at[s]).wait()


def on_device(hid, gw, vw, bw, sw, vconv, bconv, sbias, lrate, gain):
    dma = pltpu.SemaphoreType.DMA
    vmem = pltpu.VMEM
    any_space = pl.BlockSpec(memory_space=pl.ANY)
    scratch = [
        vmem((2, PAD + LEN, D), BF16),
        vmem((D, 1408), BF16),
        vmem((D, 32), BF16),
        vmem((D, HEADS), BF16),
        vmem((4, CI), F32),
        vmem((4, 256), F32),
        vmem((1, HEADS), F32),
        vmem((1, HEADS), F32),
        vmem((1, CI), F32),
        vmem((8, 128), F32),
        vmem((8, 128, 128), F32),
        vmem((256, CI), BF16),
        vmem((2, LEN, 128), F32),
        vmem((2, PAD + LEN, CI), F32),
        vmem((2, NZ, 32, 128 + LEN), BF16),
        vmem((2, LEN, 128), BF16),
        vmem((2, 128, LEN), BF16),
        vmem((2, LEN, CI), F32),
        vmem((2, LEN, CI), F32),
        vmem((2, LEN, CI), F32),
        vmem((2, LEN, CI), F32),
        vmem((2, 8, CI), F32),
        vmem((8, 128), F32),
        vmem((NS, 8, 128), F32),
        vmem((NS, 128), F32),
        vmem((NS, CI), F32),
        vmem((2, LEN, CI), BF16),
        vmem((2, NB, 128, CI), BF16),
        vmem((2, 16, 8, CI), BF16),
        vmem((NS, 8, CI), BF16),
        vmem((NS, 8, CI), BF16),
        vmem((2, 16, 8, CI), BF16),
        vmem((8, 128), F32),
        vmem((NZ, 8, 128), F32),
        vmem((2, LEN, CI), BF16),
        dma((14,)),
        dma((2,)),
        dma,
        dma,
        dma((2, NZ)),
        dma((2, NZ)),
        dma((NZ,)),
        dma((NZ,)),
        dma((NS,)),
        dma((NS,)),
        dma((NS,)),
        dma((NS,)),
        dma((NS,)),
        dma((NS,)),
        dma((NZ,)),
        dma((NZ,)),
    ]
    return pl.pallas_call(
        kernel,
        out_shape=jax.ShapeDtypeStruct((2, LEN, CI), BF16),
        in_specs=[any_space] * 10,
        out_specs=any_space,
        scratch_shapes=scratch,
        compiler_params=pltpu.CompilerParams(
            collective_id=0, has_side_effects=True, vmem_limit_bytes=56 * 2**20
        ),
    )(
        hid, gw, vw, bw, sw, vconv, bconv,
        sbias.reshape(1, HEADS), lrate.reshape(1, HEADS), gain.reshape(1, CI),
    )


def solution(mesh):
    placed = (
        P(None, "seq", None),
        P(None, "tp"),
        P(None, "tp"),
        P(None, "tp"),
        P(None, "tp"),
        P(None, "tp"),
        P(),
        P("tp"),
        P("tp"),
        P("tp"),
    )
    return jax.shard_map(
        on_device, mesh=mesh, in_specs=placed, out_specs=P(None, "seq", "tp"), check_vma=False
    )
```

```python
import jax
import jax.numpy as jnp
from jax import lax
from jax.experimental import pallas as pl
from jax.experimental.pallas import tpu as pltpu
from jax.sharding import PartitionSpec as P

MESH = pl.DeviceIdType.MESH
F32, BF16 = jnp.float32, jnp.bfloat16

NS, NZ = 32, 8
D, DI = 2560, 5120
CI = 640
LEN = 512
Q = 128
NB = LEN // Q
PAD = 16
HL = 32
HEADS = 10
EPS = 1e-05


def dot(a, b):
    return jnp.dot(a, b, preferred_element_type=F32)


def silu(x):
    half = 0.5 * x
    return half + half * jnp.tanh(half)


def split(x):
    high = x.astype(BF16)
    low = (x - high.astype(F32)).astype(BF16)
    return jnp.concatenate([high, low], axis=1)


def kernel(
    hid, gw, vw, bw, sw, vconv, bconv, sbias, lrate, gain, out,
    hx, w, bwv, swv, cv, bcv, sb, lr, gn, prm, tap, ee, bs, vp, bct, cmat, bmat,
    av, ev, fg, g, rx, dsum, dall, dxl, dx, bhl, vv, sbl, st, p1, po, pin, ssm, ssa, osc,
    ld, lo, hs, hr, bsend, brecv, dsend, drecv, s1, r1, s2, r2, zs, zr,
):
    me, z = lax.axis_index("seq"), lax.axis_index("tp")
    core, chip = me & 1, lax.div(me, 2)

    def remote(src, dst, ss, rs, seq=None, tp=None):
        where = {"seq": me if seq is None else seq, "tp": z if tp is None else tp}
        return pltpu.make_async_remote_copy(
            src_ref=src, dst_ref=dst, send_sem=ss, recv_sem=rs, device_id=where, device_id_type=MESH
        )

    small = [
        pltpu.make_async_copy(src, dst, ld.at[9 + n])
        for n, (src, dst) in enumerate(
            [(vconv, cv), (bconv, bcv), (sbias, sb), (lrate, lr), (gain, gn)]
        )
    ]
    load_b = pltpu.make_async_copy(bw, bwv, ld.at[0])
    load_s = pltpu.make_async_copy(sw, swv, ld.at[1])
    load_v0 = pltpu.make_async_copy(vw.at[:, 0:128], w.at[:, 128:256], ld.at[2])
    load_v1 = pltpu.make_async_copy(vw.at[:, 128:CI], w.at[:, 256:768], ld.at[7])
    load_g = pltpu.make_async_copy(gw, w.at[:, 768:1408], ld.at[8])

    def load_h(i):
        s, h = i // 2, i % 2
        return pltpu.make_async_copy(
            hid.at[s, pl.ds(256 * h, 256)], hx.at[s, pl.ds(PAD + 256 * h, 256)], ld.at[3 + i]
        )

    load_b.start()
    load_s.start()
    for copy in small:
        copy.start()
    load_v0.start()
    for i in range(4):
        load_h(i).start()
    load_v1.start()
    load_g.start()

    barrier = pltpu.get_barrier_semaphore()

    def greet_seq(r, _):
        pl.semaphore_signal(
            barrier, inc=1, device_id={"seq": (me + r) & (NS - 1), "tp": z}, device_id_type=MESH
        )
        return 0

    def greet_tp(r, _):
        pl.semaphore_signal(
            barrier, inc=1, device_id={"seq": me, "tp": (z + r) & (NZ - 1)}, device_id_type=MESH
        )
        return 0

    lax.fori_loop(1, NS, greet_seq, 0)
    lax.fori_loop(1, NZ, greet_tp, 0)

    row = lax.broadcasted_iota(jnp.int32, (256, CI), 0)
    col = lax.broadcasted_iota(jnp.int32, (256, CI), 1)
    ee[...] = jnp.where((row & 127) == HL + (col >> 6), 1.0, 0.0).astype(BF16)
    tri_at = lax.broadcasted_iota(jnp.int32, (Q, Q), 0) >= lax.broadcasted_iota(
        jnp.int32, (Q, Q), 1
    )
    tri = jnp.where(tri_at, 1.0, 0.0).astype(BF16)
    prm[...] = jnp.zeros((8, 128), F32)
    dsum[...] = jnp.zeros((8, 128), F32)
    for s in range(2):
        hx[s, 0:8, :] = jnp.zeros((8, D), BF16)

    @pl.when(me == 0)
    def _():
        for s in range(2):
            hx[s, 8:16, :] = jnp.zeros((8, D), BF16)

    for copy in small:
        copy.wait()
    prm[0:1, HL : HL + HEADS] = sb[...]
    prm[1:2, HL : HL + HEADS] = lr[...]
    for k in range(4):
        for h in range(2):
            taps = bcv[k : k + 1, 128 * h : 128 * h + 128]
            tap[2 * k + h] = jnp.broadcast_to(taps, (128, 128)).T
    load_b.wait()
    load_s.wait()
    for n in range(D // 128):
        lanes = slice(128 * n, 128 * n + 128)
        both = jnp.concatenate(
            [bwv[:, lanes].astype(F32), swv[:, lanes].astype(F32), jnp.zeros((86, 128), F32)], axis=0
        )
        w[lanes, 0:128] = both.T.astype(BF16)
    load_v0.wait()

    def first(s):
        for h in range(2):
            load_h(2 * s + h).wait()
            at = 256 * h
            got = dot(hx[s, PAD + at : PAD + at + 256, :], w[:, 0:256])
            bs[s, at : at + 256, :] = got[:, 0:128]
            vp[s, 0, PAD + at : PAD + at + 256, :] = got[:, 128:256]
        for b in range(NB):
            turned = bs[s, Q * b : Q * b + Q, :].T
            bct[s, z, :, Q * b : Q * b + Q] = turned[0:32, :].astype(BF16)

    def piece(p, owner, peer, n):
        part = bct.at[p, owner] if p < 2 else bhl.at[owner]
        return remote(part, part, bsend.at[p, n], brecv.at[p, owner], tp=peer)

    def away(n):
        return (z + n) & (NZ - 1)

    near = ((2, 0), (-2, 1), (1, 2), (-1, 3))

    def passed_on(p):
        turns = [(-2, 1, 4), (2, -1, 5)]
        return turns + [(-2, 2, 6) if p != 1 else (2, -2, 6)]

    def send_piece(p):
        for step, n in near:
            piece(p, z, away(step), n).start()

    def pass_piece(p):
        for step in (-2, 2):
            piece(p, away(step), away(step), 0).wait_recv()
        for owner, target, n in passed_on(p):
            piece(p, away(owner), away(target), n).start()

    def rest_of_piece(p):
        for step in (-1, 1, -3, 3, 4):
            piece(p, away(step), away(step), 0).wait_recv()

    first(0)
    pl.semaphore_wait(barrier, NS - 1 + NZ - 1)
    send_piece(0)
    first(1)
    send_piece(1)

    def halo():
        return remote(hx.at[:, 520:528], hx.at[:, 8:16], hs, hr, seq=(me + 1) & (NS - 1))

    @pl.when(me < NS - 1)
    def _():
        halo().start()

    lane = lax.broadcasted_iota(jnp.int32, (LEN, 128), 1)
    is_head = (lane >= HL) & (lane < HL + HEADS)
    rate = jnp.exp(prm[1:2, :])

    def steps(s):
        x = bs[s] + prm[0:1, :]
        size = jnp.maximum(x, 0.0) + jnp.log1p(jnp.exp(-jnp.abs(x)))
        size = jnp.where(is_head, size, 0.0)
        parts = split(-size * rate)
        so_far = jnp.zeros((1, 128), F32)
        halves, ahead, off = [], [], []
        for b in range(NB):
            sums = dot(tri, parts[Q * b : Q * b + Q, :])
            cum = sums[:, 0:128] + sums[:, 128:256]
            total = cum[Q - 1 : Q, :]
            mid = 0.5 * total
            off.append(cum - mid)
            halves.append(jnp.exp(mid))
            ahead.append(jnp.exp(so_far + mid))
            so_far = so_far + total
        off = jnp.concatenate(off, axis=0)
        av[s] = dot(split(size * jnp.exp(-off)), ee[...])
        ev[s] = dot(split(jnp.exp(off)), ee[...])
        rows = jnp.concatenate(halves + ahead + [jnp.zeros((8, 128), F32)], axis=0)
        rx[s] = dot(split(rows), ee[...])[0:8, :]
        dsum[s : s + 1, :] = so_far

    steps(0)
    steps(1)

    y, x = lax.div(chip, 4), chip & 3
    reach = [0, 1, 2, 1]
    offsets = sorted(
        ((dy, dx) for dy in range(4) for dx in range(4)), key=lambda o: -reach[o[0]] - reach[o[1]]
    )
    chips = [(((y + dy) & 3) * 4 + ((x + dx) & 3), (dy, dx) == (0, 0)) for dy, dx in offsets]
    others = [2 * c + n for c, own in chips for n in range(2) if not own] + [me + 1 - 2 * core]

    def decay(owner, peer):
        src = dsum if owner is None else dall.at[owner]
        slot = me if owner is None else owner
        return remote(src, dall.at[slot], dsend.at[peer], drecv.at[slot], seq=peer)

    for peer in others:
        decay(None, peer).start()
    dall[me] = dsum[...]
    pass_piece(0)

    @pl.when(me > 0)
    def _():
        halo().wait_recv()

    both = jnp.concatenate([hx[0, 8:16, :], hx[1, 8:16, :]], axis=0)
    got = dot(both, w[:, 0:256])
    for s in range(2):
        vp[s, 0, 8:16, :] = got[8 * s : 8 * s + 8, 128:256]
    gap = jnp.zeros((56, 128), F32)
    tail = jnp.concatenate([gap, got[8:16, 0:128], gap, got[0:8, 0:128]], axis=0).T
    bhl[z] = tail[0:32, :].astype(BF16)
    send_piece(2)

    load_v1.wait()

    def value(s):
        for at in (0, 1):
            got = dot(hx[s], w[:, 256 + 256 * at : 512 + 256 * at])
            vp[s, 1 + 2 * at] = got[:, 0:128]
            vp[s, 2 + 2 * at] = got[:, 128:256]
        for b in range(NB):
            for c in range(5):
                lanes = slice(128 * c, 128 * c + 128)
                mixed = None
                for k in range(4):
                    at = 13 + k + Q * b
                    term = cv[k : k + 1, lanes] * vp[s, c, at : at + Q, :]
                    mixed = term if mixed is None else mixed + term
                here = (s, slice(Q * b, Q * b + Q), lanes)
                vv[here] = (silu(mixed) * av[here]).astype(BF16)

    value(0)
    pass_piece(1)
    pass_piece(2)
    value(1)

    def mix(s, h):
        ahead = bhl[4 * h : 4 * h + 4].astype(F32).reshape(128, 128)
        if s == 1:
            ahead = pltpu.roll(ahead, 64, 1)
        x = bct[s, 4 * h : 4 * h + 4].astype(F32).reshape(128, LEN)
        x = jnp.concatenate([ahead, x], axis=1)
        turned = [pltpu.roll(x, 3 - k, 1) for k in range(3)] + [x]
        blocks = []
        for b in range(NB):
            lanes = slice(128 + Q * b, 256 + Q * b)
            mixed = tap[h] * turned[0][:, lanes]
            for k in range(1, 4):
                mixed = mixed + tap[2 * k + h] * turned[k][:, lanes]
            blocks.append(silu(mixed))
        return blocks

    def first_hop(source, k, s):
        owner = 2 * k + s
        return remote(st.at[s, k], p1.at[source], s1.at[owner], r1.at[source], seq=owner)

    def states(s):
        for b, block in enumerate(mix(s, 0)):
            bmat[s, :, Q * b : Q * b + Q] = block.astype(BF16)
        state = None
        for b in range(NB):
            half = rx[s, b : b + 1, :]
            added = dot(bmat[s, :, Q * b : Q * b + Q], vv[s, Q * b : Q * b + Q, :]) * half
            if state is None:
                sbl[s, b] = jnp.zeros((128, CI), BF16)
                state = added
            else:
                lifted = state * half
                sbl[s, b] = lifted.astype(BF16)
                state = lifted * half + added
        for k in range(16):
            st[s, k] = state[8 * k : 8 * k + 8, :].astype(BF16)
        for k, own in chips:
            if own:

                @pl.when(core != s)
                def _():
                    first_hop(me, k, s).start()

            else:
                first_hop(me, k, s).start()

    rest_of_piece(2)
    for s in range(2):
        rest_of_piece(s)
        states(s)
    p1[me] = st[core, chip]

    def within(s):
        for b, block in enumerate(mix(s, 1)):
            cmat[s, Q * b : Q * b + Q, :] = block.T.astype(BF16)
        for b in range(NB):
            rows = slice(Q * b, Q * b + Q)
            c_rows = cmat[s, rows, :]
            scores = dot(c_rows, bmat[s, :, rows])
            scores = jnp.where(tri_at, scores, 0.0).astype(BF16)
            left = jnp.concatenate([scores, c_rows], axis=1)
            right = jnp.concatenate([vv[s, rows, :], sbl[s, b]], axis=0)
            g[s, rows, :] = dot(left, right)

    within(0)
    within(1)

    for peer in others:
        decay(peer, peer).wait_recv()

    def pick(j, _):
        dxl[pl.ds(j, 1), :] = dall[j, pl.ds(core, 1), :]
        return 0

    lax.fori_loop(0, NS, pick, 0, unroll=True)
    dx[...] = dot(split(jnp.exp(dxl[...])), ee[...])

    for peer in others:
        first_hop(peer, chip, core).wait_recv()
    so_far = jnp.zeros((8, CI), F32)
    for j in range(NS):
        po[j] = so_far.astype(BF16)
        so_far = so_far * dx[j : j + 1, :] + p1[j].astype(F32)

    def second_hop(target, source):
        slot = pin.at[source & 1, lax.div(source, 2)]
        return remote(po.at[target], slot, s2.at[target], r2.at[source], seq=target)

    for peer in others:
        second_hop(peer, me).start()
    pin[core, chip] = po[me]

    load_g.wait()

    def gate(s, _):
        for at, wide in ((0, 256), (256, 256), (512, 128)):
            got = dot(hx[s, PAD : PAD + LEN, :], w[:, 768 + at : 768 + at + wide])
            fg[s, :, at : at + wide] = silu(got) * ev[s, :, at : at + wide]
        return 0

    lax.fori_loop(0, 2, gate, 0)

    ones = jnp.ones((16, 128), BF16)
    at_row = lax.broadcasted_iota(jnp.int32, (8, 128), 0)
    squares = jnp.zeros((8, 128), F32)
    for peer in others:
        second_hop(peer, peer).wait_recv()
    for s in range(2):
        arrived = pin[s].astype(F32).reshape(128, CI).astype(BF16)
        given = dot(cmat[s], arrived)
        for b in range(NB):
            rows = slice(Q * b, Q * b + Q)
            gated = fg[s, rows, :] * (g[s, rows, :] + given[rows] * rx[s, 4 + b : 5 + b, :])
            g[s, rows, :] = gated
            sq = gated * gated
            sq = sum(sq[:, 128 * c : 128 * c + 128] for c in range(1, 5)) + sq[:, 0:128]
            summed = lax.dot_general(
                ones, sq.astype(BF16), (((1,), (1,)), ((), ())), preferred_element_type=F32
            )[0:8, :]
            squares = jnp.where(at_row == 4 * s + b, summed, squares)
    ssm[...] = squares

    def total_sq(owner, peer):
        return remote(ssm, ssa.at[owner], zs.at[peer], zr.at[owner], tp=peer)

    for step in (4, 3, -3, 2, -2, 1, -1):
        total_sq(z, away(step)).start()
    ssa[z] = ssm[...]
    for step in (4, 3, -3, 2, -2, 1, -1):
        total_sq(away(step), away(step)).wait_recv()
    scale = lax.rsqrt(jnp.sum(ssa[...], axis=0) * (1.0 / DI) + EPS)
    gains = gn[...].reshape(1, CI)
    for s in range(2):
        for b in range(NB):
            rows = slice(Q * b, Q * b + Q)
            by_token = jnp.broadcast_to(scale[4 * s + b : 4 * s + b + 1, :], (128, 128)).T
            for c in range(5):
                lanes = slice(128 * c, 128 * c + 128)
                osc[s, rows, lanes] = (g[s, rows, lanes] * by_token * gains[:, lanes]).astype(BF16)
        pltpu.make_async_copy(osc.at[s], out.at[s], lo.at[s]).start()

    for p in range(3):
        for step, n in near:
            piece(p, z, away(step), n).wait_send()
        for owner, target, n in passed_on(p):
            piece(p, away(owner), away(target), n).wait_send()
    for step in range(1, NZ):
        total_sq(z, away(step)).wait_send()

    def sent_seq(r, _):
        peer = (me + r) & (NS - 1)
        decay(None, peer).wait_send()
        first_hop(me, lax.div(peer, 2), peer & 1).wait_send()
        second_hop(peer, me).wait_send()
        return 0

    lax.fori_loop(1, NS, sent_seq, 0)
    @pl.when(me < NS - 1)
    def _():
        halo().wait_send()

    for s in range(2):
        pltpu.make_async_copy(osc.at[s], out.at[s], lo.at[s]).wait()


def on_device(hid, gw, vw, bw, sw, vconv, bconv, sbias, lrate, gain):
    dma = pltpu.SemaphoreType.DMA
    vmem = pltpu.VMEM
    any_space = pl.BlockSpec(memory_space=pl.ANY)
    scratch = [
        vmem((2, PAD + LEN, D), BF16),
        vmem((D, 1408), BF16),
        vmem((32, D), BF16),
        vmem((HEADS, D), BF16),
        vmem((4, CI), F32),
        vmem((4, 256), F32),
        vmem((1, HEADS), F32),
        vmem((1, HEADS), F32),
        vmem((CI,), F32),
        vmem((8, 128), F32),
        vmem((8, 128, 128), F32),
        vmem((256, CI), BF16),
        vmem((2, LEN, 128), F32),
        vmem((2, 5, PAD + LEN, 128), F32),
        vmem((2, NZ, 32, LEN), BF16),
        vmem((2, LEN, 128), BF16),
        vmem((2, 128, LEN), BF16),
        vmem((2, LEN, CI), F32),
        vmem((2, LEN, CI), F32),
        vmem((2, LEN, CI), F32),
        vmem((2, LEN, CI), F32),
        vmem((2, 8, CI), F32),
        vmem((8, 128), F32),
        vmem((NS, 8, 128), F32),
        vmem((NS, 128), F32),
        vmem((NS, CI), F32),
        vmem((NZ, 32, 128), BF16),
        vmem((2, LEN, CI), BF16),
        vmem((2, NB, 128, CI), BF16),
        vmem((2, 16, 8, CI), BF16),
        vmem((NS, 8, CI), BF16),
        vmem((NS, 8, CI), BF16),
        vmem((2, 16, 8, CI), BF16),
        vmem((8, 128), F32),
        vmem((NZ, 8, 128), F32),
        vmem((2, LEN, CI), BF16),
        dma((14,)),
        dma((2,)),
        dma,
        dma,
        dma((3, 7)),
        dma((3, NZ)),
        dma((NS,)),
        dma((NS,)),
        dma((NS,)),
        dma((NS,)),
        dma((NS,)),
        dma((NS,)),
        dma((NZ,)),
        dma((NZ,)),
    ]
    return pl.pallas_call(
        kernel,
        out_shape=jax.ShapeDtypeStruct((2, LEN, CI), BF16),
        in_specs=[any_space] * 10,
        out_specs=any_space,
        scratch_shapes=scratch,
        compiler_params=pltpu.CompilerParams(
            collective_id=0, has_side_effects=True, vmem_limit_bytes=56 * 2**20
        ),
    )(
        hid, gw, vw, bw.T, sw.T, vconv, bconv,
        sbias.reshape(1, HEADS), lrate.reshape(1, HEADS), gain,
    )


def solution(mesh):
    placed = (
        P(None, "seq", None),
        P(None, "tp"),
        P(None, "tp"),
        P(None, "tp"),
        P(None, "tp"),
        P(None, "tp"),
        P(),
        P("tp"),
        P("tp"),
        P("tp"),
    )
    return jax.shard_map(
        on_device, mesh=mesh, in_specs=placed, out_specs=P(None, "seq", "tp"), check_vma=False
    )
```

```python
import jax
import jax.numpy as jnp
from jax import lax
from jax.experimental import pallas as pl
from jax.experimental.pallas import tpu as pltpu
from jax.sharding import PartitionSpec as P

MESH = pl.DeviceIdType.MESH
F32, BF16 = jnp.float32, jnp.bfloat16

NS, NZ = 32, 8
D, DI = 2560, 5120
CI = 640
LEN = 512
Q = 128
NB = LEN // Q
PAD = 16
HL = 32
HEADS = 10
EPS = 1e-05


def dot(a, b):
    return jnp.dot(a, b, preferred_element_type=F32)


def silu(x):
    half = 0.5 * x
    return half + half * jnp.tanh(half)


def split(x):
    high = x.astype(BF16)
    low = (x - high.astype(F32)).astype(BF16)
    return jnp.concatenate([high, low], axis=1)


def kernel(
    hid, gw, vw, bw, sw, vconv, bconv, sbias, lrate, gain, out, rms,
    hx, w, bwv, swv, cv, bcv, sb, lr, gn, prm, tap, ee, bs, vp, bct, cmat, bmat,
    av, ev, fg, g, rx, dsum, dall, dxl, dx, bhl, vv, sbl, st, p1, po, pin, ssm, ssa,
    ld, hs, hr, bsend, brecv, dsend, drecv, s1, r1, s2, r2, zs, zr,
):
    me, z = lax.axis_index("seq"), lax.axis_index("tp")
    core, chip = me & 1, lax.div(me, 2)

    def remote(src, dst, ss, rs, seq=None, tp=None):
        where = {"seq": me if seq is None else seq, "tp": z if tp is None else tp}
        return pltpu.make_async_remote_copy(
            src_ref=src, dst_ref=dst, send_sem=ss, recv_sem=rs, device_id=where, device_id_type=MESH
        )

    small = [
        pltpu.make_async_copy(src, dst, ld.at[9 + n])
        for n, (src, dst) in enumerate(
            [(vconv, cv), (bconv, bcv), (sbias, sb), (lrate, lr), (gain, gn)]
        )
    ]
    load_b = pltpu.make_async_copy(bw, bwv, ld.at[0])
    load_s = pltpu.make_async_copy(sw, swv, ld.at[1])
    load_v0 = pltpu.make_async_copy(vw.at[:, 0:128], w.at[:, 128:256], ld.at[2])
    load_v1 = pltpu.make_async_copy(vw.at[:, 128:CI], w.at[:, 256:768], ld.at[7])
    load_g = pltpu.make_async_copy(gw, w.at[:, 768:1408], ld.at[8])

    def load_h(i):
        s, h = i // 2, i % 2
        return pltpu.make_async_copy(
            hid.at[s, pl.ds(256 * h, 256)], hx.at[s, pl.ds(PAD + 256 * h, 256)], ld.at[3 + i]
        )

    load_b.start()
    load_s.start()
    for copy in small:
        copy.start()
    load_v0.start()
    for i in range(4):
        load_h(i).start()
    load_v1.start()
    load_g.start()

    barrier = pltpu.get_barrier_semaphore()

    def greet_seq(r, _):
        pl.semaphore_signal(
            barrier, inc=1, device_id={"seq": (me + r) & (NS - 1), "tp": z}, device_id_type=MESH
        )
        return 0

    def greet_tp(r, _):
        pl.semaphore_signal(
            barrier, inc=1, device_id={"seq": me, "tp": (z + r) & (NZ - 1)}, device_id_type=MESH
        )
        return 0

    lax.fori_loop(1, NS, greet_seq, 0)
    lax.fori_loop(1, NZ, greet_tp, 0)

    row = lax.broadcasted_iota(jnp.int32, (256, CI), 0)
    col = lax.broadcasted_iota(jnp.int32, (256, CI), 1)
    ee[...] = jnp.where((row & 127) == HL + (col >> 6), 1.0, 0.0).astype(BF16)
    tri_at = lax.broadcasted_iota(jnp.int32, (Q, Q), 0) >= lax.broadcasted_iota(
        jnp.int32, (Q, Q), 1
    )
    tri = jnp.where(tri_at, 1.0, 0.0).astype(BF16)
    prm[...] = jnp.zeros((8, 128), F32)
    dsum[...] = jnp.zeros((8, 128), F32)
    for s in range(2):
        hx[s, 0:8, :] = jnp.zeros((8, D), BF16)

    @pl.when(me == 0)
    def _():
        for s in range(2):
            hx[s, 8:16, :] = jnp.zeros((8, D), BF16)

    for copy in small:
        copy.wait()
    prm[0:1, HL : HL + HEADS] = sb[...]
    prm[1:2, HL : HL + HEADS] = lr[...]
    for k in range(4):
        for h in range(2):
            taps = bcv[k : k + 1, 128 * h : 128 * h + 128]
            tap[2 * k + h] = jnp.broadcast_to(taps, (128, 128)).T
    load_b.wait()
    load_s.wait()
    for n in range(D // 128):
        lanes = slice(128 * n, 128 * n + 128)
        both = jnp.concatenate(
            [bwv[:, lanes].astype(F32), swv[:, lanes].astype(F32), jnp.zeros((86, 128), F32)], axis=0
        )
        w[lanes, 0:128] = both.T.astype(BF16)
    load_v0.wait()

    def first(s):
        for h in range(2):
            load_h(2 * s + h).wait()
            at = 256 * h
            got = dot(hx[s, PAD + at : PAD + at + 256, :], w[:, 0:256])
            bs[s, at : at + 256, :] = got[:, 0:128]
            vp[s, 0, PAD + at : PAD + at + 256, :] = got[:, 128:256]
        for b in range(NB):
            turned = bs[s, Q * b : Q * b + Q, :].T
            bct[s, z, :, Q * b : Q * b + Q] = turned[0:32, :].astype(BF16)

    def piece(p, owner, peer, n):
        part = bct.at[p, owner] if p < 2 else bhl.at[owner]
        return remote(part, part, bsend.at[p, n], brecv.at[p, owner], tp=peer)

    def away(n):
        return (z + n) & (NZ - 1)

    near = ((2, 0), (-2, 1), (1, 2), (-1, 3))

    def passed_on(p):
        turns = [(-2, 1, 4), (2, -1, 5)]
        return turns + [(-2, 2, 6) if p != 1 else (2, -2, 6)]

    def send_piece(p):
        for step, n in near:
            piece(p, z, away(step), n).start()

    def pass_piece(p):
        for step in (-2, 2):
            piece(p, away(step), away(step), 0).wait_recv()
        for owner, target, n in passed_on(p):
            piece(p, away(owner), away(target), n).start()

    def rest_of_piece(p):
        for step in (-1, 1, -3, 3, 4):
            piece(p, away(step), away(step), 0).wait_recv()

    first(0)
    pl.semaphore_wait(barrier, NS - 1 + NZ - 1)
    send_piece(0)
    first(1)
    send_piece(1)

    def halo():
        return remote(hx.at[:, 520:528], hx.at[:, 8:16], hs, hr, seq=(me + 1) & (NS - 1))

    @pl.when(me < NS - 1)
    def _():
        halo().start()

    lane = lax.broadcasted_iota(jnp.int32, (LEN, 128), 1)
    is_head = (lane >= HL) & (lane < HL + HEADS)
    rate = jnp.exp(prm[1:2, :])

    def steps(s):
        x = bs[s] + prm[0:1, :]
        size = jnp.maximum(x, 0.0) + jnp.log1p(jnp.exp(-jnp.abs(x)))
        size = jnp.where(is_head, size, 0.0)
        parts = split(-size * rate)
        so_far = jnp.zeros((1, 128), F32)
        halves, ahead, off = [], [], []
        for b in range(NB):
            sums = dot(tri, parts[Q * b : Q * b + Q, :])
            cum = sums[:, 0:128] + sums[:, 128:256]
            total = cum[Q - 1 : Q, :]
            mid = 0.5 * total
            off.append(cum - mid)
            halves.append(jnp.exp(mid))
            ahead.append(jnp.exp(so_far + mid))
            so_far = so_far + total
        off = jnp.concatenate(off, axis=0)
        av[s] = dot(split(size * jnp.exp(-off)), ee[...])
        ev[s] = dot(split(jnp.exp(off)), ee[...])
        rows = jnp.concatenate(halves + ahead + [jnp.zeros((8, 128), F32)], axis=0)
        rx[s] = dot(split(rows), ee[...])[0:8, :]
        dsum[s : s + 1, :] = so_far

    steps(0)
    steps(1)

    y, x = lax.div(chip, 4), chip & 3
    reach = [0, 1, 2, 1]
    offsets = sorted(
        ((dy, dx) for dy in range(4) for dx in range(4)), key=lambda o: -reach[o[0]] - reach[o[1]]
    )
    chips = [(((y + dy) & 3) * 4 + ((x + dx) & 3), (dy, dx) == (0, 0)) for dy, dx in offsets]
    others = [2 * c + n for c, own in chips for n in range(2) if not own] + [me + 1 - 2 * core]

    def decay(owner, peer):
        src = dsum if owner is None else dall.at[owner]
        slot = me if owner is None else owner
        return remote(src, dall.at[slot], dsend.at[peer], drecv.at[slot], seq=peer)

    for peer in others:
        decay(None, peer).start()
    dall[me] = dsum[...]
    pass_piece(0)

    @pl.when(me > 0)
    def _():
        halo().wait_recv()

    both = jnp.concatenate([hx[0, 8:16, :], hx[1, 8:16, :]], axis=0)
    got = dot(both, w[:, 0:256])
    for s in range(2):
        vp[s, 0, 8:16, :] = got[8 * s : 8 * s + 8, 128:256]
    gap = jnp.zeros((56, 128), F32)
    tail = jnp.concatenate([gap, got[8:16, 0:128], gap, got[0:8, 0:128]], axis=0).T
    bhl[z] = tail[0:32, :].astype(BF16)
    send_piece(2)

    load_v1.wait()

    def value(s):
        for at in (0, 1):
            got = dot(hx[s], w[:, 256 + 256 * at : 512 + 256 * at])
            vp[s, 1 + 2 * at] = got[:, 0:128]
            vp[s, 2 + 2 * at] = got[:, 128:256]
        for b in range(NB):
            for c in range(5):
                lanes = slice(128 * c, 128 * c + 128)
                mixed = None
                for k in range(4):
                    at = 13 + k + Q * b
                    term = cv[k : k + 1, lanes] * vp[s, c, at : at + Q, :]
                    mixed = term if mixed is None else mixed + term
                here = (s, slice(Q * b, Q * b + Q), lanes)
                vv[here] = (silu(mixed) * av[here]).astype(BF16)

    value(0)
    pass_piece(1)
    pass_piece(2)
    value(1)

    def mix(s, h):
        ahead = bhl[4 * h : 4 * h + 4].astype(F32).reshape(128, 128)
        if s == 1:
            ahead = pltpu.roll(ahead, 64, 1)
        x = bct[s, 4 * h : 4 * h + 4].astype(F32).reshape(128, LEN)
        x = jnp.concatenate([ahead, x], axis=1)
        turned = [pltpu.roll(x, 3 - k, 1) for k in range(3)] + [x]
        blocks = []
        for b in range(NB):
            lanes = slice(128 + Q * b, 256 + Q * b)
            mixed = tap[h] * turned[0][:, lanes]
            for k in range(1, 4):
                mixed = mixed + tap[2 * k + h] * turned[k][:, lanes]
            blocks.append(silu(mixed))
        return blocks

    def first_hop(source, k, s):
        owner = 2 * k + s
        return remote(st.at[s, k], p1.at[source], s1.at[owner], r1.at[source], seq=owner)

    def states(s):
        for b, block in enumerate(mix(s, 0)):
            bmat[s, :, Q * b : Q * b + Q] = block.astype(BF16)
        state = None
        for b in range(NB):
            half = rx[s, b : b + 1, :]
            added = dot(bmat[s, :, Q * b : Q * b + Q], vv[s, Q * b : Q * b + Q, :]) * half
            if state is None:
                sbl[s, b] = jnp.zeros((128, CI), BF16)
                state = added
            else:
                lifted = state * half
                sbl[s, b] = lifted.astype(BF16)
                state = lifted * half + added
        for k in range(16):
            st[s, k] = state[8 * k : 8 * k + 8, :].astype(BF16)
        for k, own in chips:
            if own:

                @pl.when(core != s)
                def _():
                    first_hop(me, k, s).start()

            else:
                first_hop(me, k, s).start()

    rest_of_piece(2)
    for s in range(2):
        rest_of_piece(s)
        states(s)
    p1[me] = st[core, chip]

    def within(s):
        for b, block in enumerate(mix(s, 1)):
            cmat[s, Q * b : Q * b + Q, :] = block.T.astype(BF16)
        for b in range(NB):
            rows = slice(Q * b, Q * b + Q)
            c_rows = cmat[s, rows, :]
            scores = dot(c_rows, bmat[s, :, rows])
            scores = jnp.where(tri_at, scores, 0.0).astype(BF16)
            left = jnp.concatenate([scores, c_rows], axis=1)
            right = jnp.concatenate([vv[s, rows, :], sbl[s, b]], axis=0)
            g[s, rows, :] = dot(left, right)

    within(0)
    within(1)

    for peer in others:
        decay(peer, peer).wait_recv()

    def pick(j, _):
        dxl[pl.ds(j, 1), :] = dall[j, pl.ds(core, 1), :]
        return 0

    lax.fori_loop(0, NS, pick, 0, unroll=True)
    dx[...] = dot(split(jnp.exp(dxl[...])), ee[...])

    for peer in others:
        first_hop(peer, chip, core).wait_recv()
    so_far = jnp.zeros((8, CI), F32)
    for j in range(NS):
        po[j] = so_far.astype(BF16)
        so_far = so_far * dx[j : j + 1, :] + p1[j].astype(F32)

    def second_hop(target, source):
        slot = pin.at[source & 1, lax.div(source, 2)]
        return remote(po.at[target], slot, s2.at[target], r2.at[source], seq=target)

    for peer in others:
        second_hop(peer, me).start()
    pin[core, chip] = po[me]

    load_g.wait()

    def gate(s, _):
        for at, wide in ((0, 256), (256, 256), (512, 128)):
            got = dot(hx[s, PAD : PAD + LEN, :], w[:, 768 + at : 768 + at + wide])
            fg[s, :, at : at + wide] = silu(got) * ev[s, :, at : at + wide]
        return 0

    lax.fori_loop(0, 2, gate, 0)

    ones = jnp.ones((16, 128), BF16)
    at_row = lax.broadcasted_iota(jnp.int32, (8, 128), 0)
    squares = jnp.zeros((8, 128), F32)
    for peer in others:
        second_hop(peer, peer).wait_recv()
    for s in range(2):
        arrived = pin[s].astype(F32).reshape(128, CI).astype(BF16)
        given = dot(cmat[s], arrived)
        for b in range(NB):
            rows = slice(Q * b, Q * b + Q)
            gated = fg[s, rows, :] * (g[s, rows, :] + given[rows] * rx[s, 4 + b : 5 + b, :])
            g[s, rows, :] = gated
            sq = gated * gated
            sq = sum(sq[:, 128 * c : 128 * c + 128] for c in range(1, 5)) + sq[:, 0:128]
            summed = lax.dot_general(
                ones, sq.astype(BF16), (((1,), (1,)), ((), ())), preferred_element_type=F32
            )[0:8, :]
            squares = jnp.where(at_row == 4 * s + b, summed, squares)
    ssm[...] = squares

    def total_sq(owner, peer):
        return remote(ssm, ssa.at[owner], zs.at[peer], zr.at[owner], tp=peer)

    for step in (4, 3, -3, 2, -2, 1, -1):
        total_sq(z, away(step)).start()
    ssa[z] = ssm[...]
    gains = gn[...].reshape(1, CI)
    for s in range(2):
        out[s] = g[s] * gains
    for step in (4, 3, -3, 2, -2, 1, -1):
        total_sq(away(step), away(step)).wait_recv()
    rms[...] = lax.rsqrt(jnp.sum(ssa[...], axis=0) * (1.0 / DI) + EPS)

    for p in range(3):
        for step, n in near:
            piece(p, z, away(step), n).wait_send()
        for owner, target, n in passed_on(p):
            piece(p, away(owner), away(target), n).wait_send()
    for step in range(1, NZ):
        total_sq(z, away(step)).wait_send()

    def sent_seq(r, _):
        peer = (me + r) & (NS - 1)
        decay(None, peer).wait_send()
        first_hop(me, lax.div(peer, 2), peer & 1).wait_send()
        second_hop(peer, me).wait_send()
        return 0

    lax.fori_loop(1, NS, sent_seq, 0)
    @pl.when(me < NS - 1)
    def _():
        halo().wait_send()


def scaled(gated, rms, out, osc, sems):
    copies = []
    for s in range(2):
        for b in range(NB):
            n = NB * s + b
            rows = slice(Q * b, Q * b + Q)
            by_token = jnp.broadcast_to(rms[n : n + 1, :], (128, 128)).T
            for c in range(5):
                lanes = slice(128 * c, 128 * c + 128)
                osc[s, rows, lanes] = (gated[s, rows, lanes] * by_token).astype(BF16)
            copies.append(pltpu.make_async_copy(osc.at[s, rows], out.at[s, rows], sems.at[n]))
            copies[-1].start()
    for copy in copies:
        copy.wait()


def on_device(hid, gw, vw, bw, sw, vconv, bconv, sbias, lrate, gain):
    dma = pltpu.SemaphoreType.DMA
    vmem = pltpu.VMEM
    any_space = pl.BlockSpec(memory_space=pl.ANY)
    scratch = [
        vmem((2, PAD + LEN, D), BF16),
        vmem((D, 1408), BF16),
        vmem((32, D), BF16),
        vmem((HEADS, D), BF16),
        vmem((4, CI), F32),
        vmem((4, 256), F32),
        vmem((1, HEADS), F32),
        vmem((1, HEADS), F32),
        vmem((CI,), F32),
        vmem((8, 128), F32),
        vmem((8, 128, 128), F32),
        vmem((256, CI), BF16),
        vmem((2, LEN, 128), F32),
        vmem((2, 5, PAD + LEN, 128), F32),
        vmem((2, NZ, 32, LEN), BF16),
        vmem((2, LEN, 128), BF16),
        vmem((2, 128, LEN), BF16),
        vmem((2, LEN, CI), F32),
        vmem((2, LEN, CI), F32),
        vmem((2, LEN, CI), F32),
        vmem((2, LEN, CI), F32),
        vmem((2, 8, CI), F32),
        vmem((8, 128), F32),
        vmem((NS, 8, 128), F32),
        vmem((NS, 128), F32),
        vmem((NS, CI), F32),
        vmem((NZ, 32, 128), BF16),
        vmem((2, LEN, CI), BF16),
        vmem((2, NB, 128, CI), BF16),
        vmem((2, 16, 8, CI), BF16),
        vmem((NS, 8, CI), BF16),
        vmem((NS, 8, CI), BF16),
        vmem((2, 16, 8, CI), BF16),
        vmem((8, 128), F32),
        vmem((NZ, 8, 128), F32),
        dma((14,)),
        dma,
        dma,
        dma((3, 7)),
        dma((3, NZ)),
        dma((NS,)),
        dma((NS,)),
        dma((NS,)),
        dma((NS,)),
        dma((NS,)),
        dma((NS,)),
        dma((NZ,)),
        dma((NZ,)),
    ]
    in_vmem = pl.BlockSpec(memory_space=vmem)
    gated, rms = pl.pallas_call(
        kernel,
        out_shape=(vmem((2, LEN, CI), F32), vmem((8, 128), F32)),
        in_specs=[any_space] * 10,
        out_specs=(in_vmem, in_vmem),
        scratch_shapes=scratch,
        compiler_params=pltpu.CompilerParams(
            collective_id=0, has_side_effects=True, vmem_limit_bytes=56 * 2**20
        ),
    )(
        hid, gw, vw, bw.T, sw.T, vconv, bconv,
        sbias.reshape(1, HEADS), lrate.reshape(1, HEADS), gain,
    )
    return pl.pallas_call(
        scaled,
        out_shape=jax.ShapeDtypeStruct((2, LEN, CI), BF16),
        in_specs=[in_vmem, in_vmem],
        out_specs=any_space,
        scratch_shapes=[vmem((2, LEN, CI), BF16), dma((2 * NB,))],
    )(*(pltpu.with_memory_space_constraint(x, vmem) for x in (gated, rms)))


def solution(mesh):
    placed = (
        P(None, "seq", None),
        P(None, "tp"),
        P(None, "tp"),
        P(None, "tp"),
        P(None, "tp"),
        P(None, "tp"),
        P(),
        P("tp"),
        P("tp"),
        P("tp"),
    )
    return jax.shard_map(
        on_device, mesh=mesh, in_specs=placed, out_specs=P(None, "seq", "tp"), check_vma=False
    )
```

```python
import jax
import jax.numpy as jnp
from jax import lax
from jax.experimental import pallas as pl
from jax.experimental.pallas import tpu as pltpu
from jax.sharding import PartitionSpec as P

MESH = pl.DeviceIdType.MESH
F32, BF16 = jnp.float32, jnp.bfloat16

NS, NZ = 32, 8
D, DI = 2560, 5120
CI = 640
LEN = 512
Q = 128
NB = LEN // Q
PAD = 16
HL = 32
HEADS = 10
EPS = 1e-05


def dot(a, b):
    return jnp.dot(a, b, preferred_element_type=F32)


def silu(x):
    half = 0.5 * x
    return half + half * jnp.tanh(half)


def split(x):
    high = x.astype(BF16)
    low = (x - high.astype(F32)).astype(BF16)
    return jnp.concatenate([high, low], axis=1)


def kernel(
    hid, gw, vw, bw, sw, vconv, bconv, sbias, lrate, gain, out, rms,
    hx, w, bwv, swv, cv, bcv, sb, lr, gn, prm, tap, ee, bs, vp, bct, cmat, bmat,
    av, ev, fg, g, rx, dsum, dall, dxl, dx, bhl, vv, sbl, st, so, agg, p1, po, pin, ssm, ssa,
    ld, hs, hr, bsend, brecv, dsend, drecv, s1, r1, s2, r2, zs, zr, cs, cr,
):
    me, z = lax.axis_index("seq"), lax.axis_index("tp")
    core, chip = me & 1, lax.div(me, 2)
    early, late = 1 - core, core

    def remote(src, dst, ss, rs, seq=None, tp=None):
        where = {"seq": me if seq is None else seq, "tp": z if tp is None else tp}
        return pltpu.make_async_remote_copy(
            src_ref=src, dst_ref=dst, send_sem=ss, recv_sem=rs, device_id=where, device_id_type=MESH
        )

    small = [
        pltpu.make_async_copy(src, dst, ld.at[9 + n])
        for n, (src, dst) in enumerate(
            [(vconv, cv), (bconv, bcv), (sbias, sb), (lrate, lr), (gain, gn)]
        )
    ]
    load_b = pltpu.make_async_copy(bw, bwv, ld.at[0])
    load_s = pltpu.make_async_copy(sw, swv, ld.at[1])
    load_v0 = pltpu.make_async_copy(vw.at[:, 0:128], w.at[:, 128:256], ld.at[2])
    load_v1 = pltpu.make_async_copy(vw.at[:, 128:CI], w.at[:, 256:768], ld.at[7])
    load_g = pltpu.make_async_copy(gw, w.at[:, 768:1408], ld.at[8])

    def load_h(s, h):
        return pltpu.make_async_copy(
            hid.at[s, pl.ds(256 * h, 256)], hx.at[s, pl.ds(PAD + 256 * h, 256)], ld.at[3 + 2 * s + h]
        )

    load_b.start()
    load_s.start()
    for copy in small:
        copy.start()
    load_v0.start()
    for s in (early, late):
        for h in range(2):
            load_h(s, h).start()
    load_v1.start()
    load_g.start()

    barrier = pltpu.get_barrier_semaphore()

    def greet_seq(r, _):
        pl.semaphore_signal(
            barrier, inc=1, device_id={"seq": (me + r) & (NS - 1), "tp": z}, device_id_type=MESH
        )
        return 0

    def greet_tp(r, _):
        pl.semaphore_signal(
            barrier, inc=1, device_id={"seq": me, "tp": (z + r) & (NZ - 1)}, device_id_type=MESH
        )
        return 0

    lax.fori_loop(1, NS, greet_seq, 0)
    lax.fori_loop(1, NZ, greet_tp, 0)

    row = lax.broadcasted_iota(jnp.int32, (256, CI), 0)
    col = lax.broadcasted_iota(jnp.int32, (256, CI), 1)
    ee[...] = jnp.where((row & 127) == HL + (col >> 6), 1.0, 0.0).astype(BF16)
    tri_at = lax.broadcasted_iota(jnp.int32, (Q, Q), 0) >= lax.broadcasted_iota(
        jnp.int32, (Q, Q), 1
    )
    tri = jnp.where(tri_at, 1.0, 0.0).astype(BF16)
    prm[...] = jnp.zeros((8, 128), F32)
    dsum[...] = jnp.zeros((8, 128), F32)
    for s in range(2):
        hx[s, 0:8, :] = jnp.zeros((8, D), BF16)

    @pl.when(me == 0)
    def _():
        for s in range(2):
            hx[s, 8:16, :] = jnp.zeros((8, D), BF16)

    for copy in small:
        copy.wait()
    prm[0:1, HL : HL + HEADS] = sb[...]
    prm[1:2, HL : HL + HEADS] = lr[...]
    for k in range(4):
        for h in range(2):
            taps = bcv[k : k + 1, 128 * h : 128 * h + 128]
            tap[2 * k + h] = jnp.broadcast_to(taps, (128, 128)).T
    load_b.wait()
    load_s.wait()
    for n in range(D // 128):
        lanes = slice(128 * n, 128 * n + 128)
        both = jnp.concatenate(
            [bwv[:, lanes].astype(F32), swv[:, lanes].astype(F32), jnp.zeros((86, 128), F32)], axis=0
        )
        w[lanes, 0:128] = both.T.astype(BF16)
    load_v0.wait()

    def first(s):
        for h in range(2):
            load_h(s, h).wait()
            at = 256 * h
            got = dot(hx[s, PAD + at : PAD + at + 256, :], w[:, 0:256])
            bs[s, at : at + 256, :] = got[:, 0:128]
            vp[s, 0, PAD + at : PAD + at + 256, :] = got[:, 128:256]
        for b in range(NB):
            turned = bs[s, Q * b : Q * b + Q, :].T
            bct[s, z, :, Q * b : Q * b + Q] = turned[0:32, :].astype(BF16)

    def piece(p, owner, peer, n):
        part = bct.at[(early, late)[p], owner] if p < 2 else bhl.at[owner]
        return remote(part, part, bsend.at[p, n], brecv.at[p, owner], tp=peer)

    def away(n):
        return (z + n) & (NZ - 1)

    near = ((2, 0), (-2, 1), (1, 2), (-1, 3))

    def passed_on(p):
        turns = [(-2, 1, 4), (2, -1, 5)]
        return turns + [(-2, 2, 6) if p != 1 else (2, -2, 6)]

    def send_piece(p):
        for step, n in near:
            piece(p, z, away(step), n).start()

    def pass_piece(p):
        for step in (-2, 2):
            piece(p, away(step), away(step), 0).wait_recv()
        for owner, target, n in passed_on(p):
            piece(p, away(owner), away(target), n).start()

    def rest_of_piece(p):
        for step in (-1, 1, -3, 3, 4):
            piece(p, away(step), away(step), 0).wait_recv()

    first(early)
    pl.semaphore_wait(barrier, NS - 1 + NZ - 1)
    send_piece(0)
    first(late)
    send_piece(1)

    def halo():
        return remote(hx.at[:, 520:528], hx.at[:, 8:16], hs, hr, seq=(me + 1) & (NS - 1))

    @pl.when(me < NS - 1)
    def _():
        halo().start()

    lane = lax.broadcasted_iota(jnp.int32, (LEN, 128), 1)
    is_head = (lane >= HL) & (lane < HL + HEADS)
    rate = jnp.exp(prm[1:2, :])

    def steps(s):
        x = bs[s] + prm[0:1, :]
        size = jnp.maximum(x, 0.0) + jnp.log1p(jnp.exp(-jnp.abs(x)))
        size = jnp.where(is_head, size, 0.0)
        parts = split(-size * rate)
        so_far = jnp.zeros((1, 128), F32)
        halves, ahead, off = [], [], []
        for b in range(NB):
            sums = dot(tri, parts[Q * b : Q * b + Q, :])
            cum = sums[:, 0:128] + sums[:, 128:256]
            total = cum[Q - 1 : Q, :]
            mid = 0.5 * total
            off.append(cum - mid)
            halves.append(jnp.exp(mid))
            ahead.append(jnp.exp(so_far + mid))
            so_far = so_far + total
        off = jnp.concatenate(off, axis=0)
        av[s] = dot(split(size * jnp.exp(-off)), ee[...])
        ev[s] = dot(split(jnp.exp(off)), ee[...])
        rows = jnp.concatenate(halves + ahead + [jnp.zeros((8, 128), F32)], axis=0)
        rx[s] = dot(split(rows), ee[...])[0:8, :]
        dsum[pl.ds(s, 1), :] = so_far

    steps(early)
    steps(late)

    y, x = lax.div(chip, 4), chip & 3
    reach = [0, 1, 2, 1]
    offsets = sorted(
        ((dy, dx) for dy in range(4) for dx in range(4)), key=lambda o: -reach[o[0]] - reach[o[1]]
    )
    chips = [(((y + dy) & 3) * 4 + ((x + dx) & 3), (dy, dx) == (0, 0)) for dy, dx in offsets]
    others = [2 * c + n for c, own in chips for n in range(2) if not own] + [me + 1 - 2 * core]

    def decay(owner, peer):
        src = dsum if owner is None else dall.at[owner]
        slot = me if owner is None else owner
        return remote(src, dall.at[slot], dsend.at[peer], drecv.at[slot], seq=peer)

    for peer in others:
        decay(None, peer).start()
    dall[me] = dsum[...]
    pass_piece(0)

    @pl.when(me > 0)
    def _():
        halo().wait_recv()

    both = jnp.concatenate([hx[0, 8:16, :], hx[1, 8:16, :]], axis=0)
    got = dot(both, w[:, 0:256])
    for s in range(2):
        vp[s, 0, 8:16, :] = got[8 * s : 8 * s + 8, 128:256]
    gap = jnp.zeros((56, 128), F32)
    tail = jnp.concatenate([gap, got[8:16, 0:128], gap, got[0:8, 0:128]], axis=0).T
    bhl[z] = tail[0:32, :].astype(BF16)
    send_piece(2)

    load_v1.wait()

    def project(s, at):
        got = dot(hx[s], w[:, 256 + 256 * at : 512 + 256 * at])
        vp[s, 1 + 2 * at] = got[:, 0:128]
        vp[s, 2 + 2 * at] = got[:, 128:256]

    def value(s, b):
        for c in range(5):
            lanes = slice(128 * c, 128 * c + 128)
            mixed = None
            for k in range(4):
                at = 13 + k + Q * b
                term = cv[k : k + 1, lanes] * vp[s, c, at : at + Q, :]
                mixed = term if mixed is None else mixed + term
            here = (s, slice(Q * b, Q * b + Q), lanes)
            vv[here] = (silu(mixed) * av[here]).astype(BF16)

    project(early, 0)
    project(early, 1)
    for at in range(2):
        project(late, at)
        value(early, 2 * at)
        value(early, 2 * at + 1)
    pass_piece(1)
    pass_piece(2)
    for b in range(NB):
        value(late, b)

    def mix(s, h):
        ahead = bhl[4 * h : 4 * h + 4].astype(F32).reshape(128, 128)
        ahead = jnp.where(s == 1, pltpu.roll(ahead, 64, 1), ahead)
        x = bct[s, 4 * h : 4 * h + 4].astype(F32).reshape(128, LEN)
        x = jnp.concatenate([ahead, x], axis=1)
        turned = [pltpu.roll(x, 3 - k, 1) for k in range(3)] + [x]
        blocks = []
        for b in range(NB):
            lanes = slice(128 + Q * b, 256 + Q * b)
            mixed = tap[h] * turned[0][:, lanes]
            for k in range(1, 4):
                mixed = mixed + tap[2 * k + h] * turned[k][:, lanes]
            blocks.append(silu(mixed))
        return blocks

    for peer in others:
        decay(peer, peer).wait_recv()

    def pick(j, _):
        dxl[pl.ds(j, 1), :] = dall[2 * j, pl.ds(core, 1), :] + dall[2 * j + 1, pl.ds(core, 1), :]
        return 0

    lax.fori_loop(0, 16, pick, 0, unroll=True)
    dxl[16:17, :] = dall[2 * chip + 1, pl.ds(core, 1), :]
    dxl[24:32, :] = dall[2 * chip]
    dxl[17:24, :] = jnp.zeros((7, 128), F32)
    dx[...] = dot(split(jnp.exp(dxl[...])), ee[...])

    def states(s):
        for b, block in enumerate(mix(s, 0)):
            bmat[s, :, Q * b : Q * b + Q] = block.astype(BF16)
        state = None
        for b in range(NB):
            half = rx[s, b : b + 1, :]
            added = dot(bmat[s, :, Q * b : Q * b + Q], vv[s, Q * b : Q * b + Q, :]) * half
            if state is None:
                sbl[s, b] = jnp.zeros((128, CI), BF16)
                state = added
            else:
                lifted = state * half
                sbl[s, b] = lifted.astype(BF16)
                state = lifted * half + added
        for k in range(16):
            st[s, k] = state[8 * k : 8 * k + 8, :].astype(BF16)

    def across(s, n):
        return remote(st.at[s], so.at[s], cs.at[n], cr.at[n], seq=me + 1 - 2 * core)

    rest_of_piece(2)
    rest_of_piece(0)
    states(early)
    across(early, 0).start()
    rest_of_piece(1)
    states(late)

    @pl.when(core == 0)
    def _():
        across(0, 1).start()

    def first_hop(source, k):
        return remote(agg.at[k], p1.at[source], s1.at[k], r1.at[source], seq=2 * k + core)

    across(late, 0).wait_recv()
    carry = dx[16:17, :]
    for k, own in chips:
        mine, other = st[late, k].astype(F32), so[late, k].astype(F32)
        slab = jnp.where(core == 0, mine, other) * carry + jnp.where(core == 0, other, mine)
        agg[k] = slab.astype(BF16)
        if own:
            p1[k] = agg[k]
        else:
            first_hop(chip, k).start()

    def within(s):
        for b, block in enumerate(mix(s, 1)):
            cmat[s, Q * b : Q * b + Q, :] = block.T.astype(BF16)
        for b in range(NB):
            rows = slice(Q * b, Q * b + Q)
            c_rows = cmat[s, rows, :]
            scores = dot(c_rows, bmat[s, :, rows])
            scores = jnp.where(tri_at, scores, 0.0).astype(BF16)
            left = jnp.concatenate([scores, c_rows], axis=1)
            right = jnp.concatenate([vv[s, rows, :], sbl[s, b]], axis=0)
            g[s, rows, :] = dot(left, right)

    within(early)
    within(late)

    for k, own in chips:
        if not own:
            first_hop(k, chip).wait_recv()
    so_far = jnp.zeros((8, CI), F32)
    for j in range(16):
        po[j] = so_far.astype(BF16)
        so_far = so_far * dx[j : j + 1, :] + p1[j].astype(F32)

    def second_hop(target, source):
        slot = pin.at[late, source]
        return remote(po.at[target], slot, s2.at[target], r2.at[source], seq=2 * target + core)

    for k, own in chips:
        if own:
            pin[late, k] = po[k]
        else:
            second_hop(k, chip).start()

    load_g.wait()

    def gate(s, _):
        for at, wide in ((0, 256), (256, 256), (512, 128)):
            got = dot(hx[s, PAD : PAD + LEN, :], w[:, 768 + at : 768 + at + wide])
            fg[s, :, at : at + wide] = silu(got) * ev[s, :, at : at + wide]
        return 0

    lax.fori_loop(0, 2, gate, 0)

    ones = jnp.ones((16, 128), BF16)
    at_row = lax.broadcasted_iota(jnp.int32, (8, 128), 0)
    squares = jnp.zeros((8, 128), F32)
    for k, own in chips:
        if not own:
            second_hop(k, k).wait_recv()

    def back(s):
        return remote(pin.at[s], pin.at[s], cs.at[2], cr.at[2], seq=me + 1 - 2 * core)

    back(late).start()

    @pl.when(core == 1)
    def _():
        across(0, 1).wait_recv()

    for s in (late, early):
        if s is early:
            back(early).wait_recv()
        arrived = pin[s].astype(F32).reshape(128, CI)
        moved = arrived * dx[pl.ds(24 + s, 1), :] + so[s].astype(F32).reshape(128, CI)
        arrived = jnp.where(core == 1, moved, arrived).astype(BF16)
        given = dot(cmat[s], arrived)
        for b in range(NB):
            rows = slice(Q * b, Q * b + Q)
            gated = fg[s, rows, :] * (g[s, rows, :] + given[rows] * rx[s, 4 + b : 5 + b, :])
            g[s, rows, :] = gated
            sq = gated * gated
            sq = sum(sq[:, 128 * c : 128 * c + 128] for c in range(1, 5)) + sq[:, 0:128]
            summed = lax.dot_general(
                ones, sq.astype(BF16), (((1,), (1,)), ((), ())), preferred_element_type=F32
            )[0:8, :]
            squares = jnp.where(at_row == 4 * s + b, summed, squares)
    ssm[...] = squares

    def total_sq(owner, peer):
        return remote(ssm, ssa.at[owner], zs.at[peer], zr.at[owner], tp=peer)

    for step in (4, 3, -3, 2, -2, 1, -1):
        total_sq(z, away(step)).start()
    ssa[z] = ssm[...]
    gains = gn[...].reshape(1, CI)
    for s in range(2):
        out[s] = g[s] * gains
    for step in (4, 3, -3, 2, -2, 1, -1):
        total_sq(away(step), away(step)).wait_recv()
    rms[...] = lax.rsqrt(jnp.sum(ssa[...], axis=0) * (1.0 / DI) + EPS)

    for p in range(3):
        for step, n in near:
            piece(p, z, away(step), n).wait_send()
        for owner, target, n in passed_on(p):
            piece(p, away(owner), away(target), n).wait_send()
    for step in range(1, NZ):
        total_sq(z, away(step)).wait_send()

    for peer in others:
        decay(None, peer).wait_send()
    for k, own in chips:
        if not own:
            first_hop(chip, k).wait_send()
            second_hop(k, chip).wait_send()
    across(early, 0).wait_send()
    back(late).wait_send()

    @pl.when(core == 0)
    def _():
        across(0, 1).wait_send()

    @pl.when(me < NS - 1)
    def _():
        halo().wait_send()


def scaled(gated, rms, out, osc, sems):
    copies = []
    for s in range(2):
        for b in range(NB):
            n = NB * s + b
            rows = slice(Q * b, Q * b + Q)
            by_token = jnp.broadcast_to(rms[n : n + 1, :], (128, 128)).T
            for c in range(5):
                lanes = slice(128 * c, 128 * c + 128)
                osc[s, rows, lanes] = (gated[s, rows, lanes] * by_token).astype(BF16)
            copies.append(pltpu.make_async_copy(osc.at[s, rows], out.at[s, rows], sems.at[n]))
            copies[-1].start()
    for copy in copies:
        copy.wait()


def on_device(hid, gw, vw, bw, sw, vconv, bconv, sbias, lrate, gain):
    dma = pltpu.SemaphoreType.DMA
    vmem = pltpu.VMEM
    any_space = pl.BlockSpec(memory_space=pl.ANY)
    scratch = [
        vmem((2, PAD + LEN, D), BF16),
        vmem((D, 1408), BF16),
        vmem((32, D), BF16),
        vmem((HEADS, D), BF16),
        vmem((4, CI), F32),
        vmem((4, 256), F32),
        vmem((1, HEADS), F32),
        vmem((1, HEADS), F32),
        vmem((CI,), F32),
        vmem((8, 128), F32),
        vmem((8, 128, 128), F32),
        vmem((256, CI), BF16),
        vmem((2, LEN, 128), F32),
        vmem((2, 5, PAD + LEN, 128), F32),
        vmem((2, NZ, 32, LEN), BF16),
        vmem((2, LEN, 128), BF16),
        vmem((2, 128, LEN), BF16),
        vmem((2, LEN, CI), F32),
        vmem((2, LEN, CI), F32),
        vmem((2, LEN, CI), F32),
        vmem((2, LEN, CI), F32),
        vmem((2, 8, CI), F32),
        vmem((8, 128), F32),
        vmem((NS, 8, 128), F32),
        vmem((NS, 128), F32),
        vmem((NS, CI), F32),
        vmem((NZ, 32, 128), BF16),
        vmem((2, LEN, CI), BF16),
        vmem((2, NB, 128, CI), BF16),
        vmem((2, 16, 8, CI), BF16),
        vmem((2, 16, 8, CI), BF16),
        vmem((16, 8, CI), BF16),
        vmem((16, 8, CI), BF16),
        vmem((16, 8, CI), BF16),
        vmem((2, 16, 8, CI), BF16),
        vmem((8, 128), F32),
        vmem((NZ, 8, 128), F32),
        dma((14,)),
        dma,
        dma,
        dma((3, 7)),
        dma((3, NZ)),
        dma((NS,)),
        dma((NS,)),
        dma((16,)),
        dma((16,)),
        dma((16,)),
        dma((16,)),
        dma((NZ,)),
        dma((NZ,)),
        dma((3,)),
        dma((3,)),
    ]
    in_vmem = pl.BlockSpec(memory_space=vmem)
    gated, rms = pl.pallas_call(
        kernel,
        out_shape=(vmem((2, LEN, CI), F32), vmem((8, 128), F32)),
        in_specs=[any_space] * 10,
        out_specs=(in_vmem, in_vmem),
        scratch_shapes=scratch,
        compiler_params=pltpu.CompilerParams(
            collective_id=0, has_side_effects=True, vmem_limit_bytes=56 * 2**20
        ),
    )(
        hid, gw, vw, bw.T, sw.T, vconv, bconv,
        sbias.reshape(1, HEADS), lrate.reshape(1, HEADS), gain,
    )
    return pl.pallas_call(
        scaled,
        out_shape=jax.ShapeDtypeStruct((2, LEN, CI), BF16),
        in_specs=[in_vmem, in_vmem],
        out_specs=any_space,
        scratch_shapes=[vmem((2, LEN, CI), BF16), dma((2 * NB,))],
    )(*(pltpu.with_memory_space_constraint(x, vmem) for x in (gated, rms)))


def solution(mesh):
    placed = (
        P(None, "seq", None),
        P(None, "tp"),
        P(None, "tp"),
        P(None, "tp"),
        P(None, "tp"),
        P(None, "tp"),
        P(),
        P("tp"),
        P("tp"),
        P("tp"),
    )
    return jax.shard_map(
        on_device, mesh=mesh, in_specs=placed, out_specs=P(None, "seq", "tp"), check_vma=False
    )
```

```python
import jax
import jax.numpy as jnp
from jax import lax
from jax.experimental import pallas as pl
from jax.experimental.pallas import tpu as pltpu
from jax.sharding import PartitionSpec as P

MESH = pl.DeviceIdType.MESH
F32, BF16 = jnp.float32, jnp.bfloat16

NS, NZ = 32, 8
D, DI = 2560, 5120
CI = 640
LEN = 512
Q = 128
NB = LEN // Q
PAD = 16
HL = 32
HEADS = 10
EPS = 1e-05


def dot(a, b):
    return jnp.dot(a, b, preferred_element_type=F32)


def silu(x):
    half = 0.5 * x
    return half + half * jnp.tanh(half)


def split(x):
    high = x.astype(BF16)
    low = (x - high.astype(F32)).astype(BF16)
    return jnp.concatenate([high, low], axis=1)


def kernel(
    hid, gw, vw, bw, sw, vconv, bconv, sbias, lrate, gain, out, rms,
    hx, w, bwv, swv, cv, bcv, sb, lr, gn, prm, tap, ee, bs, vp, bct, cmat, bmat,
    av, es, fg, g, rx, dsum, dall, dxl, dx, bhl, vv, sbl, st, so, agg, p1, po, pin, ssm, ssa,
    ld, hs, hr, bsend, brecv, dsend, drecv, s1, r1, s2, r2, zs, zr, cs, cr,
):
    me, z = lax.axis_index("seq"), lax.axis_index("tp")
    core, chip = me & 1, lax.div(me, 2)
    early, late = 1 - core, core

    def remote(src, dst, ss, rs, seq=None, tp=None):
        where = {"seq": me if seq is None else seq, "tp": z if tp is None else tp}
        return pltpu.make_async_remote_copy(
            src_ref=src, dst_ref=dst, send_sem=ss, recv_sem=rs, device_id=where, device_id_type=MESH
        )

    small = [
        pltpu.make_async_copy(src, dst, ld.at[9 + n])
        for n, (src, dst) in enumerate(
            [(vconv, cv), (bconv, bcv), (sbias, sb), (lrate, lr), (gain, gn)]
        )
    ]
    load_b = pltpu.make_async_copy(bw, bwv, ld.at[0])
    load_s = pltpu.make_async_copy(sw, swv, ld.at[1])
    load_v0 = pltpu.make_async_copy(vw.at[:, 0:128], w.at[:, 128:256], ld.at[2])
    load_v1 = pltpu.make_async_copy(vw.at[:, 128:CI], w.at[:, 256:768], ld.at[7])
    load_g = pltpu.make_async_copy(gw, w.at[:, 768:1408], ld.at[8])

    def load_h(s, h):
        return pltpu.make_async_copy(
            hid.at[s, pl.ds(256 * h, 256)], hx.at[s, pl.ds(PAD + 256 * h, 256)], ld.at[3 + 2 * s + h]
        )

    load_b.start()
    load_s.start()
    for copy in small:
        copy.start()
    load_v0.start()
    for s in (early, late):
        for h in range(2):
            load_h(s, h).start()
    load_v1.start()
    load_g.start()

    barrier = pltpu.get_barrier_semaphore()

    def greet_seq(r, _):
        pl.semaphore_signal(
            barrier, inc=1, device_id={"seq": (me + r) & (NS - 1), "tp": z}, device_id_type=MESH
        )
        return 0

    def greet_tp(r, _):
        pl.semaphore_signal(
            barrier, inc=1, device_id={"seq": me, "tp": (z + r) & (NZ - 1)}, device_id_type=MESH
        )
        return 0

    lax.fori_loop(1, NS, greet_seq, 0)
    lax.fori_loop(1, NZ, greet_tp, 0)

    row = lax.broadcasted_iota(jnp.int32, (256, CI), 0)
    col = lax.broadcasted_iota(jnp.int32, (256, CI), 1)
    ee[...] = jnp.where((row & 127) == HL + (col >> 6), 1.0, 0.0).astype(BF16)
    tri_at = lax.broadcasted_iota(jnp.int32, (Q, Q), 0) >= lax.broadcasted_iota(
        jnp.int32, (Q, Q), 1
    )
    tri = jnp.where(tri_at, 1.0, 0.0).astype(BF16)
    prm[...] = jnp.zeros((8, 128), F32)
    dsum[...] = jnp.zeros((8, 128), F32)
    for s in range(2):
        hx[s, 0:8, :] = jnp.zeros((8, D), BF16)

    @pl.when(me == 0)
    def _():
        for s in range(2):
            hx[s, 8:16, :] = jnp.zeros((8, D), BF16)

    for copy in small:
        copy.wait()
    prm[0:1, HL : HL + HEADS] = sb[...]
    prm[1:2, HL : HL + HEADS] = lr[...]
    for k in range(4):
        for h in range(2):
            taps = bcv[k : k + 1, 128 * h : 128 * h + 128]
            tap[2 * k + h] = jnp.broadcast_to(taps, (128, 128)).T
    load_b.wait()
    load_s.wait()
    for n in range(D // 128):
        lanes = slice(128 * n, 128 * n + 128)
        both = jnp.concatenate(
            [bwv[:, lanes].astype(F32), swv[:, lanes].astype(F32), jnp.zeros((86, 128), F32)], axis=0
        )
        w[lanes, 0:128] = both.T.astype(BF16)
    load_v0.wait()

    def first(s):
        for h in range(2):
            if s is early:
                load_h(s, h).wait()
            at = 256 * h
            got = dot(hx[s, PAD + at : PAD + at + 256, :], w[:, 0:256])
            bs[s, at : at + 256, :] = got[:, 0:128]
            vp[s, 0, PAD + at : PAD + at + 256, :] = got[:, 128:256]
        for b in range(NB):
            turned = bs[s, Q * b : Q * b + Q, :].T
            bct[s, z, :, Q * b : Q * b + Q] = turned[0:32, :].astype(BF16)

    def piece(p, owner, peer, n):
        part = bct.at[(early, late)[p], owner] if p < 2 else bhl.at[owner]
        return remote(part, part, bsend.at[p, n], brecv.at[p, owner], tp=peer)

    def away(n):
        return (z + n) & (NZ - 1)

    near = ((2, 0), (-2, 1), (1, 2), (-1, 3))
    far_first = (4, 3, -3, 2, -2, 1, -1)
    to_b = jnp.where((z >= 2) & (z < 6), 1, -1)

    def send_piece(p):
        for step, n in near:
            piece(p, z, away(step), n).start()

    def passed_on(p, way, act):
        owner = away(-2 * way)
        n = jnp.where(way > 0, 4, 5)
        act(piece(p, owner, away(way), n))

        @pl.when(way == (-1 if p else 1))
        def _():
            act(piece(p, owner, away(2 * way), 6))

    def pass_piece(p, way):
        owner = away(-2 * way)
        piece(p, owner, owner, 0).wait_recv()
        passed_on(p, way, lambda copy: copy.start())

    def rest_of_piece(p, owners):
        for owner in owners:
            gap = (owner - z) & (NZ - 1)
            here = gap != 0
            if p < 2:
                here = here & (gap != 2) & (gap != 6)

            @pl.when(here)
            def _():
                piece(p, owner, owner, 0).wait_recv()

    def halo():
        return remote(hx.at[:, 520:528], hx.at[:, 8:16], hs, hr, seq=(me + 1) & (NS - 1))

    first(early)
    for h in range(2):
        load_h(late, h).wait()
    pl.semaphore_wait(barrier, NS - 1 + NZ - 1)

    @pl.when(me < NS - 1)
    def _():
        halo().start()

    send_piece(0)
    first(late)
    send_piece(1)

    lane = lax.broadcasted_iota(jnp.int32, (LEN, 128), 1)
    is_head = (lane >= HL) & (lane < HL + HEADS)
    rate = jnp.exp(prm[1:2, :])

    def steps(s):
        x = bs[s] + prm[0:1, :]
        size = jnp.maximum(x, 0.0) + jnp.log1p(jnp.exp(-jnp.abs(x)))
        size = jnp.where(is_head, size, 0.0)
        parts = split(-size * rate)
        so_far = jnp.zeros((1, 128), F32)
        halves, ahead, off = [], [], []
        for b in range(NB):
            sums = dot(tri, parts[Q * b : Q * b + Q, :])
            cum = sums[:, 0:128] + sums[:, 128:256]
            total = cum[Q - 1 : Q, :]
            mid = 0.5 * total
            off.append(cum - mid)
            halves.append(jnp.exp(mid))
            ahead.append(jnp.exp(so_far + mid))
            so_far = so_far + total
        off = jnp.concatenate(off, axis=0)
        av[s] = dot(split(size * jnp.exp(-off)), ee[...])
        es[s] = split(jnp.exp(off))
        rows = jnp.concatenate(halves + ahead + [jnp.zeros((8, 128), F32)], axis=0)
        rx[s] = dot(split(rows), ee[...])[0:8, :]
        dsum[pl.ds(s, 1), :] = so_far

    steps(early)
    steps(late)

    y, x = lax.div(chip, 4), chip & 3
    reach = [0, 1, 2, 1]
    offsets = sorted(
        ((dy, dx) for dy in range(4) for dx in range(4)), key=lambda o: -reach[o[0]] - reach[o[1]]
    )
    chips = [(((y + dy) & 3) * 4 + ((x + dx) & 3), (dy, dx) == (0, 0)) for dy, dx in offsets]
    others = [2 * c + n for c, own in chips for n in range(2) if not own] + [me + 1 - 2 * core]

    def decay(owner, peer):
        src = dsum if owner is None else dall.at[owner]
        slot = me if owner is None else owner
        return remote(src, dall.at[slot], dsend.at[peer], drecv.at[slot], seq=peer)

    for peer in others:
        decay(None, peer).start()
    dall[me] = dsum[...]

    @pl.when(me > 0)
    def _():
        halo().wait_recv()

    both = jnp.concatenate([hx[0, 8:16, :], hx[1, 8:16, :]], axis=0)
    got = dot(both, w[:, 0:256])
    for s in range(2):
        vp[s, 0, 8:16, :] = got[8 * s : 8 * s + 8, 128:256]
    gap = jnp.zeros((56, 128), F32)
    tail = jnp.concatenate([gap, got[8:16, 0:128], gap, got[0:8, 0:128]], axis=0).T
    bhl[z] = tail[0:32, :].astype(BF16)
    for step in far_first:
        piece(2, z, away(step), step & (NZ - 1)).start()

    load_v1.wait()

    def project(s, at):
        got = dot(hx[s], w[:, 256 + 256 * at : 512 + 256 * at])
        vp[s, 1 + 2 * at] = got[:, 0:128]
        vp[s, 2 + 2 * at] = got[:, 128:256]

    def value(s, b):
        for c in range(5):
            lanes = slice(128 * c, 128 * c + 128)
            mixed = None
            for k in range(4):
                at = 13 + k + Q * b
                term = cv[k : k + 1, lanes] * vp[s, c, at : at + Q, :]
                mixed = term if mixed is None else mixed + term
            here = (s, slice(Q * b, Q * b + Q), lanes)
            vv[here] = (silu(mixed) * av[here]).astype(BF16)

    project(early, 0)
    project(early, 1)
    for at in range(2):
        pass_piece(at, to_b)
        project(late, at)
        value(early, 2 * at)
        value(early, 2 * at + 1)
    for at in range(2):
        pass_piece(at, -to_b)
    for b in range(NB):
        value(late, b)

    def mix(s, h):
        ahead = bhl[4 * h : 4 * h + 4].astype(F32).reshape(128, 128)
        ahead = jnp.where(s == 1, pltpu.roll(ahead, 64, 1), ahead)
        x = bct[s, 4 * h : 4 * h + 4].astype(F32).reshape(128, LEN)
        x = jnp.concatenate([ahead, x], axis=1)
        turned = [pltpu.roll(x, 3 - k, 1) for k in range(3)] + [x]
        blocks = []
        for b in range(NB):
            lanes = slice(128 + Q * b, 256 + Q * b)
            mixed = tap[h] * turned[0][:, lanes]
            for k in range(1, 4):
                mixed = mixed + tap[2 * k + h] * turned[k][:, lanes]
            blocks.append(silu(mixed))
        return blocks

    for peer in others:
        decay(peer, peer).wait_recv()

    def pick(j, _):
        dxl[pl.ds(j, 1), :] = dall[2 * j, pl.ds(core, 1), :] + dall[2 * j + 1, pl.ds(core, 1), :]
        return 0

    lax.fori_loop(0, 16, pick, 0, unroll=True)
    dxl[16:17, :] = dall[2 * chip + 1, pl.ds(core, 1), :]
    dxl[24:32, :] = dall[2 * chip]
    dxl[17:24, :] = jnp.zeros((7, 128), F32)
    dx[...] = dot(split(jnp.exp(dxl[...])), ee[...])

    def states(s):
        for b, block in enumerate(mix(s, 0)):
            bmat[s, :, Q * b : Q * b + Q] = block.astype(BF16)
        state = None
        for b in range(NB):
            half = rx[s, b : b + 1, :]
            added = dot(bmat[s, :, Q * b : Q * b + Q], vv[s, Q * b : Q * b + Q, :]) * half
            if state is None:
                sbl[s, b] = jnp.zeros((128, CI), BF16)
                state = added
            else:
                lifted = state * half
                sbl[s, b] = lifted.astype(BF16)
                state = lifted * half + added
        for k in range(16):
            st[s, k] = state[8 * k : 8 * k + 8, :].astype(BF16)

    def across(s, n):
        return remote(st.at[s], so.at[s], cs.at[n], cr.at[n], seq=me + 1 - 2 * core)

    b_owners, c_owners = range(4), range(4, 8)
    rest_of_piece(2, b_owners)
    rest_of_piece(0, b_owners)
    states(early)
    across(early, 0).start()
    rest_of_piece(1, b_owners)
    states(late)

    @pl.when(core == 0)
    def _():
        across(0, 1).start()

    def first_hop(source, k):
        return remote(agg.at[k], p1.at[source], s1.at[k], r1.at[source], seq=2 * k + core)

    across(late, 0).wait_recv()
    carry = dx[16:17, :]
    for k, own in chips:
        mine, other = st[late, k].astype(F32), so[late, k].astype(F32)
        slab = jnp.where(core == 0, mine, other) * carry + jnp.where(core == 0, other, mine)
        agg[k] = slab.astype(BF16)
        if own:
            p1[k] = agg[k]
        else:
            first_hop(chip, k).start()

    def within(s):
        for b, block in enumerate(mix(s, 1)):
            cmat[s, Q * b : Q * b + Q, :] = block.T.astype(BF16)
        for b in range(NB):
            rows = slice(Q * b, Q * b + Q)
            c_rows = cmat[s, rows, :]
            scores = dot(c_rows, bmat[s, :, rows])
            scores = jnp.where(tri_at, scores, 0.0).astype(BF16)
            left = jnp.concatenate([scores, c_rows], axis=1)
            right = jnp.concatenate([vv[s, rows, :], sbl[s, b]], axis=0)
            g[s, rows, :] = dot(left, right)

    rest_of_piece(2, c_owners)
    rest_of_piece(0, c_owners)
    within(early)
    rest_of_piece(1, c_owners)
    within(late)

    for k, own in chips:
        if not own:
            first_hop(k, chip).wait_recv()
    so_far = jnp.zeros((8, CI), F32)
    for j in range(16):
        po[j] = so_far.astype(BF16)
        so_far = so_far * dx[j : j + 1, :] + p1[j].astype(F32)

    def second_hop(target, source):
        slot = pin.at[late, source]
        return remote(po.at[target], slot, s2.at[target], r2.at[source], seq=2 * target + core)

    for k, own in chips:
        if own:
            pin[late, k] = po[k]
        else:
            second_hop(k, chip).start()

    load_g.wait()

    def gate(s, _):
        for at, wide in ((0, 256), (256, 256), (512, 128)):
            got = dot(hx[s, PAD : PAD + LEN, :], w[:, 768 + at : 768 + at + wide])
            factor = dot(es[s], ee[:, at : at + wide])
            fg[s, :, at : at + wide] = silu(got) * factor
        return 0

    lax.fori_loop(0, 2, gate, 0)

    ones = jnp.ones((16, 128), BF16)
    at_row = lax.broadcasted_iota(jnp.int32, (8, 128), 0)
    squares = jnp.zeros((8, 128), F32)
    for k, own in chips:
        if not own:
            second_hop(k, k).wait_recv()

    def back(s):
        return remote(pin.at[s], pin.at[s], cs.at[2], cr.at[2], seq=me + 1 - 2 * core)

    back(late).start()

    @pl.when(core == 1)
    def _():
        across(0, 1).wait_recv()

    for s in (late, early):
        if s is early:
            back(early).wait_recv()
        arrived = pin[s].astype(F32).reshape(128, CI)
        moved = arrived * dx[pl.ds(24 + s, 1), :] + so[s].astype(F32).reshape(128, CI)
        arrived = jnp.where(core == 1, moved, arrived).astype(BF16)
        given = dot(cmat[s], arrived)
        for b in range(NB):
            rows = slice(Q * b, Q * b + Q)
            gated = fg[s, rows, :] * (g[s, rows, :] + given[rows] * rx[s, 4 + b : 5 + b, :])
            g[s, rows, :] = gated
            sq = gated * gated
            sq = sum(sq[:, 128 * c : 128 * c + 128] for c in range(1, 5)) + sq[:, 0:128]
            summed = lax.dot_general(
                ones, sq.astype(BF16), (((1,), (1,)), ((), ())), preferred_element_type=F32
            )[0:8, :]
            squares = jnp.where(at_row == 4 * s + b, summed, squares)
    ssm[...] = squares

    def total_sq(owner, peer):
        return remote(ssm, ssa.at[owner], zs.at[peer], zr.at[owner], tp=peer)

    for step in far_first:
        total_sq(z, away(step)).start()
    ssa[z] = ssm[...]
    gains = gn[...].reshape(1, CI)
    for s in range(2):
        out[s] = g[s] * gains
    for step in far_first:
        total_sq(away(step), away(step)).wait_recv()
    rms[...] = lax.rsqrt(jnp.sum(ssa[...], axis=0) * (1.0 / DI) + EPS)

    for p in range(2):
        for step, n in near:
            piece(p, z, away(step), n).wait_send()
        for way in (1, -1):
            passed_on(p, way, lambda copy: copy.wait_send())
    for step in far_first:
        piece(2, z, away(step), step & (NZ - 1)).wait_send()
    for step in range(1, NZ):
        total_sq(z, away(step)).wait_send()

    for peer in others:
        decay(None, peer).wait_send()
    for k, own in chips:
        if not own:
            first_hop(chip, k).wait_send()
            second_hop(k, chip).wait_send()
    across(early, 0).wait_send()
    back(late).wait_send()

    @pl.when(core == 0)
    def _():
        across(0, 1).wait_send()

    @pl.when(me < NS - 1)
    def _():
        halo().wait_send()


def scaled(gated, rms, out, osc, sems):
    copies = []
    for s in range(2):
        for b in range(NB):
            n = NB * s + b
            rows = slice(Q * b, Q * b + Q)
            by_token = jnp.broadcast_to(rms[n : n + 1, :], (128, 128)).T
            for c in range(5):
                lanes = slice(128 * c, 128 * c + 128)
                osc[s, rows, lanes] = (gated[s, rows, lanes] * by_token).astype(BF16)
            copies.append(pltpu.make_async_copy(osc.at[s, rows], out.at[s, rows], sems.at[n]))
            copies[-1].start()
    for copy in copies:
        copy.wait()


def on_device(hid, gw, vw, bw, sw, vconv, bconv, sbias, lrate, gain):
    dma = pltpu.SemaphoreType.DMA
    vmem = pltpu.VMEM
    any_space = pl.BlockSpec(memory_space=pl.ANY)
    scratch = [
        vmem((2, PAD + LEN, D), BF16),
        vmem((D, 1408), BF16),
        vmem((32, D), BF16),
        vmem((HEADS, D), BF16),
        vmem((4, CI), F32),
        vmem((4, 256), F32),
        vmem((1, HEADS), F32),
        vmem((1, HEADS), F32),
        vmem((CI,), F32),
        vmem((8, 128), F32),
        vmem((8, 128, 128), F32),
        vmem((256, CI), BF16),
        vmem((2, LEN, 128), F32),
        vmem((2, 5, PAD + LEN, 128), F32),
        vmem((2, NZ, 32, LEN), BF16),
        vmem((2, LEN, 128), BF16),
        vmem((2, 128, LEN), BF16),
        vmem((2, LEN, CI), F32),
        vmem((2, LEN, 256), BF16),
        vmem((2, LEN, CI), F32),
        vmem((2, LEN, CI), F32),
        vmem((2, 8, CI), F32),
        vmem((8, 128), F32),
        vmem((NS, 8, 128), F32),
        vmem((NS, 128), F32),
        vmem((NS, CI), F32),
        vmem((NZ, 32, 128), BF16),
        vmem((2, LEN, CI), BF16),
        vmem((2, NB, 128, CI), BF16),
        vmem((2, 16, 8, CI), BF16),
        vmem((2, 16, 8, CI), BF16),
        vmem((16, 8, CI), BF16),
        vmem((16, 8, CI), BF16),
        vmem((16, 8, CI), BF16),
        vmem((2, 16, 8, CI), BF16),
        vmem((8, 128), F32),
        vmem((NZ, 8, 128), F32),
        dma((14,)),
        dma,
        dma,
        dma((3, NZ)),
        dma((3, NZ)),
        dma((NS,)),
        dma((NS,)),
        dma((16,)),
        dma((16,)),
        dma((16,)),
        dma((16,)),
        dma((NZ,)),
        dma((NZ,)),
        dma((3,)),
        dma((3,)),
    ]
    in_vmem = pl.BlockSpec(memory_space=vmem)
    gated, rms = pl.pallas_call(
        kernel,
        out_shape=(vmem((2, LEN, CI), F32), vmem((8, 128), F32)),
        in_specs=[any_space] * 10,
        out_specs=(in_vmem, in_vmem),
        scratch_shapes=scratch,
        compiler_params=pltpu.CompilerParams(
            collective_id=0, has_side_effects=True, vmem_limit_bytes=56 * 2**20
        ),
    )(
        hid, gw, vw, bw.T, sw.T, vconv, bconv,
        sbias.reshape(1, HEADS), lrate.reshape(1, HEADS), gain,
    )
    return pl.pallas_call(
        scaled,
        out_shape=jax.ShapeDtypeStruct((2, LEN, CI), BF16),
        in_specs=[in_vmem, in_vmem],
        out_specs=any_space,
        scratch_shapes=[vmem((2, LEN, CI), BF16), dma((2 * NB,))],
    )(*(pltpu.with_memory_space_constraint(x, vmem) for x in (gated, rms)))


def solution(mesh):
    placed = (
        P(None, "seq", None),
        P(None, "tp"),
        P(None, "tp"),
        P(None, "tp"),
        P(None, "tp"),
        P(None, "tp"),
        P(),
        P("tp"),
        P("tp"),
        P("tp"),
    )
    return jax.shard_map(
        on_device, mesh=mesh, in_specs=placed, out_specs=P(None, "seq", "tp"), check_vma=False
    )
```

```python
import jax
import jax.numpy as jnp
from jax import lax
from jax.experimental import pallas as pl
from jax.experimental.pallas import tpu as pltpu
from jax.sharding import PartitionSpec as P

MESH = pl.DeviceIdType.MESH
F32, BF16 = jnp.float32, jnp.bfloat16

NS, NZ = 32, 8
D, DI = 2560, 5120
CI = 640
LEN = 512
Q = 128
NB = LEN // Q
PAD = 16
HL = 32
HEADS = 10
EPS = 1e-05


def dot(a, b):
    return jnp.dot(a, b, preferred_element_type=F32)


def silu(x):
    half = 0.5 * x
    return half + half * jnp.tanh(half)


def split(x):
    high = x.astype(BF16)
    low = (x - high.astype(F32)).astype(BF16)
    return jnp.concatenate([high, low], axis=1)


def kernel(
    hid, gw, vw, bw, sw, vconv, bconv, sbias, lrate, gain, out, rms,
    hx, w, bwv, swv, cv, bcv, sb, lr, gn, prm, tap, ee, bs, vp, bct, cmat, bmat,
    av, es, fg, g, rx, dsum, dall, dxl, dx, bhl, vv, sbl, st, so, agg, p1, po, pin, ssm, ssa,
    ld, hs, hr, bsend, brecv, bhs, bhr, dsend, drecv, s1, r1, s2, r2, zs, zr, cs, cr,
):
    me, z = lax.axis_index("seq"), lax.axis_index("tp")
    core, chip = me & 1, lax.div(me, 2)
    early, late = 1 - core, core

    def remote(src, dst, ss, rs, seq=None, tp=None):
        where = {"seq": me if seq is None else seq, "tp": z if tp is None else tp}
        return pltpu.make_async_remote_copy(
            src_ref=src, dst_ref=dst, send_sem=ss, recv_sem=rs, device_id=where, device_id_type=MESH
        )

    barrier = pltpu.get_barrier_semaphore()

    def greet_seq(r, _):
        pl.semaphore_signal(
            barrier, inc=1, device_id={"seq": (me + r) & (NS - 1), "tp": z}, device_id_type=MESH
        )
        return 0

    def greet_tp(r, _):
        pl.semaphore_signal(
            barrier, inc=1, device_id={"seq": me, "tp": (z + r) & (NZ - 1)}, device_id_type=MESH
        )
        return 0

    lax.fori_loop(1, NZ, greet_tp, 0)

    small = [
        pltpu.make_async_copy(src, dst, ld.at[9 + n])
        for n, (src, dst) in enumerate(
            [(vconv, cv), (bconv, bcv), (sbias, sb), (lrate, lr), (gain, gn)]
        )
    ]
    load_b = pltpu.make_async_copy(bw, bwv, ld.at[0])
    load_s = pltpu.make_async_copy(sw, swv, ld.at[1])
    load_v0 = pltpu.make_async_copy(vw.at[:, 0:128], w.at[:, 128:256], ld.at[2])
    load_v1 = pltpu.make_async_copy(vw.at[:, 128:CI], w.at[:, 256:768], ld.at[7])
    load_g = pltpu.make_async_copy(gw, w.at[:, 768:1408], ld.at[8])

    def load_h(s, h):
        return pltpu.make_async_copy(
            hid.at[s, pl.ds(256 * h, 256)], hx.at[s, pl.ds(PAD + 256 * h, 256)], ld.at[3 + 2 * s + h]
        )

    load_b.start()
    load_s.start()
    for copy in small:
        copy.start()
    load_v0.start()
    for h in range(2):
        load_h(early, h).start()

    lax.fori_loop(1, NS, greet_seq, 0)

    row = lax.broadcasted_iota(jnp.int32, (256, CI), 0)
    col = lax.broadcasted_iota(jnp.int32, (256, CI), 1)
    ee[...] = jnp.where((row & 127) == HL + (col >> 6), 1.0, 0.0).astype(BF16)
    tri_at = lax.broadcasted_iota(jnp.int32, (Q, Q), 0) >= lax.broadcasted_iota(
        jnp.int32, (Q, Q), 1
    )
    tri = jnp.where(tri_at, 1.0, 0.0).astype(BF16)
    prm[...] = jnp.zeros((8, 128), F32)
    dsum[...] = jnp.zeros((8, 128), F32)
    for s in range(2):
        hx[s, 0:8, :] = jnp.zeros((8, D), BF16)

    @pl.when(me == 0)
    def _():
        for s in range(2):
            hx[s, 8:16, :] = jnp.zeros((8, D), BF16)

    for copy in small:
        copy.wait()
    prm[0:1, HL : HL + HEADS] = sb[...]
    prm[1:2, HL : HL + HEADS] = lr[...]
    for k in range(4):
        for h in range(2):
            taps = bcv[k : k + 1, 128 * h : 128 * h + 128]
            tap[2 * k + h] = jnp.broadcast_to(taps, (128, 128)).T
    load_b.wait()
    load_s.wait()
    for n in range(D // 128):
        lanes = slice(128 * n, 128 * n + 128)
        both = jnp.concatenate(
            [bwv[:, lanes].astype(F32), swv[:, lanes].astype(F32), jnp.zeros((86, 128), F32)], axis=0
        )
        w[lanes, 0:128] = both.T.astype(BF16)
    for h in range(2):
        load_h(late, h).start()
    load_v0.wait()

    def first(s):
        for h in range(2):
            if s is early:
                load_h(s, h).wait()
            at = 256 * h
            got = dot(hx[s, PAD + at : PAD + at + 256, :], w[:, 0:256])
            bs[s, at : at + 256, :] = got[:, 0:128]
            vp[s, 0, PAD + at : PAD + at + 256, :] = got[:, 128:256]
        for b in range(NB):
            turned = bs[s, Q * b : Q * b + Q, :].T
            bct[s, z, :, Q * b : Q * b + Q] = turned[0:32, :].astype(BF16)

    def piece(p, owner, peer):
        if p == 2:
            return remote(bhl.at[owner], bhl.at[owner], bhs, bhr, tp=peer)
        part = bct.at[(early, late)[p], owner]
        return remote(part, part, bsend, brecv.at[p, owner], tp=peer)

    def away(n):
        return (z + n) & (NZ - 1)

    near = (2, -2, 1, -1)
    far_first = (4, 3, -3, 2, -2, 1, -1)
    to_b = jnp.where((z >= 2) & (z < 6), 1, -1)

    def send_piece(p, steps):
        for step in near[steps]:
            piece(p, z, away(step)).start()

    def pass_piece(p, way):
        owner = away(-2 * way)
        piece(p, owner, owner).wait_recv()
        piece(p, owner, away(way)).start()

        @pl.when(way == (-1 if p else 1))
        def _():
            piece(p, owner, away(2 * way)).start()

    def rest_of_piece(p, owners):
        for owner in owners:
            gap = (owner - z) & (NZ - 1)

            @pl.when((gap != 0) & (gap != 2) & (gap != 6))
            def _():
                piece(p, owner, owner).wait_recv()

    def all_of(part, ss, rs):
        return remote(part, part, ss, rs, tp=away(1))

    def halo():
        return remote(hx.at[:, 520:528], hx.at[:, 8:16], hs, hr, seq=(me + 1) & (NS - 1))

    ahead = z < NZ // 2
    first(early)
    load_v1.start()
    for h in range(2):
        load_h(late, h).wait()

    @pl.when(ahead)
    def _():
        first(late)

    pl.semaphore_wait(barrier, NS - 1 + NZ - 1)

    @pl.when(me < NS - 1)
    def _():
        halo().start()

    send_piece(0, slice(0, 2))

    @pl.when(jnp.logical_not(ahead))
    def _():
        send_piece(0, slice(2, 4))
        first(late)

    load_g.start()
    send_piece(1, slice(0, 2))

    @pl.when(ahead)
    def _():
        send_piece(0, slice(2, 4))

    send_piece(1, slice(2, 4))

    lane = lax.broadcasted_iota(jnp.int32, (LEN, 128), 1)
    is_head = (lane >= HL) & (lane < HL + HEADS)
    rate = jnp.exp(prm[1:2, :])

    def steps(s):
        x = bs[s] + prm[0:1, :]
        size = jnp.maximum(x, 0.0) + jnp.log1p(jnp.exp(-jnp.abs(x)))
        size = jnp.where(is_head, size, 0.0)
        parts = split(-size * rate)
        so_far = jnp.zeros((1, 128), F32)
        halves, ahead, off = [], [], []
        for b in range(NB):
            sums = dot(tri, parts[Q * b : Q * b + Q, :])
            cum = sums[:, 0:128] + sums[:, 128:256]
            total = cum[Q - 1 : Q, :]
            mid = 0.5 * total
            off.append(cum - mid)
            halves.append(jnp.exp(mid))
            ahead.append(jnp.exp(so_far + mid))
            so_far = so_far + total
        off = jnp.concatenate(off, axis=0)
        av[s] = dot(split(size * jnp.exp(-off)), ee[...])
        es[s] = split(jnp.exp(off))
        rows = jnp.concatenate(halves + ahead + [jnp.zeros((8, 128), F32)], axis=0)
        rx[s] = dot(split(rows), ee[...])[0:8, :]
        dsum[pl.ds(s, 1), :] = so_far

    steps(early)
    steps(late)

    y, x = lax.div(chip, 4), chip & 3
    reach = [0, 1, 2, 1]
    offsets = sorted(
        ((dy, dx) for dy in range(4) for dx in range(4)), key=lambda o: -reach[o[0]] - reach[o[1]]
    )
    chips = [(((y + dy) & 3) * 4 + ((x + dx) & 3), (dy, dx) == (0, 0)) for dy, dx in offsets]
    others = [2 * c + n for c, own in chips for n in range(2) if not own] + [me + 1 - 2 * core]

    def decay(peer):
        return remote(dsum, dall.at[me], dsend, drecv, seq=peer)

    for peer in others:
        decay(peer).start()
    dall[me] = dsum[...]

    @pl.when(me > 0)
    def _():
        halo().wait_recv()

    both = jnp.concatenate([hx[0, 8:16, :], hx[1, 8:16, :]], axis=0)
    got = dot(both, w[:, 0:256])
    for s in range(2):
        vp[s, 0, 8:16, :] = got[8 * s : 8 * s + 8, 128:256]
    gap = jnp.zeros((56, 128), F32)
    tail = jnp.concatenate([gap, got[8:16, 0:128], gap, got[0:8, 0:128]], axis=0).T
    bhl[z] = tail[0:32, :].astype(BF16)
    for step in far_first:
        piece(2, z, away(step)).start()

    load_v1.wait()

    def project(s, at):
        got = dot(hx[s], w[:, 256 + 256 * at : 512 + 256 * at])
        vp[s, 1 + 2 * at] = got[:, 0:128]
        vp[s, 2 + 2 * at] = got[:, 128:256]

    def value(s, b):
        for c in range(5):
            lanes = slice(128 * c, 128 * c + 128)
            mixed = None
            for k in range(4):
                at = 13 + k + Q * b
                term = cv[k : k + 1, lanes] * vp[s, c, at : at + Q, :]
                mixed = term if mixed is None else mixed + term
            here = (s, slice(Q * b, Q * b + Q), lanes)
            vv[here] = (silu(mixed) * av[here]).astype(BF16)

    project(early, 0)
    project(early, 1)
    pass_piece(0, to_b)

    @pl.when(ahead)
    def _():
        pass_piece(1, to_b)

    for at in range(2):
        project(late, at)
        value(early, 2 * at)
        value(early, 2 * at + 1)

    @pl.when(jnp.logical_not(ahead))
    def _():
        pass_piece(1, to_b)

    for at in range(2):
        pass_piece(at, -to_b)

    def mix(s, h):
        ahead = bhl[4 * h : 4 * h + 4].astype(F32).reshape(128, 128)
        ahead = jnp.where(s == 1, pltpu.roll(ahead, 64, 1), ahead)
        x = bct[s, 4 * h : 4 * h + 4].astype(F32).reshape(128, LEN)
        x = jnp.concatenate([ahead, x], axis=1)
        turned = [pltpu.roll(x, 3 - k, 1) for k in range(3)] + [x]
        blocks = []
        for b in range(NB):
            lanes = slice(128 + Q * b, 256 + Q * b)
            mixed = tap[h] * turned[0][:, lanes]
            for k in range(1, 4):
                mixed = mixed + tap[2 * k + h] * turned[k][:, lanes]
            blocks.append(silu(mixed))
        return blocks

    all_of(dall.at[0 : NS - 1], dsend, drecv).wait_recv()

    def pick(j, _):
        dxl[pl.ds(j, 1), :] = dall[2 * j, pl.ds(core, 1), :] + dall[2 * j + 1, pl.ds(core, 1), :]
        return 0

    lax.fori_loop(0, 16, pick, 0, unroll=True)
    dxl[16:17, :] = dall[2 * chip + 1, pl.ds(core, 1), :]
    dxl[24:32, :] = dall[2 * chip]
    dxl[17:24, :] = jnp.zeros((7, 128), F32)
    dx[...] = dot(split(jnp.exp(dxl[...])), ee[...])

    def states(s):
        for b, block in enumerate(mix(s, 0)):
            bmat[s, :, Q * b : Q * b + Q] = block.astype(BF16)
        state = None
        for b in range(NB):
            half = rx[s, b : b + 1, :]
            added = dot(bmat[s, :, Q * b : Q * b + Q], vv[s, Q * b : Q * b + Q, :]) * half
            if state is None:
                sbl[s, b] = jnp.zeros((128, CI), BF16)
                state = added
            else:
                lifted = state * half
                sbl[s, b] = lifted.astype(BF16)
                state = lifted * half + added
        for k in range(16):
            st[s, k] = state[8 * k : 8 * k + 8, :].astype(BF16)

    def across(s, n):
        return remote(st.at[s], so.at[s], cs.at[n], cr.at[n], seq=me + 1 - 2 * core)

    b_owners, c_owners = range(4), range(4, 8)
    all_of(bhl.at[0 : NZ - 1], bhs, bhr).wait_recv()
    rest_of_piece(0, b_owners)
    states(early)
    across(early, 0).start()
    for b in range(NB):
        value(late, b)
    rest_of_piece(1, b_owners)
    states(late)

    @pl.when(core == 0)
    def _():
        across(0, 1).start()

    def first_hop(source, k):
        return remote(agg.at[k], p1.at[source], s1, r1, seq=2 * k + core)

    across(late, 0).wait_recv()
    carry = dx[16:17, :]
    for k, own in chips:
        mine, other = st[late, k].astype(F32), so[late, k].astype(F32)
        slab = jnp.where(core == 0, mine, other) * carry + jnp.where(core == 0, other, mine)
        agg[k] = slab.astype(BF16)
        if own:
            p1[k] = agg[k]
        else:
            first_hop(chip, k).start()

    load_g.wait()

    def gate(s):
        for top, rows, at, wide in (
            (0, LEN, 0, 256),
            (0, LEN, 256, 256),
            (0, LEN // 2, 512, 128),
            (LEN // 2, LEN // 2, 512, 128),
        ):
            here = slice(top, top + rows)
            got = dot(hx[s, PAD + top : PAD + top + rows, :], w[:, 768 + at : 768 + at + wide])
            factor = dot(es[s, here, :], ee[:, at : at + wide])
            fg[s, here, at : at + wide] = silu(got) * factor

    gate(early)

    def within(s):
        for b, block in enumerate(mix(s, 1)):
            cmat[s, Q * b : Q * b + Q, :] = block.T.astype(BF16)
        for b in range(NB):
            rows = slice(Q * b, Q * b + Q)
            c_rows = cmat[s, rows, :]
            scores = dot(c_rows, bmat[s, :, rows])
            scores = jnp.where(tri_at, scores, 0.0).astype(BF16)
            left = jnp.concatenate([scores, c_rows], axis=1)
            right = jnp.concatenate([vv[s, rows, :], sbl[s, b]], axis=0)
            g[s, rows, :] = dot(left, right)

    rest_of_piece(0, c_owners)
    within(early)
    rest_of_piece(1, c_owners)
    within(late)

    all_of(p1.at[0:15], s1, r1).wait_recv()
    so_far = jnp.zeros((8, CI), F32)
    for j in range(16):
        po[j] = so_far.astype(BF16)
        so_far = so_far * dx[j : j + 1, :] + p1[j].astype(F32)

    def second_hop(target, source):
        slot = pin.at[late, source]
        return remote(po.at[target], slot, s2, r2, seq=2 * target + core)

    for k, own in chips:
        if own:
            pin[late, k] = po[k]
        else:
            second_hop(k, chip).start()

    gate(late)

    ones = jnp.ones((16, 128), BF16)
    at_row = lax.broadcasted_iota(jnp.int32, (8, 128), 0)
    squares = jnp.zeros((8, 128), F32)
    all_of(po.at[0:15], s2, r2).wait_recv()

    def back(s):
        return remote(pin.at[s], pin.at[s], cs.at[2], cr.at[2], seq=me + 1 - 2 * core)

    back(late).start()

    @pl.when(core == 1)
    def _():
        across(0, 1).wait_recv()

    for s in (late, early):
        if s is early:
            back(early).wait_recv()
        arrived = pin[s].astype(F32).reshape(128, CI)
        moved = arrived * dx[pl.ds(24 + s, 1), :] + so[s].astype(F32).reshape(128, CI)
        arrived = jnp.where(core == 1, moved, arrived).astype(BF16)
        given = dot(cmat[s], arrived)
        for b in range(NB):
            rows = slice(Q * b, Q * b + Q)
            gated = fg[s, rows, :] * (g[s, rows, :] + given[rows] * rx[s, 4 + b : 5 + b, :])
            g[s, rows, :] = gated
            sq = gated * gated
            sq = sum(sq[:, 128 * c : 128 * c + 128] for c in range(1, 5)) + sq[:, 0:128]
            summed = lax.dot_general(
                ones, sq.astype(BF16), (((1,), (1,)), ((), ())), preferred_element_type=F32
            )[0:8, :]
            squares = jnp.where(at_row == 4 * s + b, summed, squares)
    ssm[...] = squares

    def total_sq(owner, peer):
        return remote(ssm, ssa.at[owner], zs, zr, tp=peer)

    for step in far_first:
        total_sq(z, away(step)).start()
    ssa[z] = ssm[...]
    gains = gn[...].reshape(1, CI)
    for s in range(2):
        out[s] = (g[s] * gains).astype(BF16)

    all_of(bct.at[:, 0 : NZ - 1], bsend, bsend).wait_send()
    all_of(bhl.at[0 : NZ - 1], bhs, bhr).wait_send()
    all_of(dall.at[0 : NS - 1], dsend, drecv).wait_send()
    all_of(p1.at[0:15], s1, r1).wait_send()
    all_of(po.at[0:15], s2, r2).wait_send()
    across(early, 0).wait_send()
    back(late).wait_send()

    @pl.when(core == 0)
    def _():
        across(0, 1).wait_send()

    @pl.when(me < NS - 1)
    def _():
        halo().wait_send()

    all_of(ssa.at[0 : NZ - 1], zs, zr).wait_recv()
    rms[...] = lax.rsqrt(jnp.sum(ssa[...], axis=0) * (1.0 / DI) + EPS)
    all_of(ssa.at[0 : NZ - 1], zs, zr).wait_send()


def scaled(gated, rms, out, osc, sems):
    copies = []
    for s in range(2):
        for b in range(NB):
            n = NB * s + b
            rows = slice(Q * b, Q * b + Q)
            by_token = jnp.broadcast_to(rms[n : n + 1, :], (128, 128)).T
            for c in range(5):
                lanes = slice(128 * c, 128 * c + 128)
                osc[s, rows, lanes] = (gated[s, rows, lanes].astype(F32) * by_token).astype(BF16)
            copies.append(pltpu.make_async_copy(osc.at[s, rows], out.at[s, rows], sems.at[n]))
            copies[-1].start()
    for copy in copies:
        copy.wait()


def on_device(hid, gw, vw, bw, sw, vconv, bconv, sbias, lrate, gain):
    dma = pltpu.SemaphoreType.DMA
    vmem = pltpu.VMEM
    any_space = pl.BlockSpec(memory_space=pl.ANY)
    scratch = [
        vmem((2, PAD + LEN, D), BF16),
        vmem((D, 1408), BF16),
        vmem((32, D), BF16),
        vmem((HEADS, D), BF16),
        vmem((4, CI), F32),
        vmem((4, 256), F32),
        vmem((1, HEADS), F32),
        vmem((1, HEADS), F32),
        vmem((CI,), F32),
        vmem((8, 128), F32),
        vmem((8, 128, 128), F32),
        vmem((256, CI), BF16),
        vmem((2, LEN, 128), F32),
        vmem((2, 5, PAD + LEN, 128), F32),
        vmem((2, NZ, 32, LEN), BF16),
        vmem((2, LEN, 128), BF16),
        vmem((2, 128, LEN), BF16),
        vmem((2, LEN, CI), F32),
        vmem((2, LEN, 256), BF16),
        vmem((2, LEN, CI), F32),
        vmem((2, LEN, CI), F32),
        vmem((2, 8, CI), F32),
        vmem((8, 128), F32),
        vmem((NS, 8, 128), F32),
        vmem((NS, 128), F32),
        vmem((NS, CI), F32),
        vmem((NZ, 32, 128), BF16),
        vmem((2, LEN, CI), BF16),
        vmem((2, NB, 128, CI), BF16),
        vmem((2, 16, 8, CI), BF16),
        vmem((2, 16, 8, CI), BF16),
        vmem((16, 8, CI), BF16),
        vmem((16, 8, CI), BF16),
        vmem((16, 8, CI), BF16),
        vmem((2, 16, 8, CI), BF16),
        vmem((8, 128), F32),
        vmem((NZ, 8, 128), F32),
        dma((14,)),
        dma,
        dma,
        dma,
        dma((2, NZ)),
        dma,
        dma,
        dma,
        dma,
        dma,
        dma,
        dma,
        dma,
        dma,
        dma,
        dma((3,)),
        dma((3,)),
    ]
    in_vmem = pl.BlockSpec(memory_space=vmem)
    gated, rms = pl.pallas_call(
        kernel,
        out_shape=(vmem((2, LEN, CI), BF16), vmem((8, 128), F32)),
        in_specs=[any_space] * 10,
        out_specs=(in_vmem, in_vmem),
        scratch_shapes=scratch,
        compiler_params=pltpu.CompilerParams(
            collective_id=0, has_side_effects=True, vmem_limit_bytes=56 * 2**20
        ),
    )(
        hid, gw, vw, bw.T, sw.T, vconv, bconv,
        sbias.reshape(1, HEADS), lrate.reshape(1, HEADS), gain,
    )
    return pl.pallas_call(
        scaled,
        out_shape=jax.ShapeDtypeStruct((2, LEN, CI), BF16),
        in_specs=[in_vmem, in_vmem],
        out_specs=any_space,
        scratch_shapes=[vmem((2, LEN, CI), BF16), dma((2 * NB,))],
    )(*(pltpu.with_memory_space_constraint(x, vmem) for x in (gated, rms)))


def solution(mesh):
    placed = (
        P(None, "seq", None),
        P(None, "tp"),
        P(None, "tp"),
        P(None, "tp"),
        P(None, "tp"),
        P(None, "tp"),
        P(),
        P("tp"),
        P("tp"),
        P("tp"),
    )
    return jax.shard_map(
        on_device, mesh=mesh, in_specs=placed, out_specs=P(None, "seq", "tp"), check_vma=False
    )
```

```python
import jax
import jax.numpy as jnp
from jax import lax
from jax.experimental import pallas as pl
from jax.experimental.pallas import tpu as pltpu
from jax.sharding import PartitionSpec as P

MESH = pl.DeviceIdType.MESH
F32, BF16 = jnp.float32, jnp.bfloat16

NS, NZ = 32, 8
D, DI = 2560, 5120
CI = 640
LEN = 512
Q = 128
NB = LEN // Q
PAD = 16
HL = 32
HEADS = 10
EPS = 1e-05


def dot(a, b):
    return jnp.dot(a, b, preferred_element_type=F32)


def silu(x):
    half = 0.5 * x
    return half + half * jnp.tanh(half)


def split(x):
    high = x.astype(BF16)
    low = (x - high.astype(F32)).astype(BF16)
    return jnp.concatenate([high, low], axis=1)


def kernel(
    hid, gw, vw, bw, sw, vconv, bconv, sbias, lrate, gain, out, rms,
    hx, w, bwv, swv, cv, bcv, sb, lr, gn, prm, tap, ee, bs, vp, bct, cmat, bmat,
    av, es, fg, g, rx, dsum, dall, dxl, dx, bhl, vv, sbl, st, so, agg, p1, po, pin, ssm, ssa,
    ld, hs, hr, bsend, brecv, bhs, bhr, dsend, drecv, s1, r1, s2, r2, zs, zr, cs, cr,
):
    me, z = lax.axis_index("seq"), lax.axis_index("tp")
    core, chip = me & 1, lax.div(me, 2)
    early, late = 1 - core, core

    def remote(src, dst, ss, rs, seq=None, tp=None):
        where = {"seq": me if seq is None else seq, "tp": z if tp is None else tp}
        return pltpu.make_async_remote_copy(
            src_ref=src, dst_ref=dst, send_sem=ss, recv_sem=rs, device_id=where, device_id_type=MESH
        )

    barrier = pltpu.get_barrier_semaphore()

    def greet_seq(r, _):
        pl.semaphore_signal(
            barrier, inc=1, device_id={"seq": (me + r) & (NS - 1), "tp": z}, device_id_type=MESH
        )
        return 0

    def greet_tp(r, _):
        pl.semaphore_signal(
            barrier, inc=1, device_id={"seq": me, "tp": (z + r) & (NZ - 1)}, device_id_type=MESH
        )
        return 0

    lax.fori_loop(1, NZ, greet_tp, 0)

    small = [
        pltpu.make_async_copy(src, dst, ld.at[9 + n])
        for n, (src, dst) in enumerate(
            [(vconv, cv), (bconv, bcv), (sbias, sb), (lrate, lr), (gain, gn)]
        )
    ]
    load_b = pltpu.make_async_copy(bw, bwv, ld.at[0])
    load_s = pltpu.make_async_copy(sw, swv, ld.at[1])
    load_v0 = pltpu.make_async_copy(vw.at[:, 0:128], w.at[:, 128:256], ld.at[2])
    load_v1 = pltpu.make_async_copy(vw.at[:, 128:CI], w.at[:, 256:768], ld.at[7])
    load_g = pltpu.make_async_copy(gw, w.at[:, 768:1408], ld.at[8])

    def load_h(s, h):
        return pltpu.make_async_copy(
            hid.at[s, pl.ds(256 * h, 256)], hx.at[s, pl.ds(PAD + 256 * h, 256)], ld.at[3 + 2 * s + h]
        )

    load_b.start()
    load_s.start()
    for copy in small:
        copy.start()
    load_v0.start()
    for h in range(2):
        load_h(early, h).start()

    lax.fori_loop(1, NS, greet_seq, 0)

    row = lax.broadcasted_iota(jnp.int32, (256, CI), 0)
    col = lax.broadcasted_iota(jnp.int32, (256, CI), 1)
    ee[...] = jnp.where((row & 127) == HL + (col >> 6), 1.0, 0.0).astype(BF16)
    tri_at = lax.broadcasted_iota(jnp.int32, (Q, Q), 0) >= lax.broadcasted_iota(
        jnp.int32, (Q, Q), 1
    )
    tri = jnp.where(tri_at, 1.0, 0.0).astype(BF16)
    prm[...] = jnp.zeros((8, 128), F32)
    dsum[...] = jnp.zeros((8, 128), F32)
    for s in range(2):
        hx[s, 0:8, :] = jnp.zeros((8, D), BF16)

    @pl.when(me == 0)
    def _():
        for s in range(2):
            hx[s, 8:16, :] = jnp.zeros((8, D), BF16)

    for copy in small:
        copy.wait()
    prm[0:1, HL : HL + HEADS] = sb[...]
    prm[1:2, HL : HL + HEADS] = lr[...]
    for k in range(4):
        for h in range(2):
            taps = bcv[k : k + 1, 128 * h : 128 * h + 128]
            tap[2 * k + h] = jnp.broadcast_to(taps, (128, 128)).T
    load_b.wait()
    load_s.wait()
    for n in range(D // 128):
        lanes = slice(128 * n, 128 * n + 128)
        both = jnp.concatenate(
            [bwv[:, lanes].astype(F32), swv[:, lanes].astype(F32), jnp.zeros((86, 128), F32)], axis=0
        )
        w[lanes, 0:128] = both.T.astype(BF16)
    for h in range(2):
        load_h(late, h).start()
    load_v0.wait()

    def first(s):
        rows = 128 if s is early else 256
        for at in range(0, LEN, rows):
            if s is early and at % 256 == 0:
                load_h(s, at // 256).wait()
            got = dot(hx[s, PAD + at : PAD + at + rows, :], w[:, 0:256])
            bs[s, at : at + rows, :] = got[:, 0:128]
            vp[s, 0, PAD + at : PAD + at + rows, :] = got[:, 128:256]
        for b in range(NB):
            turned = bs[s, Q * b : Q * b + Q, :].T
            bct[s, z, :, Q * b : Q * b + Q] = turned[0:32, :].astype(BF16)

    def piece(p, owner, peer):
        if p == 2:
            return remote(bhl.at[owner], bhl.at[owner], bhs, bhr, tp=peer)
        part = bct.at[(early, late)[p], owner]
        return remote(part, part, bsend, brecv.at[p, owner], tp=peer)

    def away(n):
        return (z + n) & (NZ - 1)

    near = (2, -2, 1, -1)
    far_first = (4, 3, -3, 2, -2, 1, -1)
    to_b = jnp.where((z >= 2) & (z < 6), 1, -1)

    ahead = z < NZ // 2

    def send_piece(p, steps):
        for step in near[steps]:
            piece(p, z, away(step)).start()

    def pass_piece(p, way):
        owner = away(-2 * way)
        piece(p, owner, owner).wait_recv()
        piece(p, owner, away(way)).start()

        @pl.when(way == jnp.where(ahead, to_b, -to_b))
        def _():
            piece(p, owner, away(2 * way)).start()

    def rest_of_piece(p, owners):
        for owner in owners:
            gap = (owner - z) & (NZ - 1)

            @pl.when((gap != 0) & (gap != 2) & (gap != 6))
            def _():
                piece(p, owner, owner).wait_recv()

    def all_of(part, ss, rs):
        return remote(part, part, ss, rs, tp=away(1))

    def halo():
        return remote(hx.at[:, 520:528], hx.at[:, 8:16], hs, hr, seq=(me + 1) & (NS - 1))

    first(early)
    load_v1.start()
    for h in range(2):
        load_h(late, h).wait()

    @pl.when(ahead)
    def _():
        first(late)

    pl.semaphore_wait(barrier, NS - 1 + NZ - 1)

    @pl.when(me < NS - 1)
    def _():
        halo().start()

    send_piece(0, slice(0, 2))

    @pl.when(jnp.logical_not(ahead))
    def _():
        send_piece(0, slice(2, 4))
        first(late)

    load_g.start()

    @pl.when(ahead)
    def _():
        send_piece(1, slice(0, 2))
        send_piece(0, slice(2, 4))
        send_piece(1, slice(2, 4))

    lane = lax.broadcasted_iota(jnp.int32, (LEN, 128), 1)
    is_head = (lane >= HL) & (lane < HL + HEADS)
    rate = jnp.exp(prm[1:2, :])

    def steps(s):
        x = bs[s] + prm[0:1, :]
        size = jnp.maximum(x, 0.0) + jnp.log1p(jnp.exp(-jnp.abs(x)))
        size = jnp.where(is_head, size, 0.0)
        parts = split(-size * rate)
        so_far = jnp.zeros((1, 128), F32)
        halves, ahead, off = [], [], []
        for b in range(NB):
            sums = dot(tri, parts[Q * b : Q * b + Q, :])
            cum = sums[:, 0:128] + sums[:, 128:256]
            total = cum[Q - 1 : Q, :]
            mid = 0.5 * total
            off.append(cum - mid)
            halves.append(jnp.exp(mid))
            ahead.append(jnp.exp(so_far + mid))
            so_far = so_far + total
        off = jnp.concatenate(off, axis=0)
        av[s] = dot(split(size * jnp.exp(-off)), ee[...])
        es[s] = split(jnp.exp(off))
        rows = jnp.concatenate(halves + ahead + [jnp.zeros((8, 128), F32)], axis=0)
        rx[s] = dot(split(rows), ee[...])[0:8, :]
        dsum[pl.ds(s, 1), :] = so_far

    steps(early)
    steps(late)

    y, x = lax.div(chip, 4), chip & 3
    reach = [0, 1, 2, 1]
    offsets = sorted(
        ((dy, dx) for dy in range(4) for dx in range(4)), key=lambda o: -reach[o[0]] - reach[o[1]]
    )
    chips = [(((y + dy) & 3) * 4 + ((x + dx) & 3), (dy, dx) == (0, 0)) for dy, dx in offsets]
    others = [2 * c + n for c, own in chips for n in range(2) if not own] + [me + 1 - 2 * core]

    def decay(peer):
        return remote(dsum, dall.at[me], dsend, drecv, seq=peer)

    for peer in others:
        decay(peer).start()
    dall[me] = dsum[...]

    @pl.when(me > 0)
    def _():
        halo().wait_recv()

    both = jnp.concatenate([hx[0, 8:16, :], hx[1, 8:16, :]], axis=0)
    got = dot(both[:, : D // 2], w[: D // 2, 0:256]) + dot(both[:, D // 2 :], w[D // 2 :, 0:256])
    for s in range(2):
        vp[s, 0, 8:16, :] = got[8 * s : 8 * s + 8, 128:256]
    tail = jnp.concatenate([got[12:16, 0:128], got[4:8, 0:128]], axis=0)
    tail = jnp.where(lax.broadcasted_iota(jnp.int32, (8, 128), 1) < 32, tail, 0.0)
    bhl[z] = pltpu.roll(tail, 32 * (z & 3), 1).astype(BF16)
    for step in far_first:
        piece(2, z, away(step)).start()

    load_v1.wait()

    def project(s, at):
        got = dot(hx[s], w[:, 256 + 256 * at : 512 + 256 * at])
        vp[s, 1 + 2 * at] = got[:, 0:128]
        vp[s, 2 + 2 * at] = got[:, 128:256]

    def value(s, b):
        for c in range(5):
            lanes = slice(128 * c, 128 * c + 128)
            mixed = None
            for k in range(4):
                at = 13 + k + Q * b
                term = cv[k : k + 1, lanes] * vp[s, c, at : at + Q, :]
                mixed = term if mixed is None else mixed + term
            here = (s, slice(Q * b, Q * b + Q), lanes)
            vv[here] = (silu(mixed) * av[here]).astype(BF16)


    @pl.when(jnp.logical_not(ahead))
    def _():
        pass_piece(0, to_b)

    project(early, 0)
    project(early, 1)

    @pl.when(ahead)
    def _():
        pass_piece(0, to_b)

    pass_piece(1, to_b)

    @pl.when(jnp.logical_not(ahead))
    def _():
        send_piece(1, slice(0, 4))

    project(late, 0)
    project(late, 1)
    for b in range(NB):
        value(early, b)
    pass_piece(0, -to_b)

    def mix(s, h):
        rows = jnp.sum(bhl[4 * h : 4 * h + 4].astype(F32), axis=0)
        rows = jnp.where(s == 1, rows[0:4], rows[4:8])
        before = jnp.concatenate([jnp.zeros((124, 128), F32), rows], axis=0).T
        x = bct[s, 4 * h : 4 * h + 4].astype(F32).reshape(128, LEN)
        x = jnp.concatenate([before, x], axis=1)
        turned = [pltpu.roll(x, 3 - k, 1) for k in range(3)] + [x]
        blocks = []
        for b in range(NB):
            lanes = slice(128 + Q * b, 256 + Q * b)
            mixed = tap[h] * turned[0][:, lanes]
            for k in range(1, 4):
                mixed = mixed + tap[2 * k + h] * turned[k][:, lanes]
            blocks.append(silu(mixed))
        return blocks

    all_of(dall.at[0 : NS - 1], dsend, drecv).wait_recv()

    def pick(j, _):
        dxl[pl.ds(j, 1), :] = dall[2 * j, pl.ds(core, 1), :] + dall[2 * j + 1, pl.ds(core, 1), :]
        return 0

    lax.fori_loop(0, 16, pick, 0, unroll=True)
    dxl[16:17, :] = dall[2 * chip + 1, pl.ds(core, 1), :]
    dxl[24:32, :] = dall[2 * chip]
    dxl[17:24, :] = jnp.zeros((7, 128), F32)
    dx[...] = dot(split(jnp.exp(dxl[...])), ee[...])

    def states(s):
        for b, block in enumerate(mix(s, 0)):
            bmat[s, :, Q * b : Q * b + Q] = block.astype(BF16)
        state = None
        for b in range(NB):
            half = rx[s, b : b + 1, :]
            added = dot(bmat[s, :, Q * b : Q * b + Q], vv[s, Q * b : Q * b + Q, :]) * half
            if state is None:
                sbl[s, b] = jnp.zeros((128, CI), BF16)
                state = added
            else:
                lifted = state * half
                sbl[s, b] = lifted.astype(BF16)
                state = lifted * half + added
        for k in range(16):
            st[s, k] = state[8 * k : 8 * k + 8, :].astype(BF16)

    def across(s, n):
        return remote(st.at[s], so.at[s], cs.at[n], cr.at[n], seq=me + 1 - 2 * core)

    b_owners, c_owners = range(4), range(4, 8)
    all_of(bhl.at[0 : NZ - 1], bhs, bhr).wait_recv()
    rest_of_piece(0, b_owners)
    states(early)
    across(early, 0).start()
    for b in range(NB):
        value(late, b)
    rest_of_piece(1, b_owners)
    states(late)

    @pl.when(core == 0)
    def _():
        across(0, 1).start()

    def first_hop(source, k):
        return remote(agg.at[k], p1.at[source], s1, r1, seq=2 * k + core)

    across(late, 0).wait_recv()
    carry = dx[16:17, :]
    for k, own in chips:
        mine, other = st[late, k].astype(F32), so[late, k].astype(F32)
        slab = jnp.where(core == 0, mine, other) * carry + jnp.where(core == 0, other, mine)
        agg[k] = slab.astype(BF16)
        if own:
            p1[k] = agg[k]
        else:
            first_hop(chip, k).start()

    pass_piece(1, -to_b)

    load_g.wait()

    def gate(s):
        for top, rows, at, wide in (
            (0, LEN, 0, 256),
            (0, LEN, 256, 256),
            (0, LEN // 2, 512, 128),
            (LEN // 2, LEN // 2, 512, 128),
        ):
            here = slice(top, top + rows)
            got = dot(hx[s, PAD + top : PAD + top + rows, :], w[:, 768 + at : 768 + at + wide])
            factor = dot(es[s, here, :], ee[:, at : at + wide])
            fg[s, here, at : at + wide] = silu(got) * factor

    gate(early)

    def within(s):
        for b, block in enumerate(mix(s, 1)):
            cmat[s, Q * b : Q * b + Q, :] = block.T.astype(BF16)
        for b in range(NB):
            rows = slice(Q * b, Q * b + Q)
            c_rows = cmat[s, rows, :]
            scores = dot(c_rows, bmat[s, :, rows])
            scores = jnp.where(tri_at, scores, 0.0).astype(BF16)
            left = jnp.concatenate([scores, c_rows], axis=1)
            right = jnp.concatenate([vv[s, rows, :], sbl[s, b]], axis=0)
            g[s, rows, :] = dot(left, right)

    rest_of_piece(0, c_owners)
    within(early)

    all_of(p1.at[0:15], s1, r1).wait_recv()
    so_far = jnp.zeros((8, CI), F32)
    for j in range(16):
        po[j] = so_far.astype(BF16)
        so_far = so_far * dx[j : j + 1, :] + p1[j].astype(F32)

    def second_hop(target, source):
        slot = pin.at[late, source]
        return remote(po.at[target], slot, s2, r2, seq=2 * target + core)

    for k, own in chips:
        if own:
            pin[late, k] = po[k]
        else:
            second_hop(k, chip).start()

    rest_of_piece(1, c_owners)
    within(late)
    gate(late)

    ones = jnp.ones((16, 128), BF16)
    at_row = lax.broadcasted_iota(jnp.int32, (8, 128), 0)
    squares = jnp.zeros((8, 128), F32)
    all_of(po.at[0:15], s2, r2).wait_recv()

    def back(s):
        return remote(pin.at[s], pin.at[s], cs.at[2], cr.at[2], seq=me + 1 - 2 * core)

    back(late).start()

    @pl.when(core == 1)
    def _():
        across(0, 1).wait_recv()

    for s in (late, early):
        if s is early:
            back(early).wait_recv()
        arrived = pin[s].astype(F32).reshape(128, CI)
        moved = arrived * dx[pl.ds(24 + s, 1), :] + so[s].astype(F32).reshape(128, CI)
        arrived = jnp.where(core == 1, moved, arrived).astype(BF16)
        given = dot(cmat[s], arrived)
        for b in range(NB):
            rows = slice(Q * b, Q * b + Q)
            gated = fg[s, rows, :] * (g[s, rows, :] + given[rows] * rx[s, 4 + b : 5 + b, :])
            g[s, rows, :] = gated
            sq = gated * gated
            sq = sum(sq[:, 128 * c : 128 * c + 128] for c in range(1, 5)) + sq[:, 0:128]
            summed = lax.dot_general(
                ones, sq.astype(BF16), (((1,), (1,)), ((), ())), preferred_element_type=F32
            )[0:8, :]
            squares = jnp.where(at_row == 4 * s + b, summed, squares)
    ssm[...] = squares

    def total_sq(owner, peer):
        return remote(ssm, ssa.at[owner], zs, zr, tp=peer)

    for step in far_first:
        total_sq(z, away(step)).start()
    ssa[z] = ssm[...]
    gains = gn[...].reshape(1, CI)
    for s in range(2):
        out[s] = (g[s] * gains).astype(BF16)

    all_of(bct.at[:, 0 : NZ - 1], bsend, bsend).wait_send()
    all_of(bhl.at[0 : NZ - 1], bhs, bhr).wait_send()
    all_of(dall.at[0 : NS - 1], dsend, drecv).wait_send()
    all_of(p1.at[0:15], s1, r1).wait_send()
    all_of(po.at[0:15], s2, r2).wait_send()
    across(early, 0).wait_send()
    back(late).wait_send()

    @pl.when(core == 0)
    def _():
        across(0, 1).wait_send()

    @pl.when(me < NS - 1)
    def _():
        halo().wait_send()

    all_of(ssa.at[0 : NZ - 1], zs, zr).wait_recv()
    rms[...] = lax.rsqrt(jnp.sum(ssa[...], axis=0) * (1.0 / DI) + EPS)
    all_of(ssa.at[0 : NZ - 1], zs, zr).wait_send()


def scaled(gated, rms, out, osc, sems):
    copies = []
    for s in range(2):
        for b in range(NB):
            n = NB * s + b
            rows = slice(Q * b, Q * b + Q)
            by_token = jnp.broadcast_to(rms[n : n + 1, :], (128, 128)).T
            for c in range(5):
                lanes = slice(128 * c, 128 * c + 128)
                osc[s, rows, lanes] = (gated[s, rows, lanes].astype(F32) * by_token).astype(BF16)
            copies.append(pltpu.make_async_copy(osc.at[s, rows], out.at[s, rows], sems.at[n]))
            copies[-1].start()
    for copy in copies:
        copy.wait()


def on_device(hid, gw, vw, bw, sw, vconv, bconv, sbias, lrate, gain):
    dma = pltpu.SemaphoreType.DMA
    vmem = pltpu.VMEM
    any_space = pl.BlockSpec(memory_space=pl.ANY)
    scratch = [
        vmem((2, PAD + LEN, D), BF16),
        vmem((D, 1408), BF16),
        vmem((32, D), BF16),
        vmem((HEADS, D), BF16),
        vmem((4, CI), F32),
        vmem((4, 256), F32),
        vmem((1, HEADS), F32),
        vmem((1, HEADS), F32),
        vmem((CI,), F32),
        vmem((8, 128), F32),
        vmem((8, 128, 128), F32),
        vmem((256, CI), BF16),
        vmem((2, LEN, 128), F32),
        vmem((2, 5, PAD + LEN, 128), F32),
        vmem((2, NZ, 32, LEN), BF16),
        vmem((2, LEN, 128), BF16),
        vmem((2, 128, LEN), BF16),
        vmem((2, LEN, CI), F32),
        vmem((2, LEN, 256), BF16),
        vmem((2, LEN, CI), F32),
        vmem((2, LEN, CI), F32),
        vmem((2, 8, CI), F32),
        vmem((8, 128), F32),
        vmem((NS, 8, 128), F32),
        vmem((NS, 128), F32),
        vmem((NS, CI), F32),
        vmem((NZ, 8, 128), BF16),
        vmem((2, LEN, CI), BF16),
        vmem((2, NB, 128, CI), BF16),
        vmem((2, 16, 8, CI), BF16),
        vmem((2, 16, 8, CI), BF16),
        vmem((16, 8, CI), BF16),
        vmem((16, 8, CI), BF16),
        vmem((16, 8, CI), BF16),
        vmem((2, 16, 8, CI), BF16),
        vmem((8, 128), F32),
        vmem((NZ, 8, 128), F32),
        dma((14,)),
        dma,
        dma,
        dma,
        dma((2, NZ)),
        dma,
        dma,
        dma,
        dma,
        dma,
        dma,
        dma,
        dma,
        dma,
        dma,
        dma((3,)),
        dma((3,)),
    ]
    in_vmem = pl.BlockSpec(memory_space=vmem)
    gated, rms = pl.pallas_call(
        kernel,
        out_shape=(vmem((2, LEN, CI), BF16), vmem((8, 128), F32)),
        in_specs=[any_space] * 10,
        out_specs=(in_vmem, in_vmem),
        scratch_shapes=scratch,
        compiler_params=pltpu.CompilerParams(
            collective_id=0, has_side_effects=True, vmem_limit_bytes=56 * 2**20
        ),
    )(
        hid, gw, vw, bw.T, sw.T, vconv, bconv,
        sbias.reshape(1, HEADS), lrate.reshape(1, HEADS), gain,
    )
    return pl.pallas_call(
        scaled,
        out_shape=jax.ShapeDtypeStruct((2, LEN, CI), BF16),
        in_specs=[in_vmem, in_vmem],
        out_specs=any_space,
        scratch_shapes=[vmem((2, LEN, CI), BF16), dma((2 * NB,))],
    )(*(pltpu.with_memory_space_constraint(x, vmem) for x in (gated, rms)))


def solution(mesh):
    placed = (
        P(None, "seq", None),
        P(None, "tp"),
        P(None, "tp"),
        P(None, "tp"),
        P(None, "tp"),
        P(None, "tp"),
        P(),
        P("tp"),
        P("tp"),
        P("tp"),
    )
    return jax.shard_map(
        on_device, mesh=mesh, in_specs=placed, out_specs=P(None, "seq", "tp"), check_vma=False
    )
```

```python
import jax
import jax.numpy as jnp
from jax import lax
from jax.experimental import pallas as pl
from jax.experimental.pallas import tpu as pltpu
from jax.sharding import PartitionSpec as P

MESH = pl.DeviceIdType.MESH
F32, BF16 = jnp.float32, jnp.bfloat16

NS, NZ = 32, 8
D, DI = 2560, 5120
CI = 640
LEN = 512
Q = 128
NB = LEN // Q
PAD = 16
HL = 32
HEADS = 10
EPS = 1e-05


def dot(a, b):
    return jnp.dot(a, b, preferred_element_type=F32)


def silu(x):
    half = 0.5 * x
    return half + half * jnp.tanh(half)


def split(x):
    high = x.astype(BF16)
    low = (x - high.astype(F32)).astype(BF16)
    return jnp.concatenate([high, low], axis=1)


def kernel(
    hid, gw, vw, bw, sw, vconv, bconv, sbias, lrate, gain, out, rms,
    hx, w, bwv, swv, cv, bcv, sb, lr, gn, prm, tap, ee, bs, vp, bct, cmat, bmat,
    av, es, fg, g, rx, dsum, dall, dxl, dx, bhl, vv, sbl, st, so, agg, p1, po, pin, ssm, ssa,
    ld, hs, hr, bsend, brecv, bhs, bhr, dsend, drecv, s1, r1, s2, r2, zs, zr, cs, cr,
):
    me, z = lax.axis_index("seq"), lax.axis_index("tp")
    core, chip = me & 1, lax.div(me, 2)
    early, late = 1 - core, core

    def remote(src, dst, ss, rs, seq=None, tp=None):
        where = {"seq": me if seq is None else seq, "tp": z if tp is None else tp}
        return pltpu.make_async_remote_copy(
            src_ref=src, dst_ref=dst, send_sem=ss, recv_sem=rs, device_id=where, device_id_type=MESH
        )

    barrier = pltpu.get_barrier_semaphore()

    def greet_seq(r, _):
        pl.semaphore_signal(
            barrier, inc=1, device_id={"seq": (me + r) & (NS - 1), "tp": z}, device_id_type=MESH
        )
        return 0

    def greet_tp(r, _):
        pl.semaphore_signal(
            barrier, inc=1, device_id={"seq": me, "tp": (z + r) & (NZ - 1)}, device_id_type=MESH
        )
        return 0

    lax.fori_loop(1, NZ, greet_tp, 0)

    small = [
        pltpu.make_async_copy(src, dst, ld.at[8 + n])
        for n, (src, dst) in enumerate(
            [(vconv, cv), (bconv, bcv), (sbias, sb), (lrate, lr), (gain, gn)]
        )
    ]
    load_b = pltpu.make_async_copy(bw, bwv, ld.at[0])
    load_s = pltpu.make_async_copy(sw, swv, ld.at[1])
    load_v0 = pltpu.make_async_copy(vw.at[:, 0:128], w.at[:, 128:256], ld.at[2])
    load_v1 = pltpu.make_async_copy(vw.at[:, 128:CI], w.at[:, 256:768], ld.at[6])
    load_g = pltpu.make_async_copy(gw, w.at[:, 768:1408], ld.at[7])

    def load_h(s, h):
        return pltpu.make_async_copy(
            hid.at[s, pl.ds(256 * h, 256)], hx.at[s, pl.ds(PAD + 256 * h, 256)], ld.at[3 + h]
        )

    load_b.start()
    load_s.start()
    for copy in small:
        copy.start()
    load_v0.start()
    for h in range(2):
        load_h(early, h).start()

    lax.fori_loop(1, NS, greet_seq, 0)

    row = lax.broadcasted_iota(jnp.int32, (256, CI), 0)
    col = lax.broadcasted_iota(jnp.int32, (256, CI), 1)
    ee[...] = jnp.where((row & 127) == HL + (col >> 6), 1.0, 0.0).astype(BF16)
    tri_at = lax.broadcasted_iota(jnp.int32, (Q, Q), 0) >= lax.broadcasted_iota(
        jnp.int32, (Q, Q), 1
    )
    tri = jnp.where(tri_at, 1.0, 0.0).astype(BF16)
    prm[...] = jnp.zeros((8, 128), F32)
    dsum[...] = jnp.zeros((8, 128), F32)
    for s in range(2):
        hx[s, 0:8, :] = jnp.zeros((8, D), BF16)

    @pl.when(me == 0)
    def _():
        for s in range(2):
            hx[s, 8:16, :] = jnp.zeros((8, D), BF16)

    for copy in small:
        copy.wait()
    prm[0:1, HL : HL + HEADS] = sb[...]
    prm[1:2, HL : HL + HEADS] = lr[...]
    for k in range(4):
        for h in range(2):
            taps = bcv[k : k + 1, 128 * h : 128 * h + 128]
            tap[2 * k + h] = jnp.broadcast_to(taps, (128, 128)).T
    load_b.wait()
    load_s.wait()
    for n in range(D // 128):
        lanes = slice(128 * n, 128 * n + 128)
        both = jnp.concatenate(
            [bwv[:, lanes].astype(F32), swv[:, lanes].astype(F32), jnp.zeros((86, 128), F32)], axis=0
        )
        w[lanes, 0:128] = both.T.astype(BF16)
    load_late = pltpu.make_async_copy(hid.at[late], hx.at[late, PAD : PAD + LEN], ld.at[5])
    load_late.start()
    load_v0.wait()

    def first(s):
        rows = 128 if s is early else 256
        for at in range(0, LEN, rows):
            if s is early and at % 256 == 0:
                load_h(s, at // 256).wait()
            got = dot(hx[s, PAD + at : PAD + at + rows, :], w[:, 0:256])
            bs[s, at : at + rows, :] = got[:, 0:128]
            vp[s, 0, PAD + at : PAD + at + rows, :] = got[:, 128:256]
        for b in range(NB):
            turned = bs[s, Q * b : Q * b + Q, :].T
            bct[s, z, :, Q * b : Q * b + Q] = turned[0:32, :].astype(BF16)

    def piece(p, owner, peer):
        if p == 2:
            return remote(bhl.at[owner], bhl.at[owner], bhs, bhr, tp=peer)
        part = bct.at[(early, late)[p], owner]
        return remote(part, part, bsend, brecv.at[p, owner], tp=peer)

    def away(n):
        return (z + n) & (NZ - 1)

    near = (2, -2, 1, -1)
    far_first = (4, 3, -3, 2, -2, 1, -1)
    to_b = jnp.where((z >= 2) & (z < 6), 1, -1)

    ahead = z < NZ // 2

    def send_piece(p, steps):
        for step in near[steps]:
            piece(p, z, away(step)).start()

    def pass_piece(p, way):
        owner = away(-2 * way)
        piece(p, owner, owner).wait_recv()
        piece(p, owner, away(way)).start()

        @pl.when(way == jnp.where(ahead, to_b, -to_b))
        def _():
            piece(p, owner, away(2 * way)).start()

    def rest_of_piece(p, owners):
        for owner in owners:
            gap = (owner - z) & (NZ - 1)

            @pl.when((gap != 0) & (gap != 2) & (gap != 6))
            def _():
                piece(p, owner, owner).wait_recv()

    def all_of(part, ss, rs):
        return remote(part, part, ss, rs, tp=away(1))

    def halo():
        return remote(hx.at[:, 520:528], hx.at[:, 8:16], hs, hr, seq=(me + 1) & (NS - 1))

    first(early)
    load_v1.start()
    load_late.wait()

    @pl.when(ahead)
    def _():
        first(late)

    pl.semaphore_wait(barrier, NS - 1 + NZ - 1)

    @pl.when(me < NS - 1)
    def _():
        halo().start()

    send_piece(0, slice(0, 2))

    @pl.when(jnp.logical_not(ahead))
    def _():
        send_piece(0, slice(2, 4))
        first(late)

    load_g.start()

    @pl.when(ahead)
    def _():
        send_piece(0, slice(2, 4))
        send_piece(1, slice(0, 4))

    lane = lax.broadcasted_iota(jnp.int32, (LEN, 128), 1)
    is_head = (lane >= HL) & (lane < HL + HEADS)
    rate = jnp.exp(prm[1:2, :])

    def steps(s):
        x = bs[s] + prm[0:1, :]
        size = jnp.maximum(x, 0.0) + jnp.log1p(jnp.exp(-jnp.abs(x)))
        size = jnp.where(is_head, size, 0.0)
        parts = split(-size * rate)
        so_far = jnp.zeros((1, 128), F32)
        halves, ahead, off = [], [], []
        for b in range(NB):
            sums = dot(tri, parts[Q * b : Q * b + Q, :])
            cum = sums[:, 0:128] + sums[:, 128:256]
            total = cum[Q - 1 : Q, :]
            mid = 0.5 * total
            off.append(cum - mid)
            halves.append(jnp.exp(mid))
            ahead.append(jnp.exp(so_far + mid))
            so_far = so_far + total
        off = jnp.concatenate(off, axis=0)
        av[s] = dot(split(size * jnp.exp(-off)), ee[...])
        es[s] = split(jnp.exp(off))
        rows = jnp.concatenate(halves + ahead + [jnp.zeros((8, 128), F32)], axis=0)
        rx[s] = dot(split(rows), ee[...])[0:8, :]
        dsum[pl.ds(s, 1), :] = so_far

    steps(early)
    steps(late)

    y, x = lax.div(chip, 4), chip & 3
    reach = [0, 1, 2, 1]
    offsets = sorted(
        ((dy, dx) for dy in range(4) for dx in range(4)), key=lambda o: -reach[o[0]] - reach[o[1]]
    )
    chips = [(((y + dy) & 3) * 4 + ((x + dx) & 3), (dy, dx) == (0, 0)) for dy, dx in offsets]
    others = [2 * c + n for c, own in chips for n in range(2) if not own] + [me + 1 - 2 * core]

    def decay(peer):
        return remote(dsum, dall.at[me], dsend, drecv, seq=peer)

    for peer in others:
        decay(peer).start()
    dall[me] = dsum[...]

    @pl.when(me > 0)
    def _():
        halo().wait_recv()

    both = jnp.concatenate([hx[0, 8:16, :], hx[1, 8:16, :]], axis=0)
    got = dot(both[:, : D // 2], w[: D // 2, 0:256]) + dot(both[:, D // 2 :], w[D // 2 :, 0:256])
    for s in range(2):
        vp[s, 0, 8:16, :] = got[8 * s : 8 * s + 8, 128:256]
    tail = jnp.concatenate([got[12:16, 0:128], got[4:8, 0:128]], axis=0)
    tail = jnp.where(lax.broadcasted_iota(jnp.int32, (8, 128), 1) < 32, tail, 0.0)
    bhl[z] = pltpu.roll(tail, 32 * (z & 3), 1).astype(BF16)
    for step in far_first:
        piece(2, z, away(step)).start()

    load_v1.wait()

    def project(s, at):
        got = dot(hx[s], w[:, 256 + 256 * at : 512 + 256 * at])
        vp[s, 1 + 2 * at] = got[:, 0:128]
        vp[s, 2 + 2 * at] = got[:, 128:256]

    def value(s, b):
        for c in range(5):
            lanes = slice(128 * c, 128 * c + 128)
            mixed = None
            for k in range(4):
                at = 13 + k + Q * b
                term = cv[k : k + 1, lanes] * vp[s, c, at : at + Q, :]
                mixed = term if mixed is None else mixed + term
            here = (s, slice(Q * b, Q * b + Q), lanes)
            vv[here] = (silu(mixed) * av[here]).astype(BF16)


    @pl.when(jnp.logical_not(ahead))
    def _():
        pass_piece(0, to_b)

    project(early, 0)
    project(early, 1)

    @pl.when(ahead)
    def _():
        pass_piece(0, to_b)

    pass_piece(1, to_b)

    @pl.when(jnp.logical_not(ahead))
    def _():
        send_piece(1, slice(0, 4))

    project(late, 0)
    project(late, 1)
    for b in range(NB):
        value(early, b)
    pass_piece(0, -to_b)

    def mix(s, h):
        rows = jnp.sum(bhl[4 * h : 4 * h + 4].astype(F32), axis=0)
        rows = jnp.where(s == 1, rows[0:4], rows[4:8])
        before = jnp.concatenate([jnp.zeros((124, 128), F32), rows], axis=0).T
        x = bct[s, 4 * h : 4 * h + 4].astype(F32).reshape(128, LEN)
        x = jnp.concatenate([before, x], axis=1)
        turned = [pltpu.roll(x, 3 - k, 1) for k in range(3)] + [x]
        blocks = []
        for b in range(NB):
            lanes = slice(128 + Q * b, 256 + Q * b)
            mixed = tap[h] * turned[0][:, lanes]
            for k in range(1, 4):
                mixed = mixed + tap[2 * k + h] * turned[k][:, lanes]
            blocks.append(silu(mixed))
        return blocks

    all_of(dall.at[0 : NS - 1], dsend, drecv).wait_recv()

    def pick(j, _):
        dxl[pl.ds(j, 1), :] = dall[2 * j, pl.ds(core, 1), :] + dall[2 * j + 1, pl.ds(core, 1), :]
        return 0

    lax.fori_loop(0, 16, pick, 0, unroll=True)
    dxl[16:17, :] = dall[2 * chip + 1, pl.ds(core, 1), :]
    dxl[24:32, :] = dall[2 * chip]
    dxl[17:24, :] = jnp.zeros((7, 128), F32)
    dx[...] = dot(split(jnp.exp(dxl[...])), ee[...])

    def states(s):
        for b, block in enumerate(mix(s, 0)):
            bmat[s, :, Q * b : Q * b + Q] = block.astype(BF16)
        state = None
        for b in range(NB):
            half = rx[s, b : b + 1, :]
            added = dot(bmat[s, :, Q * b : Q * b + Q], vv[s, Q * b : Q * b + Q, :]) * half
            if state is None:
                sbl[s, b] = jnp.zeros((128, CI), BF16)
                state = added
            else:
                lifted = state * half
                sbl[s, b] = lifted.astype(BF16)
                state = lifted * half + added
        for k in range(16):
            st[s, k] = state[8 * k : 8 * k + 8, :].astype(BF16)

    def across(s, n):
        return remote(st.at[s], so.at[s], cs.at[n], cr.at[n], seq=me + 1 - 2 * core)

    b_owners, c_owners = range(4), range(4, 8)
    all_of(bhl.at[0 : NZ - 1], bhs, bhr).wait_recv()
    rest_of_piece(0, b_owners)
    states(early)
    across(early, 0).start()
    for b in range(NB):
        value(late, b)
    rest_of_piece(1, b_owners)
    states(late)

    @pl.when(core == 0)
    def _():
        across(0, 1).start()

    def first_hop(source, k):
        return remote(agg.at[k], p1.at[source], s1, r1, seq=2 * k + core)

    across(late, 0).wait_recv()
    carry = dx[16:17, :]
    for k, own in chips:
        mine, other = st[late, k].astype(F32), so[late, k].astype(F32)
        slab = jnp.where(core == 0, mine, other) * carry + jnp.where(core == 0, other, mine)
        agg[k] = slab.astype(BF16)
        if own:
            p1[k] = agg[k]
        else:
            first_hop(chip, k).start()

    pass_piece(1, -to_b)

    load_g.wait()

    def gate(s):
        for top, rows, at, wide in (
            (0, LEN, 0, 256),
            (0, LEN, 256, 256),
            (0, LEN // 2, 512, 128),
            (LEN // 2, LEN // 2, 512, 128),
        ):
            here = slice(top, top + rows)
            got = dot(hx[s, PAD + top : PAD + top + rows, :], w[:, 768 + at : 768 + at + wide])
            factor = dot(es[s, here, :], ee[:, at : at + wide])
            fg[s, here, at : at + wide] = silu(got) * factor

    gate(early)

    def within(s):
        for b, block in enumerate(mix(s, 1)):
            cmat[s, Q * b : Q * b + Q, :] = block.T.astype(BF16)
        for b in range(NB):
            rows = slice(Q * b, Q * b + Q)
            c_rows = cmat[s, rows, :]
            scores = dot(c_rows, bmat[s, :, rows])
            scores = jnp.where(tri_at, scores, 0.0).astype(BF16)
            left = jnp.concatenate([scores, c_rows], axis=1)
            right = jnp.concatenate([vv[s, rows, :], sbl[s, b]], axis=0)
            g[s, rows, :] = dot(left, right)

    rest_of_piece(0, c_owners)
    within(early)

    all_of(p1.at[0:15], s1, r1).wait_recv()
    so_far = jnp.zeros((8, CI), F32)
    for j in range(16):
        po[j] = so_far.astype(BF16)
        so_far = so_far * dx[j : j + 1, :] + p1[j].astype(F32)

    def second_hop(target, source):
        slot = pin.at[late, source]
        return remote(po.at[target], slot, s2, r2, seq=2 * target + core)

    for k, own in chips:
        if own:
            pin[late, k] = po[k]
        else:
            second_hop(k, chip).start()

    rest_of_piece(1, c_owners)
    within(late)
    gate(late)

    ones = jnp.ones((16, 128), BF16)
    at_row = lax.broadcasted_iota(jnp.int32, (8, 128), 0)
    squares = jnp.zeros((8, 128), F32)
    all_of(po.at[0:15], s2, r2).wait_recv()

    def back(s):
        return remote(pin.at[s], pin.at[s], cs.at[2], cr.at[2], seq=me + 1 - 2 * core)

    back(late).start()

    @pl.when(core == 1)
    def _():
        across(0, 1).wait_recv()

    for s in (late, early):
        if s is early:
            back(early).wait_recv()
        arrived = pin[s].astype(F32).reshape(128, CI)
        moved = arrived * dx[pl.ds(24 + s, 1), :] + so[s].astype(F32).reshape(128, CI)
        arrived = jnp.where(core == 1, moved, arrived).astype(BF16)
        given = dot(cmat[s], arrived)
        for b in range(NB):
            rows = slice(Q * b, Q * b + Q)
            gated = fg[s, rows, :] * (g[s, rows, :] + given[rows] * rx[s, 4 + b : 5 + b, :])
            g[s, rows, :] = gated
            sq = gated * gated
            sq = sum(sq[:, 128 * c : 128 * c + 128] for c in range(1, 5)) + sq[:, 0:128]
            summed = lax.dot_general(
                ones, sq.astype(BF16), (((1,), (1,)), ((), ())), preferred_element_type=F32
            )[0:8, :]
            squares = jnp.where(at_row == 4 * s + b, summed, squares)
    ssm[...] = squares

    def total_sq(owner, peer):
        return remote(ssm, ssa.at[owner], zs, zr, tp=peer)

    for step in far_first:
        total_sq(z, away(step)).start()
    ssa[z] = ssm[...]
    gains = gn[...].reshape(1, CI)
    for s in range(2):
        out[s] = (g[s] * gains).astype(BF16)

    all_of(bct.at[:, 0 : NZ - 1], bsend, bsend).wait_send()
    all_of(bhl.at[0 : NZ - 1], bhs, bhr).wait_send()
    all_of(dall.at[0 : NS - 1], dsend, drecv).wait_send()
    all_of(p1.at[0:15], s1, r1).wait_send()
    all_of(po.at[0:15], s2, r2).wait_send()
    across(early, 0).wait_send()
    back(late).wait_send()

    @pl.when(core == 0)
    def _():
        across(0, 1).wait_send()

    @pl.when(me < NS - 1)
    def _():
        halo().wait_send()

    all_of(ssa.at[0 : NZ - 1], zs, zr).wait_recv()
    rms[...] = lax.rsqrt(jnp.sum(ssa[...], axis=0) * (1.0 / DI) + EPS)
    all_of(ssa.at[0 : NZ - 1], zs, zr).wait_send()


def scaled(gated, rms, out, osc, sems):
    copies = []
    for s in range(2):
        for b in range(NB):
            n = NB * s + b
            rows = slice(Q * b, Q * b + Q)
            by_token = jnp.broadcast_to(rms[n : n + 1, :], (128, 128)).T
            for c in range(5):
                lanes = slice(128 * c, 128 * c + 128)
                osc[s, rows, lanes] = (gated[s, rows, lanes].astype(F32) * by_token).astype(BF16)
            if b % 2:
                pair = slice(Q * b - Q, Q * b + Q)
                copies.append(pltpu.make_async_copy(osc.at[s, pair], out.at[s, pair], sems.at[n // 2]))
                copies[-1].start()
    for copy in copies:
        copy.wait()


def on_device(hid, gw, vw, bw, sw, vconv, bconv, sbias, lrate, gain):
    dma = pltpu.SemaphoreType.DMA
    vmem = pltpu.VMEM
    any_space = pl.BlockSpec(memory_space=pl.ANY)
    scratch = [
        vmem((2, PAD + LEN, D), BF16),
        vmem((D, 1408), BF16),
        vmem((32, D), BF16),
        vmem((HEADS, D), BF16),
        vmem((4, CI), F32),
        vmem((4, 256), F32),
        vmem((1, HEADS), F32),
        vmem((1, HEADS), F32),
        vmem((CI,), F32),
        vmem((8, 128), F32),
        vmem((8, 128, 128), F32),
        vmem((256, CI), BF16),
        vmem((2, LEN, 128), F32),
        vmem((2, 5, PAD + LEN, 128), F32),
        vmem((2, NZ, 32, LEN), BF16),
        vmem((2, LEN, 128), BF16),
        vmem((2, 128, LEN), BF16),
        vmem((2, LEN, CI), F32),
        vmem((2, LEN, 256), BF16),
        vmem((2, LEN, CI), F32),
        vmem((2, LEN, CI), F32),
        vmem((2, 8, CI), F32),
        vmem((8, 128), F32),
        vmem((NS, 8, 128), F32),
        vmem((NS, 128), F32),
        vmem((NS, CI), F32),
        vmem((NZ, 8, 128), BF16),
        vmem((2, LEN, CI), BF16),
        vmem((2, NB, 128, CI), BF16),
        vmem((2, 16, 8, CI), BF16),
        vmem((2, 16, 8, CI), BF16),
        vmem((16, 8, CI), BF16),
        vmem((16, 8, CI), BF16),
        vmem((16, 8, CI), BF16),
        vmem((2, 16, 8, CI), BF16),
        vmem((8, 128), F32),
        vmem((NZ, 8, 128), F32),
        dma((13,)),
        dma,
        dma,
        dma,
        dma((2, NZ)),
        dma,
        dma,
        dma,
        dma,
        dma,
        dma,
        dma,
        dma,
        dma,
        dma,
        dma((3,)),
        dma((3,)),
    ]
    in_vmem = pl.BlockSpec(memory_space=vmem)
    gated, rms = pl.pallas_call(
        kernel,
        out_shape=(vmem((2, LEN, CI), BF16), vmem((8, 128), F32)),
        in_specs=[any_space] * 10,
        out_specs=(in_vmem, in_vmem),
        scratch_shapes=scratch,
        compiler_params=pltpu.CompilerParams(
            collective_id=0, has_side_effects=True, vmem_limit_bytes=56 * 2**20
        ),
    )(
        hid, gw, vw, bw.T, sw.T, vconv, bconv,
        sbias.reshape(1, HEADS), lrate.reshape(1, HEADS), gain,
    )
    return pl.pallas_call(
        scaled,
        out_shape=jax.ShapeDtypeStruct((2, LEN, CI), BF16),
        in_specs=[in_vmem, in_vmem],
        out_specs=any_space,
        scratch_shapes=[vmem((2, LEN, CI), BF16), dma((NB,))],
    )(*(pltpu.with_memory_space_constraint(x, vmem) for x in (gated, rms)))


def solution(mesh):
    placed = (
        P(None, "seq", None),
        P(None, "tp"),
        P(None, "tp"),
        P(None, "tp"),
        P(None, "tp"),
        P(None, "tp"),
        P(),
        P("tp"),
        P("tp"),
        P("tp"),
    )
    return jax.shard_map(
        on_device, mesh=mesh, in_specs=placed, out_specs=P(None, "seq", "tp"), check_vma=False
    )
```

```python
import jax
import jax.numpy as jnp
from jax import lax
from jax.experimental import pallas as pl
from jax.experimental.pallas import tpu as pltpu
from jax.sharding import PartitionSpec as P

MESH = pl.DeviceIdType.MESH
F32, BF16 = jnp.float32, jnp.bfloat16

NS, NZ = 32, 8
D, DI = 2560, 5120
CI = 640
LEN = 512
Q = 128
NB = LEN // Q
PAD = 16
HL = 32
HEADS = 10
EPS = 1e-05


def dot(a, b):
    return jnp.dot(a, b, preferred_element_type=F32)


def silu(x):
    half = 0.5 * x
    return half + half * jnp.tanh(half)


def split(x):
    high = x.astype(BF16)
    low = (x - high.astype(F32)).astype(BF16)
    return jnp.concatenate([high, low], axis=1)


def kernel(
    hid, gw, vw, bw, sw, vconv, bconv, sbias, lrate, gain, out, rms,
    hx, w, bwv, swv, cv, bcv, sb, lr, gn, prm, tap, ee, bs, vp, bct, cmat, bmat,
    av, es, fg, g, rx, dsum, dall, dxl, dx, bhl, vv, sbl, st, so, agg, p1, po, pin, ssm, ssa,
    ld, hs, hr, bsend, brecv, bhs, bhr, dsend, drecv, s1, r1, s2, r2, zs, zr, cs, cr,
):
    me, z = lax.axis_index("seq"), lax.axis_index("tp")
    core, chip = me & 1, lax.div(me, 2)
    early, late = 1 - core, core

    def remote(src, dst, ss, rs, seq=None, tp=None):
        where = {"seq": me if seq is None else seq, "tp": z if tp is None else tp}
        return pltpu.make_async_remote_copy(
            src_ref=src, dst_ref=dst, send_sem=ss, recv_sem=rs, device_id=where, device_id_type=MESH
        )

    barrier = pltpu.get_barrier_semaphore()

    def greet_seq(r, _):
        pl.semaphore_signal(
            barrier, inc=1, device_id={"seq": (me + r) & (NS - 1), "tp": z}, device_id_type=MESH
        )
        return 0

    def greet_tp(r, _):
        pl.semaphore_signal(
            barrier, inc=1, device_id={"seq": me, "tp": (z + r) & (NZ - 1)}, device_id_type=MESH
        )
        return 0

    lax.fori_loop(1, NZ, greet_tp, 0)

    small = [
        pltpu.make_async_copy(src, dst, ld.at[9 + n])
        for n, (src, dst) in enumerate(
            [(vconv, cv), (bconv, bcv), (sbias, sb), (lrate, lr), (gain, gn)]
        )
    ]
    load_b = pltpu.make_async_copy(bw, bwv, ld.at[0])
    load_s = pltpu.make_async_copy(sw, swv, ld.at[1])
    load_v0 = pltpu.make_async_copy(vw.at[:, 0:128], w.at[:, 128:256], ld.at[2])
    load_v1 = pltpu.make_async_copy(vw.at[:, 128:CI], w.at[:, 256:768], ld.at[7])
    load_g = pltpu.make_async_copy(gw, w.at[:, 768:1408], ld.at[8])

    def load_h(s, h):
        return pltpu.make_async_copy(
            hid.at[s, pl.ds(256 * h, 256)], hx.at[s, pl.ds(PAD + 256 * h, 256)], ld.at[3 + 2 * s + h]
        )

    load_b.start()
    load_s.start()
    for copy in small:
        copy.start()
    load_v0.start()
    for h in range(2):
        load_h(early, h).start()

    lax.fori_loop(1, NS, greet_seq, 0)

    row = lax.broadcasted_iota(jnp.int32, (256, CI), 0)
    col = lax.broadcasted_iota(jnp.int32, (256, CI), 1)
    ee[...] = jnp.where((row & 127) == HL + (col >> 6), 1.0, 0.0).astype(BF16)
    tri_at = lax.broadcasted_iota(jnp.int32, (Q, Q), 0) >= lax.broadcasted_iota(
        jnp.int32, (Q, Q), 1
    )
    tri = jnp.where(tri_at, 1.0, 0.0).astype(BF16)
    prm[...] = jnp.zeros((8, 128), F32)
    dsum[...] = jnp.zeros((8, 128), F32)
    for s in range(2):
        hx[s, 0:8, :] = jnp.zeros((8, D), BF16)

    @pl.when(me == 0)
    def _():
        for s in range(2):
            hx[s, 8:16, :] = jnp.zeros((8, D), BF16)

    for copy in small:
        copy.wait()
    prm[0:1, HL : HL + HEADS] = sb[...]
    prm[1:2, HL : HL + HEADS] = lr[...]
    for k in range(4):
        for h in range(2):
            taps = bcv[k : k + 1, 128 * h : 128 * h + 128]
            tap[2 * k + h] = jnp.broadcast_to(taps, (128, 128)).T
    load_b.wait()
    load_s.wait()
    for n in range(D // 128):
        lanes = slice(128 * n, 128 * n + 128)
        both = jnp.concatenate(
            [bwv[:, lanes].astype(F32), swv[:, lanes].astype(F32), jnp.zeros((86, 128), F32)], axis=0
        )
        w[lanes, 0:128] = both.T.astype(BF16)
    for h in range(2):
        load_h(late, h).start()
    load_v0.wait()

    def first(s):
        rows = 128 if s is early else 256
        for at in range(0, LEN, rows):
            if s is early and at % 256 == 0:
                load_h(s, at // 256).wait()
            got = dot(hx[s, PAD + at : PAD + at + rows, :], w[:, 0:256])
            bs[s, at : at + rows, :] = got[:, 0:128]
            vp[s, 0, PAD + at : PAD + at + rows, :] = got[:, 128:256]
        for b in range(NB):
            turned = bs[s, Q * b : Q * b + Q, :].T
            bct[s, z, :, Q * b : Q * b + Q] = turned[0:32, :].astype(BF16)

    def piece(p, owner, peer):
        if p == 2:
            return remote(bhl.at[owner], bhl.at[owner], bhs, bhr, tp=peer)
        part = bct.at[(early, late)[p], owner]
        return remote(part, part, bsend, brecv.at[p, owner], tp=peer)

    def away(n):
        return (z + n) & (NZ - 1)

    near = (2, -2, 1, -1)
    far_first = (4, 3, -3, 2, -2, 1, -1)
    to_b = jnp.where((z >= 2) & (z < 6), 1, -1)

    ahead = z < NZ // 2

    def send_piece(p, steps):
        for step in near[steps]:
            piece(p, z, away(step)).start()

    def pass_piece(p, way):
        owner = away(-2 * way)
        piece(p, owner, owner).wait_recv()
        piece(p, owner, away(way)).start()

        @pl.when(way == jnp.where(ahead, to_b, -to_b))
        def _():
            piece(p, owner, away(2 * way)).start()

    def rest_of_piece(p, owners):
        for owner in owners:
            gap = (owner - z) & (NZ - 1)

            @pl.when((gap != 0) & (gap != 2) & (gap != 6))
            def _():
                piece(p, owner, owner).wait_recv()

    def all_of(part, ss, rs):
        return remote(part, part, ss, rs, tp=away(1))

    def halo():
        return remote(hx.at[:, 520:528], hx.at[:, 8:16], hs, hr, seq=(me + 1) & (NS - 1))

    first(early)
    load_v1.start()
    for h in range(2):
        load_h(late, h).wait()

    @pl.when(ahead)
    def _():
        first(late)

    pl.semaphore_wait(barrier, NS - 1 + NZ - 1)

    @pl.when(me < NS - 1)
    def _():
        halo().start()

    send_piece(0, slice(0, 2))

    @pl.when(jnp.logical_not(ahead))
    def _():
        send_piece(0, slice(2, 4))
        first(late)

    load_g.start()

    @pl.when(ahead)
    def _():
        send_piece(1, slice(0, 2))
        send_piece(0, slice(2, 4))
        send_piece(1, slice(2, 4))

    lane = lax.broadcasted_iota(jnp.int32, (LEN, 128), 1)
    is_head = (lane >= HL) & (lane < HL + HEADS)
    rate = jnp.exp(prm[1:2, :])

    def steps(s):
        x = bs[s] + prm[0:1, :]
        size = jnp.maximum(x, 0.0) + jnp.log1p(jnp.exp(-jnp.abs(x)))
        size = jnp.where(is_head, size, 0.0)
        parts = split(-size * rate)
        so_far = jnp.zeros((1, 128), F32)
        halves, ahead, off = [], [], []
        for b in range(NB):
            sums = dot(tri, parts[Q * b : Q * b + Q, :])
            cum = sums[:, 0:128] + sums[:, 128:256]
            total = cum[Q - 1 : Q, :]
            mid = 0.5 * total
            off.append(cum - mid)
            halves.append(jnp.exp(mid))
            ahead.append(jnp.exp(so_far + mid))
            so_far = so_far + total
        off = jnp.concatenate(off, axis=0)
        av[s] = dot(split(size * jnp.exp(-off)), ee[...])
        es[s] = split(jnp.exp(off))
        rows = jnp.concatenate(halves + ahead + [jnp.zeros((8, 128), F32)], axis=0)
        rx[s] = dot(split(rows), ee[...])[0:8, :]
        dsum[pl.ds(s, 1), :] = so_far

    steps(early)
    steps(late)

    y, x = lax.div(chip, 4), chip & 3
    reach = [0, 1, 2, 1]
    offsets = sorted(
        ((dy, dx) for dy in range(4) for dx in range(4)), key=lambda o: -reach[o[0]] - reach[o[1]]
    )
    chips = [(((y + dy) & 3) * 4 + ((x + dx) & 3), (dy, dx) == (0, 0)) for dy, dx in offsets]
    others = [2 * c + n for c, own in chips for n in range(2) if not own] + [me + 1 - 2 * core]

    def decay(peer):
        return remote(dsum, dall.at[me], dsend, drecv, seq=peer)

    for peer in others:
        decay(peer).start()
    dall[me] = dsum[...]

    @pl.when(me > 0)
    def _():
        halo().wait_recv()

    both = jnp.concatenate([hx[0, 8:16, :], hx[1, 8:16, :]], axis=0)
    got = dot(both[:, : D // 2], w[: D // 2, 0:256]) + dot(both[:, D // 2 :], w[D // 2 :, 0:256])
    for s in range(2):
        vp[s, 0, 8:16, :] = got[8 * s : 8 * s + 8, 128:256]
    tail = jnp.concatenate([got[12:16, 0:128], got[4:8, 0:128]], axis=0)
    tail = jnp.where(lax.broadcasted_iota(jnp.int32, (8, 128), 1) < 32, tail, 0.0)
    bhl[z] = pltpu.roll(tail, 32 * (z & 3), 1).astype(BF16)
    for step in far_first:
        piece(2, z, away(step)).start()

    load_v1.wait()

    def project(s, at):
        got = dot(hx[s], w[:, 256 + 256 * at : 512 + 256 * at])
        vp[s, 1 + 2 * at] = got[:, 0:128]
        vp[s, 2 + 2 * at] = got[:, 128:256]

    def value(s, b):
        for c in range(5):
            lanes = slice(128 * c, 128 * c + 128)
            mixed = None
            for k in range(4):
                at = 13 + k + Q * b
                term = cv[k : k + 1, lanes] * vp[s, c, at : at + Q, :]
                mixed = term if mixed is None else mixed + term
            here = (s, slice(Q * b, Q * b + Q), lanes)
            vv[here] = (silu(mixed) * av[here]).astype(BF16)


    @pl.when(jnp.logical_not(ahead))
    def _():
        pass_piece(0, to_b)

    project(early, 0)
    project(early, 1)

    @pl.when(ahead)
    def _():
        pass_piece(0, to_b)

    pass_piece(1, to_b)

    @pl.when(jnp.logical_not(ahead))
    def _():
        send_piece(1, slice(0, 4))

    project(late, 0)
    project(late, 1)
    for b in range(NB):
        value(early, b)
    pass_piece(0, -to_b)

    def mix(s, h):
        rows = jnp.sum(bhl[4 * h : 4 * h + 4].astype(F32), axis=0)
        rows = jnp.where(s == 1, rows[0:4], rows[4:8])
        before = jnp.concatenate([jnp.zeros((124, 128), F32), rows], axis=0).T
        x = bct[s, 4 * h : 4 * h + 4].astype(F32).reshape(128, LEN)
        x = jnp.concatenate([before, x], axis=1)
        turned = [pltpu.roll(x, 3 - k, 1) for k in range(3)] + [x]
        blocks = []
        for b in range(NB):
            lanes = slice(128 + Q * b, 256 + Q * b)
            mixed = tap[h] * turned[0][:, lanes]
            for k in range(1, 4):
                mixed = mixed + tap[2 * k + h] * turned[k][:, lanes]
            blocks.append(silu(mixed))
        return blocks

    all_of(dall.at[0 : NS - 1], dsend, drecv).wait_recv()

    def pick(j, _):
        dxl[pl.ds(j, 1), :] = dall[2 * j, pl.ds(core, 1), :] + dall[2 * j + 1, pl.ds(core, 1), :]
        return 0

    lax.fori_loop(0, 16, pick, 0, unroll=True)
    dxl[16:17, :] = dall[2 * chip + 1, pl.ds(core, 1), :]
    dxl[24:32, :] = dall[2 * chip]
    dxl[17:24, :] = jnp.zeros((7, 128), F32)
    dx[...] = dot(split(jnp.exp(dxl[...])), ee[...])

    def states(s):
        for b, block in enumerate(mix(s, 0)):
            bmat[s, :, Q * b : Q * b + Q] = block.astype(BF16)
        state = None
        for b in range(NB):
            half = rx[s, b : b + 1, :]
            added = dot(bmat[s, :, Q * b : Q * b + Q], vv[s, Q * b : Q * b + Q, :]) * half
            if state is None:
                sbl[s, b] = jnp.zeros((128, CI), BF16)
                state = added
            else:
                lifted = state * half
                sbl[s, b] = lifted.astype(BF16)
                state = lifted * half + added
        for k in range(16):
            st[s, k] = state[8 * k : 8 * k + 8, :].astype(BF16)

    def across(s, n):
        return remote(st.at[s], so.at[s], cs.at[n], cr.at[n], seq=me + 1 - 2 * core)

    b_owners, c_owners = range(4), range(4, 8)
    all_of(bhl.at[0 : NZ - 1], bhs, bhr).wait_recv()
    rest_of_piece(0, b_owners)
    states(early)
    across(early, 0).start()
    for b in range(NB):
        value(late, b)
    rest_of_piece(1, b_owners)
    states(late)

    @pl.when(core == 0)
    def _():
        across(0, 1).start()

    def first_hop(source, k):
        return remote(agg.at[k], p1.at[source], s1, r1, seq=2 * k + core)

    across(late, 0).wait_recv()
    carry = dx[16:17, :]
    for k, own in chips:
        mine, other = st[late, k].astype(F32), so[late, k].astype(F32)
        slab = jnp.where(core == 0, mine, other) * carry + jnp.where(core == 0, other, mine)
        agg[k] = slab.astype(BF16)
        if own:
            p1[k] = agg[k]
        else:
            first_hop(chip, k).start()

    pass_piece(1, -to_b)

    load_g.wait()

    def gate(s):
        for top, rows, at, wide in (
            (0, LEN, 0, 256),
            (0, LEN, 256, 256),
            (0, LEN // 2, 512, 128),
            (LEN // 2, LEN // 2, 512, 128),
        ):
            here = slice(top, top + rows)
            got = dot(hx[s, PAD + top : PAD + top + rows, :], w[:, 768 + at : 768 + at + wide])
            factor = dot(es[s, here, :], ee[:, at : at + wide])
            fg[s, here, at : at + wide] = silu(got) * factor

    gate(early)

    def within(s):
        for b, block in enumerate(mix(s, 1)):
            cmat[s, Q * b : Q * b + Q, :] = block.T.astype(BF16)
        for b in range(NB):
            rows = slice(Q * b, Q * b + Q)
            c_rows = cmat[s, rows, :]
            scores = dot(c_rows, bmat[s, :, rows])
            scores = jnp.where(tri_at, scores, 0.0).astype(BF16)
            left = jnp.concatenate([scores, c_rows], axis=1)
            right = jnp.concatenate([vv[s, rows, :], sbl[s, b]], axis=0)
            g[s, rows, :] = dot(left, right)

    rest_of_piece(0, c_owners)
    within(early)

    all_of(p1.at[0:15], s1, r1).wait_recv()
    so_far = jnp.zeros((8, CI), F32)
    for j in range(16):
        po[j] = so_far.astype(BF16)
        so_far = so_far * dx[j : j + 1, :] + p1[j].astype(F32)

    def second_hop(target, source, group):
        slot = pin.at[late, source]
        return remote(po.at[target], slot, s2, r2.at[group], seq=2 * target + core)

    for n, (k, own) in enumerate(chips):
        if own:
            pin[late, k] = po[k]
        else:
            second_hop(k, chip, int(n < 5)).start()

    rest_of_piece(1, c_owners)
    within(late)
    gate(late)

    ones = jnp.ones((16, 128), BF16)
    at_row = lax.broadcasted_iota(jnp.int32, (8, 128), 0)
    squares = jnp.zeros((8, 128), F32)

    def back(s):
        return remote(pin.at[s], pin.at[s], cs.at[2], cr.at[2], seq=me + 1 - 2 * core)

    def back_slab(k):
        slab = pin.at[late, k]
        return remote(slab, slab, cs.at[2], cr.at[2], seq=me + 1 - 2 * core)

    all_of(po.at[0:10], s2, r2.at[0]).wait_recv()
    for k, _ in chips[5:]:
        back_slab(k).start()
    all_of(po.at[0:5], s2, r2.at[1]).wait_recv()
    for k, _ in chips[:5]:
        back_slab(k).start()

    @pl.when(core == 1)
    def _():
        across(0, 1).wait_recv()

    for s in (late, early):
        if s is early:
            back(early).wait_recv()
        arrived = pin[s].astype(F32).reshape(128, CI)
        moved = arrived * dx[pl.ds(24 + s, 1), :] + so[s].astype(F32).reshape(128, CI)
        arrived = jnp.where(core == 1, moved, arrived).astype(BF16)
        given = dot(cmat[s], arrived)
        for b in range(NB):
            rows = slice(Q * b, Q * b + Q)
            gated = fg[s, rows, :] * (g[s, rows, :] + given[rows] * rx[s, 4 + b : 5 + b, :])
            g[s, rows, :] = gated
            sq = gated * gated
            sq = sum(sq[:, 128 * c : 128 * c + 128] for c in range(1, 5)) + sq[:, 0:128]
            summed = lax.dot_general(
                ones, sq.astype(BF16), (((1,), (1,)), ((), ())), preferred_element_type=F32
            )[0:8, :]
            squares = jnp.where(at_row == 4 * s + b, summed, squares)
    ssm[...] = squares

    def total_sq(owner, peer):
        return remote(ssm, ssa.at[owner], zs, zr, tp=peer)

    for step in far_first:
        total_sq(z, away(step)).start()
    ssa[z] = ssm[...]
    gains = gn[...].reshape(1, CI)
    for s in range(2):
        out[s] = (g[s] * gains).astype(BF16)

    all_of(bct.at[:, 0 : NZ - 1], bsend, bsend).wait_send()
    all_of(bhl.at[0 : NZ - 1], bhs, bhr).wait_send()
    all_of(dall.at[0 : NS - 1], dsend, drecv).wait_send()
    all_of(p1.at[0:15], s1, r1).wait_send()
    all_of(po.at[0:15], s2, r2.at[0]).wait_send()
    across(early, 0).wait_send()
    back(late).wait_send()

    @pl.when(core == 0)
    def _():
        across(0, 1).wait_send()

    @pl.when(me < NS - 1)
    def _():
        halo().wait_send()

    all_of(ssa.at[0 : NZ - 1], zs, zr).wait_recv()
    rms[...] = lax.rsqrt(jnp.sum(ssa[...], axis=0) * (1.0 / DI) + EPS)
    all_of(ssa.at[0 : NZ - 1], zs, zr).wait_send()


def scaled(gated, rms, out, osc, sems):
    copies = []
    for s in range(2):
        for b in range(NB):
            n = NB * s + b
            rows = slice(Q * b, Q * b + Q)
            by_token = jnp.broadcast_to(rms[n : n + 1, :], (128, 128)).T
            for c in range(5):
                lanes = slice(128 * c, 128 * c + 128)
                osc[s, rows, lanes] = (gated[s, rows, lanes].astype(F32) * by_token).astype(BF16)
            copies.append(pltpu.make_async_copy(osc.at[s, rows], out.at[s, rows], sems.at[n]))
            copies[-1].start()
    for copy in copies:
        copy.wait()


def on_device(hid, gw, vw, bw, sw, vconv, bconv, sbias, lrate, gain):
    dma = pltpu.SemaphoreType.DMA
    vmem = pltpu.VMEM
    any_space = pl.BlockSpec(memory_space=pl.ANY)
    scratch = [
        vmem((2, PAD + LEN, D), BF16),
        vmem((D, 1408), BF16),
        vmem((32, D), BF16),
        vmem((HEADS, D), BF16),
        vmem((4, CI), F32),
        vmem((4, 256), F32),
        vmem((1, HEADS), F32),
        vmem((1, HEADS), F32),
        vmem((CI,), F32),
        vmem((8, 128), F32),
        vmem((8, 128, 128), F32),
        vmem((256, CI), BF16),
        vmem((2, LEN, 128), F32),
        vmem((2, 5, PAD + LEN, 128), F32),
        vmem((2, NZ, 32, LEN), BF16),
        vmem((2, LEN, 128), BF16),
        vmem((2, 128, LEN), BF16),
        vmem((2, LEN, CI), F32),
        vmem((2, LEN, 256), BF16),
        vmem((2, LEN, CI), F32),
        vmem((2, LEN, CI), F32),
        vmem((2, 8, CI), F32),
        vmem((8, 128), F32),
        vmem((NS, 8, 128), F32),
        vmem((NS, 128), F32),
        vmem((NS, CI), F32),
        vmem((NZ, 8, 128), BF16),
        vmem((2, LEN, CI), BF16),
        vmem((2, NB, 128, CI), BF16),
        vmem((2, 16, 8, CI), BF16),
        vmem((2, 16, 8, CI), BF16),
        vmem((16, 8, CI), BF16),
        vmem((16, 8, CI), BF16),
        vmem((16, 8, CI), BF16),
        vmem((2, 16, 8, CI), BF16),
        vmem((8, 128), F32),
        vmem((NZ, 8, 128), F32),
        dma((14,)),
        dma,
        dma,
        dma,
        dma((2, NZ)),
        dma,
        dma,
        dma,
        dma,
        dma,
        dma,
        dma,
        dma((2,)),
        dma,
        dma,
        dma((3,)),
        dma((3,)),
    ]
    in_vmem = pl.BlockSpec(memory_space=vmem)
    gated, rms = pl.pallas_call(
        kernel,
        out_shape=(vmem((2, LEN, CI), BF16), vmem((8, 128), F32)),
        in_specs=[any_space] * 10,
        out_specs=(in_vmem, in_vmem),
        scratch_shapes=scratch,
        compiler_params=pltpu.CompilerParams(
            collective_id=0, has_side_effects=True, vmem_limit_bytes=56 * 2**20
        ),
    )(
        hid, gw, vw, bw.T, sw.T, vconv, bconv,
        sbias.reshape(1, HEADS), lrate.reshape(1, HEADS), gain,
    )
    return pl.pallas_call(
        scaled,
        out_shape=jax.ShapeDtypeStruct((2, LEN, CI), BF16),
        in_specs=[in_vmem, in_vmem],
        out_specs=any_space,
        scratch_shapes=[vmem((2, LEN, CI), BF16), dma((2 * NB,))],
    )(*(pltpu.with_memory_space_constraint(x, vmem) for x in (gated, rms)))


def solution(mesh):
    placed = (
        P(None, "seq", None),
        P(None, "tp"),
        P(None, "tp"),
        P(None, "tp"),
        P(None, "tp"),
        P(None, "tp"),
        P(),
        P("tp"),
        P("tp"),
        P("tp"),
    )
    return jax.shard_map(
        on_device, mesh=mesh, in_specs=placed, out_specs=P(None, "seq", "tp"), check_vma=False
    )
```
